32 devices in a mesh: gx: 4 (over y, core), gz: 2 (over x), ta: 4 (over z).
Axes of the slice: x: 2, y: 2, z: 4, core: 2. Of those that a mesh axis runs over, the one named last changes fastest.
Arguments:
- links: float32 [4, 2, 3, 3, 16, 8, 512], P(None, None, None, None, 'ta', 'gz', 'gx'), may hold values from -1 to 1, as said below
Outputs:
- force: float32 [4, 2, 3, 3, 16, 8, 512], P(None, None, None, None, 'ta', 'gz', 'gx')
The draws below stay inside these ranges and needn't reach their ends.
Inputs may be any that keep to these rules, and one draw needn't show every extreme that they name: Every link matrix (real part links[mu, 0], imaginary part links[mu, 1]) is special unitary, up to float32 rounding.
All inputs are finite; a program needn't handle non-finite values.
Results may differ from the reference program's by a relative error of at most 0.0003.
Values sent between devices are 32-bit elements; how exact they have to be, the bound alone decides.
A program may use at most 64 MiB of HBM per device.

```python
import jax
import jax.numpy as jnp

NX = 16
NY = 32
NZ = 8
NT = 16
NXY = 512


def draw_links(key, part):
    sample = jax.random.normal(key, (2, 4, 3, 3, NT, NZ, NXY), jnp.float32)
    real0 = sample[0][:, 0]
    imag0 = sample[1][:, 0]
    length0 = jnp.maximum(jnp.sqrt(jnp.sum(real0 * real0 + imag0 * imag0, axis=1, keepdims=True)), 1e-06)
    real0 = real0 / length0
    imag0 = imag0 / length0
    real1 = sample[0][:, 1]
    imag1 = sample[1][:, 1]
    inner_real = jnp.sum(real0 * real1 + imag0 * imag1, axis=1, keepdims=True)
    inner_imag = jnp.sum(real0 * imag1 - imag0 * real1, axis=1, keepdims=True)
    real1 = real1 - (inner_real * real0 - inner_imag * imag0)
    imag1 = imag1 - (inner_real * imag0 + inner_imag * real0)
    length1 = jnp.maximum(jnp.sqrt(jnp.sum(real1 * real1 + imag1 * imag1, axis=1, keepdims=True)), 1e-06)
    real1 = real1 / length1
    imag1 = imag1 / length1
    real_cols = []
    imag_cols = []
    for column in range(3):
        next_col = (column + 1) % 3
        last_col = (column + 2) % 3
        cross_real = real0[:, next_col] * real1[:, last_col] - imag0[:, next_col] * imag1[:, last_col] - real0[:, last_col] * real1[:, next_col] + imag0[:, last_col] * imag1[:, next_col]
        cross_imag = real0[:, next_col] * imag1[:, last_col] + imag0[:, next_col] * real1[:, last_col] - real0[:, last_col] * imag1[:, next_col] - imag0[:, last_col] * real1[:, next_col]
        real_cols.append(cross_real)
        imag_cols.append(-cross_imag)
    real2 = jnp.stack(real_cols, axis=1)
    imag2 = jnp.stack(imag_cols, axis=1)
    real_rows = jnp.stack([real0, real1, real2], axis=1)
    imag_rows = jnp.stack([imag0, imag1, imag2], axis=1)
    return jnp.stack([real_rows, imag_rows], axis=1)


def setup_inputs(seed: int = 0) -> dict:
    seeds = jax.random.split(jax.random.key(seed), 2)
    links = draw_links(jax.random.fold_in(seeds[1], 71), 0)
    return dict(links=links)


COEFF = -1.9


def matprod(left, right):
    total = left[:, 0][:, None] * right[0][None, :]
    total = total + left[:, 1][:, None] * right[1][None, :]
    return total + left[:, 2][:, None] * right[2][None, :]


def complex_mul(left, right):
    return (matprod(left[0], right[0]) - matprod(left[1], right[1]),
            matprod(left[0], right[1]) + matprod(left[1], right[0]))


def dagger(matrix):
    return (jnp.swapaxes(matrix[0], 0, 1), -jnp.swapaxes(matrix[1], 0, 1))


def unit_step(direction, sign):
    offset = [0, 0, 0, 0]
    offset[direction] = sign
    return tuple(offset)


def joined(first_step, second_step):
    return tuple(first_step[position] + second_step[position] for position in range(4))


def gauge_force(fetch_link):
    blocks = []
    still = (0, 0, 0, 0)
    for direction in range(4):
        ahead = unit_step(direction, 1)
        summed = None
        for transverse in range(4):
            if transverse == direction:
                continue
            side_up = unit_step(transverse, 1)
            side_down = unit_step(transverse, -1)
            upper = complex_mul(complex_mul(fetch_link(transverse, ahead), dagger(fetch_link(direction, side_up))),
                                dagger(fetch_link(transverse, still)))
            lower = complex_mul(complex_mul(dagger(fetch_link(transverse, joined(ahead, side_down))),
                                            dagger(fetch_link(direction, side_down))),
                                fetch_link(transverse, side_down))
            staple = (upper[0] + lower[0], upper[1] + lower[1])
            summed = staple if summed is None else (summed[0] + staple[0], summed[1] + staple[1])
        loop_matrix = complex_mul(fetch_link(direction, still), summed)
        real_part = 0.5 * (loop_matrix[0] - jnp.swapaxes(loop_matrix[0], 0, 1))
        imag_part = 0.5 * (loop_matrix[1] + jnp.swapaxes(loop_matrix[1], 0, 1))
        trace_third = (loop_matrix[1][0, 0] + loop_matrix[1][1, 1] + loop_matrix[1][2, 2]) / 3.0
        identity = jnp.eye(3, dtype=jnp.float32).reshape((3, 3) + (1,) * trace_third.ndim)
        imag_part = imag_part - identity * trace_third
        blocks.append(COEFF * jnp.stack([real_part, imag_part], axis=0))
    return jnp.stack(blocks, axis=0)


def reference(links):
    lattice = links.reshape(links.shape[:6] + (NY, NX))

    def fetch_link(direction, offset):
        field = lattice[direction]
        field = jnp.roll(field, (-offset[0], -offset[1], -offset[2], -offset[3]), axis=(3, 4, 5, 6))
        return (field[0], field[1])

    return gauge_force(fetch_link).reshape(links.shape)
```

```python
import functools

import jax
import jax.numpy as jnp
from jax import lax
from jax.experimental import pallas as pl
from jax.experimental.pallas import tpu as pltpu
from jax.sharding import PartitionSpec as P

NX = 16
COEFF = -1.9
AXES = ("ta", "gz", "gx")
SUB, LANES = 8, 128


def others(d):
    return [m for m in range(4) if m != d]


class Lattice:
    def __init__(self, depth):
        self.depth = depth
        self.per = SUB // depth
        self.ygroups = LANES // NX
        self.row = lax.broadcasted_iota(jnp.int32, (SUB, LANES), 0)
        self.lane = lax.broadcasted_iota(jnp.int32, (SUB, LANES), 1)
        self.zrow = self.row % depth
        self.xcol = self.lane % NX

    def rows(self, value, shift):
        shift %= SUB
        return pltpu.roll(value, shift, 0) if shift else value

    def lanes(self, value, shift):
        shift %= LANES
        return pltpu.roll(value, shift, 1) if shift else value


def entry(left, right, i, j, part, left_h, right_h):
    total = None
    for k in range(3):
        li = (k, i) if left_h else (i, k)
        ri = (j, k) if right_h else (k, j)
        lr, lm = left[0][li[0]][li[1]], left[1][li[0]][li[1]]
        rr, rm = right[0][ri[0]][ri[1]], right[1][ri[0]][ri[1]]
        if part == 0:
            first, second = lr * rr, lm * rm
            minus = left_h == right_h
        elif left_h:
            first, second = lr * rm, lm * rr
            minus = True
        else:
            first, second = lm * rr, lr * rm
            minus = right_h
        value = first - second if minus else first + second
        total = value if total is None else total + value
    return total


def product(left, right, left_h=False, right_h=False):
    return [
        [[entry(left, right, i, j, part, left_h, right_h) for j in range(3)] for i in range(3)]
        for part in range(2)
    ]


def projected(left, right, left_h=False, right_h=False):
    get = lambda i, j, part: entry(left, right, i, j, part, left_h, right_h)
    pairs = ((0, 1), (0, 2), (1, 2))
    real = [get(i, j, 0) - get(j, i, 0) for i, j in pairs]
    imag = [get(i, j, 1) + get(j, i, 1) for i, j in pairs]
    diag = [get(i, i, 1) for i in range(3)]
    third = (diag[0] + diag[1] + diag[2]) * (1.0 / 3.0)
    return real + imag + [diag[0] - third, diag[1] - third]


def third_row(real, imag):
    rows_r, rows_i = [], []
    for column in range(3):
        n, l = (column + 1) % 3, (column + 2) % 3
        rows_r.append(
            real[0][n] * real[1][l]
            - imag[0][n] * imag[1][l]
            - real[0][l] * real[1][n]
            + imag[0][l] * imag[1][n]
        )
        rows_i.append(
            real[0][l] * imag[1][n]
            + imag[0][l] * real[1][n]
            - real[0][n] * imag[1][l]
            - imag[0][n] * real[1][l]
        )
    return rows_r, rows_i


PLANES = ((2, 3), (1, 3), (1, 2), (0, 1), (0, 2), (0, 3))
KINDS = ({0: 1}, {1: 1}, {2: 1}, {0: 1, 1: -1}, {0: 1, 2: -1}, {1: 1, 2: -1})
CORNERS = {(0, 1): (3, 1), (1, 0): (3, -1), (0, 2): (4, 1), (2, 0): (4, -1), (1, 2): (5, 1), (2, 1): (5, -1)}
FIXED = [(0, 1, 0), (0, 2, 0), (1, 0, -1), (1, 2, None), (2, 0, -1), (2, 1, None)]


def force_terms(
    counts, depth, halves, hbm, acc,
    u, ahead_s, local_s, fixed_s, st, sz, sy, rt, rz, ry, vts, vzs, vys, vtr, vzr, vyr,
    c01, c10, c02, c20, c12, c21, k01, k10, k02, k20, k12, k21,
    load_sem, send, recv, ready,
):
    g = Lattice(depth)
    last = halves - 1
    me = [lax.axis_index(a) for a in AXES]
    corner_out = {(0, 1): c01, (1, 0): c10, (0, 2): c02, (2, 0): c20, (1, 2): c12, (2, 1): c21}
    corner_in = {(0, 1): k01, (1, 0): k10, (0, 2): k02, (2, 0): k20, (1, 2): k12, (2, 1): k21}

    loads = [
        pltpu.make_async_copy(hbm.at[m, :, 0:2], u.at[m, :, 0:2], load_sem.at[m]) for m in range(4)
    ]
    last_rows = pltpu.make_async_copy(hbm.at[:, :, 2], u.at[:, :, 2], load_sem.at[4])
    for m in (0, 3, 1, 2):
        loads[m].start()
    last_rows.start()

    def peer(kind, sign):
        where = list(me)
        for i, step in KINDS[kind].items():
            where[i] = lax.rem(me[i] + counts[i] + sign * step, counts[i])
        by = dict(zip(AXES, where))
        return (by["gx"], by["gz"], by["ta"])

    def axis_of(kind):
        return next(iter(KINDS[kind]))

    def greets(axis, sign):
        return me[axis] < counts[axis] - 1 if sign > 0 else me[axis] == 0

    barrier = pltpu.get_barrier_semaphore()
    expected = 0
    for axis in range(3):
        for sign in (1, -1):
            kinds = [k for k in range(6) if axis_of(k) == axis]
            expected = expected + jnp.where(greets(axis, sign), 0, len(kinds))

            @pl.when(greets(axis, sign))
            def _():
                for k in kinds:
                    pl.semaphore_signal(
                        barrier, inc=1, device_id=peer(k, sign), device_id_type=pl.DeviceIdType.MESH
                    )

    @pl.when(expected > 0)
    def _():
        pl.semaphore_wait(barrier, expected)

    for axis in range(3):
        for sign in (1, -1):
            kinds = [k for k in range(6) if axis_of(k) == axis]

            @pl.when(jnp.logical_not(greets(axis, sign)))
            def _():
                for k in kinds:
                    pl.semaphore_signal(
                        ready.at[2 * k + (sign > 0)], inc=1,
                        device_id=peer(k, sign), device_id_type=pl.DeviceIdType.MESH,
                    )

    def met(kind, sign):
        pl.semaphore_wait(ready.at[2 * kind + (sign < 0)], 1)

    def meet(kind, sign):
        @pl.when(greets(axis_of(kind), sign))
        def _():
            met(kind, sign)

    def load(m, part, i, j, h):
        return u[m, part, i, j, h * SUB : (h + 1) * SUB, :]

    COMPS = [(part, i, j) for part in range(2) for i in range(2) for j in range(3)]

    def comps(m):
        return [(m,) + c for c in COMPS]

    def all_comps(d):
        return [c for m in others(d) for c in comps(m)]

    def flat(value):
        return [value[part][i][j] for part, i, j in COMPS]

    def merge(values, index, step):
        total = None
        for k, x in enumerate(values):
            total = x if total is None else jnp.where(index >= step * k, x, total)
        return total

    def pack_t(m):
        cs, base = comps(m), 12 * others(0).index(m)
        for c0 in range(0, 12, g.per):
            r = (base + c0) // g.per * SUB
            st[r : r + SUB, :] = merge(
                [g.rows(load(*cs[c0 + k], 0), depth * k) for k in range(g.per)], g.row, depth
            )

    def pack_z(m):
        cs, base = comps(m), 12 * others(1).index(m)
        for c0 in range(0, 12, depth):
            for h in range(halves):
                r = ((base + c0) // depth * halves + h) * SUB
                sz[r : r + SUB, :] = merge(
                    [g.rows(load(*cs[c0 + k], h), k) for k in range(depth)], g.zrow, 1
                )

    def pack_y():
        cs = all_comps(2)
        for c0 in range(0, len(cs), g.ygroups):
            for h in range(halves):
                r = (c0 // g.ygroups * halves + h) * SUB
                sy[r : r + SUB, :] = merge(
                    [
                        g.lanes(load(*cs[c0 + k], h), NX * k)
                        for k in range(min(g.ygroups, len(cs) - c0))
                    ],
                    g.lane, NX,
                )

    def pack_vt(m, v):
        base = 12 * others(0).index(m)
        for c0 in range(0, 12, g.per):
            r = (base + c0) // g.per * SUB
            vts[r : r + SUB, :] = merge(
                [g.rows(v[c0 + k], depth * (k + 1)) for k in range(g.per)], g.row, depth
            )

    def pack_vz(m, h, v):
        base = 12 * others(1).index(m)
        for c0 in range(0, 12, depth):
            r = ((base + c0) // depth * halves + h) * SUB
            vzs[r : r + SUB, :] = merge(
                [g.rows(v[c0 + k], k + 1 - depth) for k in range(depth)], g.zrow, 1
            )

    def pack_vy(m, v):
        n = vys.shape[0] // 3
        for c0 in range(0, 12 * halves, g.ygroups):
            r = others(2).index(m) * n + c0 // g.ygroups * SUB
            vys[r : r + SUB, :] = merge(
                [
                    g.lanes(v[c0 + k], NX * (k + 1))
                    for k in range(min(g.ygroups, 12 * halves - c0))
                ],
                g.lane, NX,
            )

    def by_groups(d, h, up, shift, index, step):
        cs = comps(d)
        return merge(
            [
                merge(
                    [
                        g.lanes(g.rows(load(*cs[c], h), shift(c // g.ygroups)), NX * (c % g.ygroups + up))
                        for c in range(c0, min(12, c0 + g.ygroups))
                    ],
                    g.lane, NX,
                )
                for c0 in range(0, 12, g.ygroups)
            ],
            index, step,
        )

    def pack_corner(d, m):
        ref, cs = corner_out[d, m], comps(d)
        if (d, m) in ((0, 1), (1, 0)):
            source = SUB - depth if d == 0 else depth - 1
            for c0 in range(0, 12, SUB):
                ref[c0 : c0 + SUB, :] = merge(
                    [
                        g.rows(load(*cs[c0 + k], last if d == 0 else 0), k - source)
                        for k in range(min(SUB, 12 - c0))
                    ],
                    g.row, 1,
                )
        elif (d, m) == (0, 2):
            ref[...] = by_groups(0, last, 0, lambda k: depth * (k + 1), g.row, depth)
        elif (d, m) == (2, 0):
            ref[...] = by_groups(2, 0, 1, lambda k: depth * k, g.row, depth)
        else:
            for h in range(halves):
                up, source = (0, depth - 1) if d == 1 else (1, 0)
                ref[h * SUB : (h + 1) * SUB, :] = by_groups(
                    d, h, up, lambda k: k - source, g.zrow, 1
                )

    def corner(d, m, h, c):
        ref = corner_in[d, m]
        k, group = c // g.ygroups, NX * (c % g.ygroups)
        if (d, m) in ((0, 1), (1, 0)):
            target = depth - 1 if d == 0 else SUB - depth
            r = c // SUB * SUB
            return g.rows(ref[r : r + SUB, :], target - c % SUB)
        if (d, m) == (0, 2):
            return g.lanes(g.rows(ref[...], -depth * k), LANES - NX - group)
        if (d, m) == (2, 0):
            return g.lanes(g.rows(ref[...], SUB - depth - depth * k), -group)
        value = ref[h * SUB : (h + 1) * SUB, :]
        if d == 1:
            return g.lanes(g.rows(value, -k), LANES - NX - group)
        return g.lanes(g.rows(value, depth - 1 - k), -group)

    slots = {}

    def remote(src, dst, kind, sign):
        slot = len(slots)
        slots[slot] = pltpu.make_async_remote_copy(
            src_ref=src, dst_ref=dst, send_sem=send.at[slot], recv_sem=recv.at[slot],
            device_id=peer(kind, sign), device_id_type=pl.DeviceIdType.MESH,
        )
        return slots[slot]

    def chunk(ref, d, m):
        n = ref.shape[0] // 3
        k = others(d).index(m)
        return ref.at[k * n : (k + 1) * n]

    low = {
        (d, m): remote(chunk(s, d, m), chunk(r, d, m), d, -1)
        for d, s, r in ((0, st, rt), (1, sz, rz)) for m in others(d)
    }
    low[2, None] = remote(sy, ry, 2, -1)
    high = {
        (d, m): remote(chunk(s, d, m), chunk(r, d, m), d, 1)
        for d, s, r in ((0, vts, vtr), (1, vzs, vzr), (2, vys, vyr)) for m in others(d)
    }
    corners = {
        key: remote(corner_out[key], corner_in[key], kind, sign)
        for key, (kind, sign) in CORNERS.items()
    }

    def matrix(m, h):
        return [[[load(m, part, i, j, h) for j in range(3)] for i in range(3)] for part in range(2)]

    def save(ref, index, value):
        for part in range(2):
            for i in range(len(value[part])):
                for j in range(3):
                    ref[index, part, i, j] = value[part][i][j]

    def saved(ref, index, rows=3):
        return [[[ref[index, part, i, j] for j in range(3)] for i in range(rows)] for part in range(2)]

    def rolled(m, d, h, part, i, j):
        v = load(m, part, i, j, h)
        if d == 3:
            return jnp.where(g.xcol == NX - 1, g.lanes(v, NX - 1), g.lanes(v, -1))
        if d == 2:
            return g.lanes(v, -NX)
        if d == 1:
            return g.rows(v, -1)
        if h + 1 < halves:
            beyond = g.rows(load(m, part, i, j, h + 1), -depth)
            return jnp.where(g.row >= SUB - depth, beyond, g.rows(v, -depth))
        return g.rows(v, -depth)

    def complete(d, h):
        return d == 3 or (d == 0 and h + 1 < halves)

    def far_edge(d):
        return (g.row >= SUB - depth, g.zrow == depth - 1, g.lane >= LANES - NX)[d]

    ahead_slot = {}

    def prepare(m, d, h, rows):
        value = [
            [[rolled(m, d, h, part, i, j) for j in range(3)] for i in range(3 if rows == 3 or complete(d, h) else 2)]
            for part in range(2)
        ]
        ahead_slot[m, d, h] = len(ahead_slot)
        keep = 3 if complete(d, h) else 2
        save(ahead_s, ahead_slot[m, d, h], [part[:keep] for part in value])
        return value

    def transported(b, m, d, h, b_h):
        moved = prepare(m, d, h, 3)
        value = [
            [[entry(b, moved, i, j, part, b_h, False) for j in range(3)] for i in range(2)]
            for part in range(2)
        ]
        if not complete(d, h):
            edge = far_edge(d)
            for part in range(2):
                for i in range(2):
                    for j in range(3):
                        own = b[part][j][i] if b_h else b[part][i][j]
                        own = -own if b_h and part else own
                        value[part][i][j] = jnp.where(edge, own, value[part][i][j])
        return flat(value)

    local = {}

    def local_product(mu, nu, h):
        b = product(matrix(mu, h), matrix(nu, h), left_h=True)
        save(local_s, PLANES.index((mu, nu)) * halves + h, b)
        return b

    for copy in [loads[m] for m in (0, 3, 1, 2)] + [last_rows]:
        copy.wait()
    pack_corner(0, 1)
    pack_corner(0, 2)
    for m in (3, 1, 2):
        b = local_product(0, m, last)
        pack_vt(m, transported(b, 0, m, last, False))

    at_end = me[0] == counts[0] - 1
    upward = [corners[0, 1], corners[0, 2]] + [high[0, m] for m in (3, 1, 2)]
    downward = [low[0, m] for m in (3, 1, 2)] + [corners[1, 0], corners[2, 0]]

    @pl.when(at_end)
    def _():
        for copy in upward:
            copy.start()

    pack_y()
    meet(2, -1)
    low[2, None].start()
    for m in (3, 2, 0):
        pack_z(m)
    pack_corner(1, 2)
    pack_corner(2, 1)
    meet(1, -1)
    for m in (3, 2, 0):
        low[1, m].start()
    meet(5, 1)
    corners[1, 2].start()
    meet(5, -1)
    corners[2, 1].start()
    for m in (3, 1, 2):
        pack_t(m)
    pack_corner(1, 0)
    pack_corner(2, 0)

    @pl.when(me[0] > 0)
    def _():
        for copy in downward:
            copy.start()

    @pl.when(jnp.logical_not(at_end))
    def _():
        for kind in (0, 3, 4):
            met(kind, 1)
        for copy in upward:
            copy.start()

    for mu, nu in ((2, 3), (1, 3), (1, 2), (0, 2), (0, 1), (0, 3)):
        lifted = {}
        for h in range(halves):
            if mu == 0 and h == last:
                b = saved(local_s, PLANES.index((mu, nu)) * halves + h)
            else:
                b = local_product(mu, nu, h)
            if mu:
                lifted[mu, nu, h] = transported(b, mu, nu, h, False)
            elif h != last:
                prepare(mu, nu, h, 2)
            if nu != 3:
                lifted[nu, mu, h] = transported(b, nu, mu, h, True)
            else:
                prepare(nu, mu, h, 2)
        for d, m in ((mu, nu), (nu, mu)):
            if d == 1:
                for h in range(halves):
                    pack_vz(m, h, lifted[d, m, h])
            elif d == 2:
                pack_vy(m, [x for h in range(halves) for x in lifted[d, m, h]])
            if d in (1, 2):
                if (d, m) in ((2, 3), (1, 3)):
                    meet(d, 1)
                high[d, m].start()

    def ahead(m, d, h):
        if complete(d, h):
            return saved(ahead_s, ahead_slot[m, d, h])
        index = {c: n for n, c in enumerate(all_comps(d))}

        def get(part, i, j):
            v = ahead_s[ahead_slot[m, d, h], part, i, j]
            c = index[(m, part, i, j)]
            if d == 0:
                r = c // g.per * SUB
                edge = g.rows(rt[r : r + SUB, :], SUB - depth - depth * (c % g.per))
            elif d == 1:
                r = (c // depth * halves + h) * SUB
                edge = g.rows(rz[r : r + SUB, :], depth - 1 - c % depth)
            else:
                r = (c // g.ygroups * halves + h) * SUB
                edge = g.lanes(ry[r : r + SUB, :], LANES - NX - NX * (c % g.ygroups))
            return jnp.where(far_edge(d), edge, v)

        return complete_rows(get)

    def complete_rows(get):
        real = [[get(0, i, j) for j in range(3)] for i in range(2)]
        imag = [[get(1, i, j) for j in range(3)] for i in range(2)]
        third_r, third_i = third_row(real, imag)
        return [real + [third_r], imag + [third_i]]

    seen = set()

    def add(m, c, h, value):
        r = ((m * 8 + c) * halves + h) * SUB
        if (m, c, h) in seen:
            acc[r : r + SUB, :] += value
        else:
            seen.add((m, c, h))
            acc[r : r + SUB, :] = value

    def shifted(q, d):
        if d == 3:
            return jnp.where(g.xcol == 0, g.lanes(q, 1 - NX), g.lanes(q, 1))
        if d == 2:
            return jnp.where(g.lane >= NX, g.lanes(q, NX), 0.0)
        if d == 1:
            return jnp.where(g.zrow > 0, g.rows(q, 1), 0.0)
        return jnp.where(g.row >= depth, g.rows(q, depth), 0.0)

    def plane(mu, nu, h):
        a = product(ahead(nu, mu, h), ahead(mu, nu, h), right_h=True)
        b = saved(local_s, PLANES.index((mu, nu)) * halves + h)
        e = product(matrix(mu, h), a)
        upper = projected(e, matrix(nu, h), right_h=True)
        q = projected(a, b, left_h=True)
        for c in range(8):
            add(mu, c, h, shifted(q[c], nu) + upper[c])
        q = projected(a, b, right_h=True)
        for c in range(8):
            add(nu, c, h, shifted(q[c], mu) - upper[c])
            if mu == 0 and h + 1 < halves:
                add(nu, c, h + 1, jnp.where(g.row < depth, g.rows(q[c], depth), 0.0))

    fixed_slot = {}

    def fix(d, m, h):
        beyond = complete_rows(lambda part, i, j: corner(d, m, h, part * 6 + i * 3 + j))
        own = matrix(m, h)
        moved = product(own, beyond, right_h=True)
        edge = far_edge(m)
        fixed_slot[d, m, h] = len(fixed_slot)
        save(
            fixed_s, fixed_slot[d, m, h],
            [[[jnp.where(edge, moved[p][i][j], own[p][i][j]) for j in range(3)] for i in range(3)] for p in range(2)],
        )

    def lower(d, m, h):
        def get(part, i, j):
            c = part * 6 + i * 3 + j
            base = 12 * others(d).index(m) + c
            if d == 0:
                r = base // g.per * SUB
                return g.rows(vtr[r : r + SUB, :], -depth * (base % g.per))
            if d == 1:
                r = (base // depth * halves + h) * SUB
                return g.rows(vzr[r : r + SUB, :], -(base % depth))
            n, k = vyr.shape[0] // 3, h * 12 + c
            r = others(2).index(m) * n + k // g.ygroups * SUB
            return g.lanes(vyr[r : r + SUB, :], -NX * (k % g.ygroups))

        if (d, m, h) in fixed_slot:
            left = saved(fixed_s, fixed_slot[d, m, h])
        else:
            left = matrix(m, h)
        q = projected(left, complete_rows(get), right_h=True)
        near = (g.row < depth, g.zrow == 0, g.lane < NX)[d]
        for c in range(8):
            add(m, c, h, jnp.where(near, q[c], 0.0))

    for h in range(last):
        plane(0, 3, h)
    low[2, None].wait_recv()
    for h in range(halves):
        plane(2, 3, h)
    for h in range(last):
        plane(0, 2, h)
    low[1, 3].wait_recv()
    for h in range(halves):
        plane(1, 3, h)
    low[1, 2].wait_recv()
    for h in range(halves):
        plane(1, 2, h)
    low[1, 0].wait_recv()
    for h in range(last):
        plane(0, 1, h)

    @pl.when(me[0] == 0)
    def _():
        for kind in (0, 3, 4):
            met(kind, -1)
        for copy in downward:
            copy.start()

    for d, m in ((2, 3), (2, 1), (2, 0), (1, 3), (1, 2), (1, 0)):
        if (d, m) in ((2, 1), (1, 2)):
            corners[d, m].wait_recv()
            for h in range(halves):
                fix(d, m, h)
        high[d, m].wait_recv()
        for h in range(halves if m else last):
            lower(d, m, h)
    for m in (3, 1, 2):
        low[0, m].wait_recv()
        plane(0, m, last)
    for d in (1, 2):
        corners[d, 0].wait_recv()
        fix(d, 0, last)
        lower(d, 0, last)
    for m in (1, 2):
        corners[0, m].wait_recv()
        fix(0, m, 0)
    for m in (3, 1, 2):
        high[0, m].wait_recv()
        lower(0, m, 0)
    for copy in slots.values():
        copy.wait_send()


def expand(halves, acc, hbm, out, sems):
    copies = []
    for m in range(4):
        for h in range(halves):
            rows = [((m * 8 + c) * halves + h) * SUB for c in range(8)]
            f = [acc[r : r + SUB, :] * (COEFF * 0.5 if c < 6 else COEFF) for c, r in enumerate(rows)]

            def put(part, i, j, value):
                out[m, part, i, j, h * SUB : (h + 1) * SUB, :] = value

            for n, (i, j) in enumerate(((0, 1), (0, 2), (1, 2))):
                put(0, i, j, f[n])
                put(0, j, i, -f[n])
                put(1, i, j, f[3 + n])
                put(1, j, i, f[3 + n])
            for i in range(3):
                put(0, i, i, jnp.zeros((SUB, LANES), jnp.float32))
            put(1, 0, 0, f[6])
            put(1, 1, 1, f[7])
            put(1, 2, 2, -(f[6] + f[7]))
        copies.append(pltpu.make_async_copy(out.at[m], hbm.at[m], sems.at[m]))
        copies[-1].start()
    for copy in copies:
        copy.wait()


def per_device(counts, links):
    time_len, depth, flat = links.shape[4:]
    sites = time_len * depth
    assert flat == LANES and SUB % depth == 0 and sites % SUB == 0 and 2 <= depth <= SUB // 2
    halves = sites // SUB
    per, yg = SUB // depth, LANES // NX
    up = lambda a, b: -(-a // b) * SUB
    vmem = lambda *s: pltpu.VMEM(s + (LANES,), jnp.float32)
    shape = links.shape[:4] + (sites, flat)
    rt, rz, ry = up(36, per), up(36, depth) * halves, up(36, yg) * halves
    vy = 3 * up(12 * halves, yg)
    corner = [vmem(r) for r in (2 * SUB, 2 * SUB, SUB, SUB, SUB * halves, SUB * halves)]
    terms = pl.pallas_call(
        functools.partial(force_terms, counts, depth, halves),
        out_shape=pltpu.VMEM((32 * sites, flat), jnp.float32),
        in_specs=[pl.BlockSpec(memory_space=pl.ANY)],
        out_specs=pl.BlockSpec(memory_space=pltpu.VMEM),
        scratch_shapes=[
            vmem(*shape[:-1]),
            vmem(12 * halves, 2, 3, 3, SUB),
            vmem(6 * halves, 2, 3, 3, SUB),
            vmem(4 + 2 * halves, 2, 3, 3, SUB),
        ]
        + [vmem(r) for r in (rt, rz, ry) * 2 + (rt, rz, vy) * 2]
        + corner * 2
        + [
            pltpu.SemaphoreType.DMA((5,)),
            pltpu.SemaphoreType.DMA((22,)),
            pltpu.SemaphoreType.DMA((22,)),
            pltpu.SemaphoreType.REGULAR((12,)),
        ],
        compiler_params=pltpu.CompilerParams(collective_id=0, has_side_effects=True),
        name="force_terms",
    )(links.reshape(shape))
    out = pl.pallas_call(
        functools.partial(expand, halves),
        out_shape=jax.ShapeDtypeStruct(shape, jnp.float32),
        in_specs=[pl.BlockSpec(memory_space=pltpu.VMEM)],
        out_specs=pl.BlockSpec(memory_space=pl.ANY),
        scratch_shapes=[vmem(*shape[:-1]), pltpu.SemaphoreType.DMA((4,))],
        name="expand",
    )(pltpu.with_memory_space_constraint(terms, pltpu.VMEM))
    return out.reshape(links.shape)


def solution(mesh):
    assert mesh.axis_names == ("gx", "gz", "ta")
    counts = tuple(mesh.shape[a] for a in AXES)
    spec = P(None, None, None, None, "ta", "gz", "gx")
    return jax.shard_map(
        functools.partial(per_device, counts),
        mesh=mesh,
        in_specs=(spec,),
        out_specs=spec,
        check_vma=False,
    )
```

```python
import functools

import jax
import jax.numpy as jnp
from jax import lax
from jax.experimental import pallas as pl
from jax.experimental.pallas import tpu as pltpu
from jax.sharding import PartitionSpec as P

NX = 16
COEFF = -1.9
AXES = ("ta", "gz", "gx")
SUB, LANES = 8, 128


def others(d):
    return [m for m in range(4) if m != d]


class Lattice:
    def __init__(self, depth):
        self.depth = depth
        self.per = SUB // depth
        self.ygroups = LANES // NX
        self.row = lax.broadcasted_iota(jnp.int32, (SUB, LANES), 0)
        self.lane = lax.broadcasted_iota(jnp.int32, (SUB, LANES), 1)
        self.zrow = self.row % depth
        self.xcol = self.lane % NX

    def rows(self, value, shift):
        shift %= SUB
        return pltpu.roll(value, shift, 0) if shift else value

    def lanes(self, value, shift):
        shift %= LANES
        return pltpu.roll(value, shift, 1) if shift else value


def entry(left, right, i, j, part, left_h, right_h):
    total = None
    for k in range(3):
        li = (k, i) if left_h else (i, k)
        ri = (j, k) if right_h else (k, j)
        lr, lm = left[0][li[0]][li[1]], left[1][li[0]][li[1]]
        rr, rm = right[0][ri[0]][ri[1]], right[1][ri[0]][ri[1]]
        if part == 0:
            first, second = lr * rr, lm * rm
            minus = left_h == right_h
        elif left_h:
            first, second = lr * rm, lm * rr
            minus = True
        else:
            first, second = lm * rr, lr * rm
            minus = right_h
        value = first - second if minus else first + second
        total = value if total is None else total + value
    return total


def product(left, right, left_h=False, right_h=False):
    return [
        [[entry(left, right, i, j, part, left_h, right_h) for j in range(3)] for i in range(3)]
        for part in range(2)
    ]


def projected(left, right, left_h=False, right_h=False):
    get = lambda i, j, part: entry(left, right, i, j, part, left_h, right_h)
    pairs = ((0, 1), (0, 2), (1, 2))
    real = [get(i, j, 0) - get(j, i, 0) for i, j in pairs]
    imag = [get(i, j, 1) + get(j, i, 1) for i, j in pairs]
    diag = [get(i, i, 1) for i in range(3)]
    third = (diag[0] + diag[1] + diag[2]) * (1.0 / 3.0)
    return real + imag + [diag[0] - third, diag[1] - third]


def third_row(real, imag):
    rows_r, rows_i = [], []
    for column in range(3):
        n, l = (column + 1) % 3, (column + 2) % 3
        rows_r.append(
            real[0][n] * real[1][l]
            - imag[0][n] * imag[1][l]
            - real[0][l] * real[1][n]
            + imag[0][l] * imag[1][n]
        )
        rows_i.append(
            real[0][l] * imag[1][n]
            + imag[0][l] * real[1][n]
            - real[0][n] * imag[1][l]
            - imag[0][n] * real[1][l]
        )
    return rows_r, rows_i


PLANES = ((2, 3), (1, 3), (1, 2), (0, 1), (0, 2), (0, 3))
KINDS = ({0: 1}, {1: 1}, {2: 1}, {0: 1, 1: -1}, {0: 1, 2: -1}, {1: 1, 2: -1})
CORNERS = {(0, 1): (3, 1), (1, 0): (3, -1), (0, 2): (4, 1), (2, 0): (4, -1), (1, 2): (5, 1), (2, 1): (5, -1)}
FIXED = [(0, 1, 0), (0, 2, 0), (1, 0, -1), (1, 2, None), (2, 0, -1), (2, 1, None)]


def force_terms(
    counts, depth, halves, hbm, acc,
    u, ahead_s, local_s, fixed_s, st, sz, sy, rt, rz, ry, vts, vzs, vys, vtr, vzr, vyr,
    c01, c10, c02, c20, c12, c21, k01, k10, k02, k20, k12, k21,
    load_sem, send, recv, ready,
):
    g = Lattice(depth)
    last = halves - 1
    me = [lax.axis_index(a) for a in AXES]
    corner_out = {(0, 1): c01, (1, 0): c10, (0, 2): c02, (2, 0): c20, (1, 2): c12, (2, 1): c21}
    corner_in = {(0, 1): k01, (1, 0): k10, (0, 2): k02, (2, 0): k20, (1, 2): k12, (2, 1): k21}

    loads = [
        pltpu.make_async_copy(hbm.at[m, :, 0:2], u.at[m, :, 0:2], load_sem.at[m]) for m in range(4)
    ]
    last_rows = pltpu.make_async_copy(hbm.at[:, :, 2], u.at[:, :, 2], load_sem.at[4])
    for m in (0, 3, 1, 2):
        loads[m].start()
    last_rows.start()

    def peer(kind, sign):
        where = list(me)
        for i, step in KINDS[kind].items():
            where[i] = lax.rem(me[i] + counts[i] + sign * step, counts[i])
        by = dict(zip(AXES, where))
        return (by["gx"], by["gz"], by["ta"])

    def above(axis, sign):
        return me[axis] < counts[axis] - 1 if sign > 0 else me[axis] == 0

    def lowest(kind, sign):
        tests = [above(i, sign * step) for i, step in KINDS[kind].items()]
        return functools.reduce(jnp.logical_and, tests)

    def highest(kind, sign):
        tests = [above(i, sign * step) for i, step in KINDS[kind].items()]
        return jnp.logical_not(functools.reduce(jnp.logical_or, tests))

    barrier = pltpu.get_barrier_semaphore()
    pairs = [(kind, sign) for kind in range(6) for sign in (1, -1)]
    expected = 0
    for kind, sign in pairs:
        expected = expected + jnp.where(highest(kind, sign), 1, 0)

        @pl.when(lowest(kind, sign))
        def _():
            pl.semaphore_signal(
                barrier, inc=1, device_id=peer(kind, sign), device_id_type=pl.DeviceIdType.MESH
            )

    @pl.when(expected > 0)
    def _():
        pl.semaphore_wait(barrier, expected)

    for kind, sign in pairs:

        @pl.when(highest(kind, sign))
        def _():
            pl.semaphore_signal(
                ready.at[2 * kind + (sign > 0)], inc=1,
                device_id=peer(kind, sign), device_id_type=pl.DeviceIdType.MESH,
            )

    def early(kind, sign, copies):
        @pl.when(highest(kind, sign))
        def _():
            for copy in copies:
                copy.start()

    def late(kind, sign, copies):
        @pl.when(lowest(kind, sign))
        def _():
            pl.semaphore_wait(ready.at[2 * kind + (sign < 0)], 1)
            for copy in copies:
                copy.start()

    def load(m, part, i, j, h):
        return u[m, part, i, j, h * SUB : (h + 1) * SUB, :]

    COMPS = [(part, i, j) for part in range(2) for i in range(2) for j in range(3)]

    def comps(m):
        return [(m,) + c for c in COMPS]

    def all_comps(d):
        return [c for m in others(d) for c in comps(m)]

    def flat(value):
        return [value[part][i][j] for part, i, j in COMPS]

    def merge(values, index, step):
        total = None
        for k, x in enumerate(values):
            total = x if total is None else jnp.where(index >= step * k, x, total)
        return total

    def pack_t(m):
        cs, base = comps(m), 12 * others(0).index(m)
        for c0 in range(0, 12, g.per):
            r = (base + c0) // g.per * SUB
            st[r : r + SUB, :] = merge(
                [g.rows(load(*cs[c0 + k], 0), depth * k) for k in range(g.per)], g.row, depth
            )

    def pack_z(m):
        cs, base = comps(m), 12 * others(1).index(m)
        for c0 in range(0, 12, depth):
            for h in range(halves):
                r = ((base + c0) // depth * halves + h) * SUB
                sz[r : r + SUB, :] = merge(
                    [g.rows(load(*cs[c0 + k], h), k) for k in range(depth)], g.zrow, 1
                )

    def pack_y():
        cs = all_comps(2)
        for c0 in range(0, len(cs), g.ygroups):
            for h in range(halves):
                r = (c0 // g.ygroups * halves + h) * SUB
                sy[r : r + SUB, :] = merge(
                    [
                        g.lanes(load(*cs[c0 + k], h), NX * k)
                        for k in range(min(g.ygroups, len(cs) - c0))
                    ],
                    g.lane, NX,
                )

    def pack_vt(m, v):
        base = 12 * others(0).index(m)
        for c0 in range(0, 12, g.per):
            r = (base + c0) // g.per * SUB
            vts[r : r + SUB, :] = merge(
                [g.rows(v[c0 + k], depth * (k + 1)) for k in range(g.per)], g.row, depth
            )

    def pack_vz(m, h, v):
        base = 12 * others(1).index(m)
        for c0 in range(0, 12, depth):
            r = ((base + c0) // depth * halves + h) * SUB
            vzs[r : r + SUB, :] = merge(
                [g.rows(v[c0 + k], k + 1 - depth) for k in range(depth)], g.zrow, 1
            )

    def pack_vy(m, v):
        n = vys.shape[0] // 3
        for c0 in range(0, 12 * halves, g.ygroups):
            r = others(2).index(m) * n + c0 // g.ygroups * SUB
            vys[r : r + SUB, :] = merge(
                [
                    g.lanes(v[c0 + k], NX * (k + 1))
                    for k in range(min(g.ygroups, 12 * halves - c0))
                ],
                g.lane, NX,
            )

    def by_groups(d, h, up, shift, index, step):
        cs = comps(d)
        return merge(
            [
                merge(
                    [
                        g.lanes(g.rows(load(*cs[c], h), shift(c // g.ygroups)), NX * (c % g.ygroups + up))
                        for c in range(c0, min(12, c0 + g.ygroups))
                    ],
                    g.lane, NX,
                )
                for c0 in range(0, 12, g.ygroups)
            ],
            index, step,
        )

    def pack_corner(d, m):
        ref, cs = corner_out[d, m], comps(d)
        if (d, m) in ((0, 1), (1, 0)):
            source = SUB - depth if d == 0 else depth - 1
            for c0 in range(0, 12, SUB):
                ref[c0 : c0 + SUB, :] = merge(
                    [
                        g.rows(load(*cs[c0 + k], last if d == 0 else 0), k - source)
                        for k in range(min(SUB, 12 - c0))
                    ],
                    g.row, 1,
                )
        elif (d, m) == (0, 2):
            ref[...] = by_groups(0, last, 0, lambda k: depth * (k + 1), g.row, depth)
        elif (d, m) == (2, 0):
            ref[...] = by_groups(2, 0, 1, lambda k: depth * k, g.row, depth)
        else:
            for h in range(halves):
                up, source = (0, depth - 1) if d == 1 else (1, 0)
                ref[h * SUB : (h + 1) * SUB, :] = by_groups(
                    d, h, up, lambda k: k - source, g.zrow, 1
                )

    def corner(d, m, h, c):
        ref = corner_in[d, m]
        k, group = c // g.ygroups, NX * (c % g.ygroups)
        if (d, m) in ((0, 1), (1, 0)):
            target = depth - 1 if d == 0 else SUB - depth
            r = c // SUB * SUB
            return g.rows(ref[r : r + SUB, :], target - c % SUB)
        if (d, m) == (0, 2):
            return g.lanes(g.rows(ref[...], -depth * k), LANES - NX - group)
        if (d, m) == (2, 0):
            return g.lanes(g.rows(ref[...], SUB - depth - depth * k), -group)
        value = ref[h * SUB : (h + 1) * SUB, :]
        if d == 1:
            return g.lanes(g.rows(value, -k), LANES - NX - group)
        return g.lanes(g.rows(value, depth - 1 - k), -group)

    slots = {}

    def remote(src, dst, kind, sign):
        slot = len(slots)
        slots[slot] = pltpu.make_async_remote_copy(
            src_ref=src, dst_ref=dst, send_sem=send.at[slot], recv_sem=recv.at[slot],
            device_id=peer(kind, sign), device_id_type=pl.DeviceIdType.MESH,
        )
        return slots[slot]

    def chunk(ref, d, m):
        n = ref.shape[0] // 3
        k = others(d).index(m)
        return ref.at[k * n : (k + 1) * n]

    low = {
        (d, m): remote(chunk(s, d, m), chunk(r, d, m), d, -1)
        for d, s, r in ((0, st, rt), (1, sz, rz)) for m in others(d)
    }
    low[2, None] = remote(sy, ry, 2, -1)
    high = {
        (d, m): remote(chunk(s, d, m), chunk(r, d, m), d, 1)
        for d, s, r in ((0, vts, vtr), (1, vzs, vzr), (2, vys, vyr)) for m in others(d)
    }
    corners = {
        key: remote(corner_out[key], corner_in[key], kind, sign)
        for key, (kind, sign) in CORNERS.items()
    }

    def matrix(m, h):
        return [[[load(m, part, i, j, h) for j in range(3)] for i in range(3)] for part in range(2)]

    def save(ref, index, value):
        for part in range(2):
            for i in range(len(value[part])):
                for j in range(3):
                    ref[index, part, i, j] = value[part][i][j]

    def saved(ref, index, rows=3):
        return [[[ref[index, part, i, j] for j in range(3)] for i in range(rows)] for part in range(2)]

    def rolled(m, d, h, part, i, j):
        v = load(m, part, i, j, h)
        if d == 3:
            return jnp.where(g.xcol == NX - 1, g.lanes(v, NX - 1), g.lanes(v, -1))
        if d == 2:
            return g.lanes(v, -NX)
        if d == 1:
            return g.rows(v, -1)
        if h + 1 < halves:
            beyond = g.rows(load(m, part, i, j, h + 1), -depth)
            return jnp.where(g.row >= SUB - depth, beyond, g.rows(v, -depth))
        return g.rows(v, -depth)

    def complete(d, h):
        return d == 3 or (d == 0 and h + 1 < halves)

    def far_edge(d):
        return (g.row >= SUB - depth, g.zrow == depth - 1, g.lane >= LANES - NX)[d]

    ahead_slot = {}

    def prepare(m, d, h, rows):
        value = [
            [[rolled(m, d, h, part, i, j) for j in range(3)] for i in range(3 if rows == 3 or complete(d, h) else 2)]
            for part in range(2)
        ]
        ahead_slot[m, d, h] = len(ahead_slot)
        keep = 3 if complete(d, h) else 2
        save(ahead_s, ahead_slot[m, d, h], [part[:keep] for part in value])
        return value

    def transported(b, m, d, h, b_h):
        moved = prepare(m, d, h, 3)
        value = [
            [[entry(b, moved, i, j, part, b_h, False) for j in range(3)] for i in range(2)]
            for part in range(2)
        ]
        if not complete(d, h):
            edge = far_edge(d)
            for part in range(2):
                for i in range(2):
                    for j in range(3):
                        own = b[part][j][i] if b_h else b[part][i][j]
                        own = -own if b_h and part else own
                        value[part][i][j] = jnp.where(edge, own, value[part][i][j])
        return flat(value)

    local = {}

    def local_product(mu, nu, h):
        b = product(matrix(mu, h), matrix(nu, h), left_h=True)
        save(local_s, PLANES.index((mu, nu)) * halves + h, b)
        return b

    for copy in [loads[m] for m in (0, 3, 1, 2)] + [last_rows]:
        copy.wait()
    pack_corner(0, 1)
    pack_corner(0, 2)
    for m in (3, 1, 2):
        b = local_product(0, m, last)
        pack_vt(m, transported(b, 0, m, last, False))

    above_t, below_t = [high[0, m] for m in (3, 1, 2)], [low[0, m] for m in (3, 1, 2)]
    above_z, below_z = [high[1, m] for m in (3, 0, 2)], [low[1, m] for m in (3, 2, 0)]
    above_y, below_y = [high[2, m] for m in (3, 0, 1)], [low[2, None]]
    for d in (1, 2):
        early(*CORNERS[0, d], [corners[0, d]])
    early(0, 1, above_t)
    for m in (3, 1, 2):
        pack_t(m)
    early(0, -1, below_t)
    for m in (3, 2, 0):
        pack_z(m)
    early(1, -1, below_z)
    pack_y()
    early(2, -1, below_y)
    for key in ((1, 0), (2, 0), (1, 2), (2, 1)):
        pack_corner(*key)
    for key in ((1, 0), (2, 0), (1, 2), (2, 1)):
        early(*CORNERS[key], [corners[key]])

    lifted = {}

    def lift(mu, nu):
        for h in range(halves):
            if mu == 0 and h == last:
                b = saved(local_s, PLANES.index((mu, nu)) * halves + h)
            else:
                b = local_product(mu, nu, h)
            if mu:
                lifted[mu, nu, h] = transported(b, mu, nu, h, False)
            elif h != last:
                prepare(mu, nu, h, 2)
            if nu != 3:
                lifted[nu, mu, h] = transported(b, nu, mu, h, True)
            else:
                prepare(nu, mu, h, 2)
        for d, m in ((mu, nu), (nu, mu)):
            if d == 1:
                for h in range(halves):
                    pack_vz(m, h, lifted[d, m, h])
            elif d == 2:
                pack_vy(m, [x for h in range(halves) for x in lifted[d, m, h]])

    lift(1, 3)
    lift(0, 1)
    lift(1, 2)
    early(1, 1, above_z)
    late(1, -1, below_z)
    late(0, 1, above_t)
    late(2, -1, below_y)
    late(1, 1, above_z)
    lift(2, 3)
    lift(0, 2)
    early(2, 1, above_y)
    late(2, 1, above_y)
    lift(0, 3)
    for key in ((0, 1), (0, 2), (1, 2), (2, 1)):
        late(*CORNERS[key], [corners[key]])

        @pl.when(jnp.logical_not(jnp.logical_or(lowest(*CORNERS[key]), highest(*CORNERS[key]))))
        def _():
            corners[key].start()

    for key in ((1, 0), (2, 0)):

        @pl.when(jnp.logical_and(me[0] > 0, jnp.logical_not(highest(*CORNERS[key]))))
        def _():
            corners[key].start()

    def ahead(m, d, h):
        if complete(d, h):
            return saved(ahead_s, ahead_slot[m, d, h])
        index = {c: n for n, c in enumerate(all_comps(d))}

        def get(part, i, j):
            v = ahead_s[ahead_slot[m, d, h], part, i, j]
            c = index[(m, part, i, j)]
            if d == 0:
                r = c // g.per * SUB
                edge = g.rows(rt[r : r + SUB, :], SUB - depth - depth * (c % g.per))
            elif d == 1:
                r = (c // depth * halves + h) * SUB
                edge = g.rows(rz[r : r + SUB, :], depth - 1 - c % depth)
            else:
                r = (c // g.ygroups * halves + h) * SUB
                edge = g.lanes(ry[r : r + SUB, :], LANES - NX - NX * (c % g.ygroups))
            return jnp.where(far_edge(d), edge, v)

        return complete_rows(get)

    def complete_rows(get):
        real = [[get(0, i, j) for j in range(3)] for i in range(2)]
        imag = [[get(1, i, j) for j in range(3)] for i in range(2)]
        third_r, third_i = third_row(real, imag)
        return [real + [third_r], imag + [third_i]]

    seen = set()

    def add(m, c, h, value):
        r = ((m * 8 + c) * halves + h) * SUB
        if (m, c, h) in seen:
            acc[r : r + SUB, :] += value
        else:
            seen.add((m, c, h))
            acc[r : r + SUB, :] = value

    def shifted(q, d):
        if d == 3:
            return jnp.where(g.xcol == 0, g.lanes(q, 1 - NX), g.lanes(q, 1))
        if d == 2:
            return jnp.where(g.lane >= NX, g.lanes(q, NX), 0.0)
        if d == 1:
            return jnp.where(g.zrow > 0, g.rows(q, 1), 0.0)
        return jnp.where(g.row >= depth, g.rows(q, depth), 0.0)

    def plane(mu, nu, h):
        a = product(ahead(nu, mu, h), ahead(mu, nu, h), right_h=True)
        b = saved(local_s, PLANES.index((mu, nu)) * halves + h)
        e = product(matrix(mu, h), a)
        upper = projected(e, matrix(nu, h), right_h=True)
        q = projected(a, b, left_h=True)
        for c in range(8):
            add(mu, c, h, shifted(q[c], nu) + upper[c])
        q = projected(a, b, right_h=True)
        for c in range(8):
            add(nu, c, h, shifted(q[c], mu) - upper[c])
            if mu == 0 and h + 1 < halves:
                add(nu, c, h + 1, jnp.where(g.row < depth, g.rows(q[c], depth), 0.0))

    fixed_slot = {}

    def fix(d, m, h):
        beyond = complete_rows(lambda part, i, j: corner(d, m, h, part * 6 + i * 3 + j))
        own = matrix(m, h)
        moved = product(own, beyond, right_h=True)
        edge = far_edge(m)
        fixed_slot[d, m, h] = len(fixed_slot)
        save(
            fixed_s, fixed_slot[d, m, h],
            [[[jnp.where(edge, moved[p][i][j], own[p][i][j]) for j in range(3)] for i in range(3)] for p in range(2)],
        )

    def lower(d, m, h):
        def get(part, i, j):
            c = part * 6 + i * 3 + j
            base = 12 * others(d).index(m) + c
            if d == 0:
                r = base // g.per * SUB
                return g.rows(vtr[r : r + SUB, :], -depth * (base % g.per))
            if d == 1:
                r = (base // depth * halves + h) * SUB
                return g.rows(vzr[r : r + SUB, :], -(base % depth))
            n, k = vyr.shape[0] // 3, h * 12 + c
            r = others(2).index(m) * n + k // g.ygroups * SUB
            return g.lanes(vyr[r : r + SUB, :], -NX * (k % g.ygroups))

        if (d, m, h) in fixed_slot:
            left = saved(fixed_s, fixed_slot[d, m, h])
        else:
            left = matrix(m, h)
        q = projected(left, complete_rows(get), right_h=True)
        near = (g.row < depth, g.zrow == 0, g.lane < NX)[d]
        for c in range(8):
            add(m, c, h, jnp.where(near, q[c], 0.0))

    for h in range(last):
        plane(0, 3, h)
    low[2, None].wait_recv()
    for h in range(halves):
        plane(2, 3, h)
    for h in range(last):
        plane(0, 2, h)
    late(0, -1, below_t)
    for key in ((1, 0), (2, 0)):
        late(*CORNERS[key], [corners[key]])

        @pl.when(jnp.logical_and(me[0] == 0, jnp.logical_not(lowest(*CORNERS[key]))))
        def _():
            corners[key].start()

    low[1, 3].wait_recv()
    for h in range(halves):
        plane(1, 3, h)
    low[1, 2].wait_recv()
    for h in range(halves):
        plane(1, 2, h)
    low[1, 0].wait_recv()
    for h in range(last):
        plane(0, 1, h)

    for d, m in ((2, 3), (2, 1), (2, 0), (1, 3), (1, 2), (1, 0)):
        if (d, m) in ((2, 1), (1, 2)):
            corners[d, m].wait_recv()
            for h in range(halves):
                fix(d, m, h)
        high[d, m].wait_recv()
        for h in range(halves if m else last):
            lower(d, m, h)
    for m in (3, 1, 2):
        low[0, m].wait_recv()
        plane(0, m, last)
    for d in (1, 2):
        corners[d, 0].wait_recv()
        fix(d, 0, last)
        lower(d, 0, last)
    for m in (1, 2):
        corners[0, m].wait_recv()
        fix(0, m, 0)
    for m in (3, 1, 2):
        high[0, m].wait_recv()
        lower(0, m, 0)
    for copy in slots.values():
        copy.wait_send()


def expand(halves, acc, hbm, out, sems):
    copies = []
    for m in range(4):
        for h in range(halves):
            rows = [((m * 8 + c) * halves + h) * SUB for c in range(8)]
            f = [acc[r : r + SUB, :] * (COEFF * 0.5 if c < 6 else COEFF) for c, r in enumerate(rows)]

            def put(part, i, j, value):
                out[m, part, i, j, h * SUB : (h + 1) * SUB, :] = value

            for n, (i, j) in enumerate(((0, 1), (0, 2), (1, 2))):
                put(0, i, j, f[n])
                put(0, j, i, -f[n])
                put(1, i, j, f[3 + n])
                put(1, j, i, f[3 + n])
            for i in range(3):
                put(0, i, i, jnp.zeros((SUB, LANES), jnp.float32))
            put(1, 0, 0, f[6])
            put(1, 1, 1, f[7])
            put(1, 2, 2, -(f[6] + f[7]))
        copies.append(pltpu.make_async_copy(out.at[m], hbm.at[m], sems.at[m]))
        copies[-1].start()
    for copy in copies:
        copy.wait()


def per_device(counts, links):
    time_len, depth, flat = links.shape[4:]
    sites = time_len * depth
    assert flat == LANES and SUB % depth == 0 and sites % SUB == 0 and 2 <= depth <= SUB // 2
    halves = sites // SUB
    per, yg = SUB // depth, LANES // NX
    up = lambda a, b: -(-a // b) * SUB
    vmem = lambda *s: pltpu.VMEM(s + (LANES,), jnp.float32)
    shape = links.shape[:4] + (sites, flat)
    rt, rz, ry = up(36, per), up(36, depth) * halves, up(36, yg) * halves
    vy = 3 * up(12 * halves, yg)
    corner = [vmem(r) for r in (2 * SUB, 2 * SUB, SUB, SUB, SUB * halves, SUB * halves)]
    terms = pl.pallas_call(
        functools.partial(force_terms, counts, depth, halves),
        out_shape=pltpu.VMEM((32 * sites, flat), jnp.float32),
        in_specs=[pl.BlockSpec(memory_space=pl.ANY)],
        out_specs=pl.BlockSpec(memory_space=pltpu.VMEM),
        scratch_shapes=[
            vmem(*shape[:-1]),
            vmem(12 * halves, 2, 3, 3, SUB),
            vmem(6 * halves, 2, 3, 3, SUB),
            vmem(4 + 2 * halves, 2, 3, 3, SUB),
        ]
        + [vmem(r) for r in (rt, rz, ry) * 2 + (rt, rz, vy) * 2]
        + corner * 2
        + [
            pltpu.SemaphoreType.DMA((5,)),
            pltpu.SemaphoreType.DMA((22,)),
            pltpu.SemaphoreType.DMA((22,)),
            pltpu.SemaphoreType.REGULAR((12,)),
        ],
        compiler_params=pltpu.CompilerParams(collective_id=0, has_side_effects=True),
        name="force_terms",
    )(links.reshape(shape))
    out = pl.pallas_call(
        functools.partial(expand, halves),
        out_shape=jax.ShapeDtypeStruct(shape, jnp.float32),
        in_specs=[pl.BlockSpec(memory_space=pltpu.VMEM)],
        out_specs=pl.BlockSpec(memory_space=pl.ANY),
        scratch_shapes=[vmem(*shape[:-1]), pltpu.SemaphoreType.DMA((4,))],
        name="expand",
    )(pltpu.with_memory_space_constraint(terms, pltpu.VMEM))
    return out.reshape(links.shape)


def solution(mesh):
    assert mesh.axis_names == ("gx", "gz", "ta")
    counts = tuple(mesh.shape[a] for a in AXES)
    spec = P(None, None, None, None, "ta", "gz", "gx")
    return jax.shard_map(
        functools.partial(per_device, counts),
        mesh=mesh,
        in_specs=(spec,),
        out_specs=spec,
        check_vma=False,
    )
```

```python
import functools

import jax
import jax.numpy as jnp
from jax import lax
from jax.experimental import pallas as pl
from jax.experimental.pallas import tpu as pltpu
from jax.sharding import PartitionSpec as P

NX = 16
COEFF = -1.9
AXES = ("ta", "gz", "gx")
SUB, LANES = 8, 128


def others(d):
    return [m for m in range(4) if m != d]


class Lattice:
    def __init__(self, depth):
        self.depth = depth
        self.per = SUB // depth
        self.ygroups = LANES // NX
        self.row = lax.broadcasted_iota(jnp.int32, (SUB, LANES), 0)
        self.lane = lax.broadcasted_iota(jnp.int32, (SUB, LANES), 1)
        self.zrow = self.row % depth
        self.xcol = self.lane % NX

    def rows(self, value, shift):
        shift %= SUB
        return pltpu.roll(value, shift, 0) if shift else value

    def lanes(self, value, shift):
        shift %= LANES
        return pltpu.roll(value, shift, 1) if shift else value


def entry(left, right, i, j, part, left_h, right_h):
    total = None
    for k in range(3):
        li = (k, i) if left_h else (i, k)
        ri = (j, k) if right_h else (k, j)
        lr, lm = left[0][li[0]][li[1]], left[1][li[0]][li[1]]
        rr, rm = right[0][ri[0]][ri[1]], right[1][ri[0]][ri[1]]
        if part == 0:
            first, second = lr * rr, lm * rm
            minus = left_h == right_h
        elif left_h:
            first, second = lr * rm, lm * rr
            minus = True
        else:
            first, second = lm * rr, lr * rm
            minus = right_h
        value = first - second if minus else first + second
        total = value if total is None else total + value
    return total


def product(left, right, left_h=False, right_h=False):
    return [
        [[entry(left, right, i, j, part, left_h, right_h) for j in range(3)] for i in range(3)]
        for part in range(2)
    ]


def projected(left, right, left_h=False, right_h=False):
    get = lambda i, j, part: entry(left, right, i, j, part, left_h, right_h)
    pairs = ((0, 1), (0, 2), (1, 2))
    real = [get(i, j, 0) - get(j, i, 0) for i, j in pairs]
    imag = [get(i, j, 1) + get(j, i, 1) for i, j in pairs]
    diag = [get(i, i, 1) for i in range(3)]
    third = (diag[0] + diag[1] + diag[2]) * (1.0 / 3.0)
    return real + imag + [diag[0] - third, diag[1] - third]


def third_row(real, imag):
    rows_r, rows_i = [], []
    for column in range(3):
        n, l = (column + 1) % 3, (column + 2) % 3
        rows_r.append(
            real[0][n] * real[1][l]
            - imag[0][n] * imag[1][l]
            - real[0][l] * real[1][n]
            + imag[0][l] * imag[1][n]
        )
        rows_i.append(
            real[0][l] * imag[1][n]
            + imag[0][l] * real[1][n]
            - real[0][n] * imag[1][l]
            - imag[0][n] * real[1][l]
        )
    return rows_r, rows_i


PLANES = ((2, 3), (1, 3), (1, 2), (0, 1), (0, 2), (0, 3))
KINDS = ({0: 1}, {1: 1}, {2: 1}, {0: 1, 1: -1}, {0: 1, 2: -1}, {1: 1, 2: -1})
CORNERS = {(0, 1): (3, 1), (1, 0): (3, -1), (0, 2): (4, 1), (2, 0): (4, -1), (1, 2): (5, 1), (2, 1): (5, -1)}
FIXED = [(0, 1, 0), (0, 2, 0), (1, 0, -1), (1, 2, None), (2, 0, -1), (2, 1, None)]


def mail(depth, halves):
    up = lambda a, b: -(-a // b) * SUB
    per, yg = SUB // depth, LANES // NX
    t, z, y = up(12, per), up(12, depth) * halves, up(36, yg) * halves
    groups = (
        ((("low", 2), y),),
        ((("low", 1, 3), z),),
        ((("low", 1, 0), z),),
        ((("low", 1, 2), z),),
        ((("high", 2), 3 * up(12 * halves, yg)), ((2, 1), SUB * halves)),
        ((("high", 1, 3), z), (("high", 1, 0), z)),
        ((("high", 1, 2), z), ((1, 2), SUB * halves)),
        ((("low", 0, 3), t),),
        ((("low", 0, 1), t), (("low", 0, 2), t)),
        (((1, 0), 2 * SUB), ((2, 0), SUB)),
        ((("high", 0, 3), t), ((0, 1), 2 * SUB), ((0, 2), SUB)),
        ((("high", 0, 1), t),),
        ((("high", 0, 2), t),),
    )
    places, spans, row = {}, [], 0
    for group in groups:
        first = row
        for name, rows in group:
            places[name] = (row, rows, len(spans))
            row += rows
        spans.append((first, row))
    return places, spans


def force_terms(
    counts, depth, halves, hbm, acc,
    u, ahead_s, local_s, fixed_s, outbox, inbox, load_sem, send, recv, ready,
):
    g = Lattice(depth)
    last = halves - 1
    me = [lax.axis_index(a) for a in AXES]
    places, spans = mail(depth, halves)

    upper_rows = pltpu.make_async_copy(hbm.at[:, :, 0:2], u.at[:, :, 0:2], load_sem.at[0])
    last_rows = pltpu.make_async_copy(hbm.at[:, :, 2], u.at[:, :, 2], load_sem.at[1])
    upper_rows.start()
    last_rows.start()

    def peer(kind, sign):
        where = list(me)
        for i, step in KINDS[kind].items():
            where[i] = lax.rem(me[i] + counts[i] + sign * step, counts[i])
        by = dict(zip(AXES, where))
        return (by["gx"], by["gz"], by["ta"])

    def above(axis, sign):
        return me[axis] < counts[axis] - 1 if sign > 0 else me[axis] == 0

    def lowest(kind, sign):
        tests = [above(i, sign * step) for i, step in KINDS[kind].items()]
        return functools.reduce(jnp.logical_and, tests)

    def highest(kind, sign):
        tests = [above(i, sign * step) for i, step in KINDS[kind].items()]
        return jnp.logical_not(functools.reduce(jnp.logical_or, tests))

    barrier = pltpu.get_barrier_semaphore()
    pairs = [(kind, sign) for kind in range(6) for sign in (1, -1)]
    expected = 0
    for kind, sign in pairs:
        expected = expected + jnp.where(highest(kind, sign), 1, 0)

        @pl.when(lowest(kind, sign))
        def _():
            pl.semaphore_signal(
                barrier, inc=1, device_id=peer(kind, sign), device_id_type=pl.DeviceIdType.MESH
            )

    @pl.when(expected > 0)
    def _():
        pl.semaphore_wait(barrier, expected)

    def answer_group(kind, sign):
        if kind < 3:
            return 2 if (kind, sign) == (0, -1) else 0
        return 3 if kind < 5 and sign < 0 else 1

    for kind, sign in pairs:

        @pl.when(highest(kind, sign))
        def _():
            pl.semaphore_signal(
                ready.at[answer_group(kind, -sign)], inc=1,
                device_id=peer(kind, sign), device_id_type=pl.DeviceIdType.MESH,
            )

    def answers(group):
        count = 0
        for kind, sign in pairs:
            if answer_group(kind, sign) == group:
                count = count + jnp.where(lowest(kind, sign), 1, 0)

        @pl.when(count > 0)
        def _():
            pl.semaphore_wait(ready.at[group], count)

    def start(copies):
        for copy in copies:
            copy.start()

    def early(kind, sign, copies):
        pl.when(highest(kind, sign))(lambda: start(copies))

    def late(kind, sign, copies):
        pl.when(lowest(kind, sign))(lambda: start(copies))

    def middle(kind, sign, copies):
        between = jnp.logical_not(jnp.logical_or(lowest(kind, sign), highest(kind, sign)))
        pl.when(between)(lambda: start(copies))

    def put(name, r, value):
        row = places[name][0] + r
        outbox[row : row + SUB, :] = value

    def got(name, r):
        row = places[name][0] + r
        return inbox[row : row + SUB, :]

    def load(m, part, i, j, h):
        return u[m, part, i, j, h * SUB : (h + 1) * SUB, :]

    COMPS = [(part, i, j) for part in range(2) for i in range(2) for j in range(3)]

    def comps(m):
        return [(m,) + c for c in COMPS]

    def all_comps(d):
        return [c for m in others(d) for c in comps(m)]

    def flat(value):
        return [value[part][i][j] for part, i, j in COMPS]

    def merge(values, index, step):
        total = None
        for k, x in enumerate(values):
            total = x if total is None else jnp.where(index >= step * k, x, total)
        return total

    def pack_t(m):
        cs = comps(m)
        for c0 in range(0, 12, g.per):
            put(
                ("low", 0, m), c0 // g.per * SUB,
                merge([g.rows(load(*cs[c0 + k], 0), depth * k) for k in range(g.per)], g.row, depth),
            )

    def pack_z(m):
        cs = comps(m)
        for c0 in range(0, 12, depth):
            for h in range(halves):
                put(
                    ("low", 1, m), (c0 // depth * halves + h) * SUB,
                    merge([g.rows(load(*cs[c0 + k], h), k) for k in range(depth)], g.zrow, 1),
                )

    def pack_y():
        cs = all_comps(2)
        for c0 in range(0, len(cs), g.ygroups):
            for h in range(halves):
                ks = range(min(g.ygroups, len(cs) - c0))
                put(
                    ("low", 2), (c0 // g.ygroups * halves + h) * SUB,
                    merge([g.lanes(load(*cs[c0 + k], h), NX * k) for k in ks], g.lane, NX),
                )

    def pack_vt(m, v):
        for c0 in range(0, 12, g.per):
            put(
                ("high", 0, m), c0 // g.per * SUB,
                merge([g.rows(v[c0 + k], depth * (k + 1)) for k in range(g.per)], g.row, depth),
            )

    def pack_vz(m, h, v):
        for c0 in range(0, 12, depth):
            put(
                ("high", 1, m), (c0 // depth * halves + h) * SUB,
                merge([g.rows(v[c0 + k], k + 1 - depth) for k in range(depth)], g.zrow, 1),
            )

    def pack_vy(m, v):
        n = places["high", 2][1] // 3
        for c0 in range(0, 12 * halves, g.ygroups):
            ks = range(min(g.ygroups, 12 * halves - c0))
            put(
                ("high", 2), others(2).index(m) * n + c0 // g.ygroups * SUB,
                merge([g.lanes(v[c0 + k], NX * (k + 1)) for k in ks], g.lane, NX),
            )

    def by_groups(d, h, up, shift, index, step):
        cs = comps(d)
        return merge(
            [
                merge(
                    [
                        g.lanes(g.rows(load(*cs[c], h), shift(c // g.ygroups)), NX * (c % g.ygroups + up))
                        for c in range(c0, min(12, c0 + g.ygroups))
                    ],
                    g.lane, NX,
                )
                for c0 in range(0, 12, g.ygroups)
            ],
            index, step,
        )

    def pack_corner(d, m):
        cs = comps(d)
        if (d, m) in ((0, 1), (1, 0)):
            source = SUB - depth if d == 0 else depth - 1
            for c0 in range(0, 12, SUB):
                ks = range(min(SUB, 12 - c0))
                values = [g.rows(load(*cs[c0 + k], last if d == 0 else 0), k - source) for k in ks]
                put((d, m), c0, merge(values, g.row, 1))
        elif (d, m) == (0, 2):
            put((d, m), 0, by_groups(0, last, 0, lambda k: depth * (k + 1), g.row, depth))
        elif (d, m) == (2, 0):
            put((d, m), 0, by_groups(2, 0, 1, lambda k: depth * k, g.row, depth))
        else:
            for h in range(halves):
                up, source = (0, depth - 1) if d == 1 else (1, 0)
                put((d, m), h * SUB, by_groups(d, h, up, lambda k: k - source, g.zrow, 1))

    def corner(d, m, h, c):
        k, group = c // g.ygroups, NX * (c % g.ygroups)
        if (d, m) in ((0, 1), (1, 0)):
            target = depth - 1 if d == 0 else SUB - depth
            return g.rows(got((d, m), c // SUB * SUB), target - c % SUB)
        if (d, m) == (0, 2):
            return g.lanes(g.rows(got((d, m), 0), -depth * k), LANES - NX - group)
        if (d, m) == (2, 0):
            return g.lanes(g.rows(got((d, m), 0), SUB - depth - depth * k), -group)
        if d == 1:
            return g.lanes(g.rows(got((d, m), h * SUB), -k), LANES - NX - group)
        return g.lanes(g.rows(got((d, m), h * SUB), depth - 1 - k), -group)

    def remote(first, end, group, kind, sign):
        return pltpu.make_async_remote_copy(
            src_ref=outbox.at[first:end], dst_ref=inbox.at[first:end],
            send_sem=send.at[0], recv_sem=recv.at[group],
            device_id=peer(kind, sign), device_id_type=pl.DeviceIdType.MESH,
        )

    def message(name, kind, sign):
        first, rows, group = places[name]
        return remote(first, first + rows, group, kind, sign)

    def arrived(name):
        group = places[name][2]
        remote(*spans[group], group, 0, 1).wait_recv()

    low = {(d, m): message(("low", d, m), d, -1) for d in (0, 1) for m in others(d)}
    high = {(d, m): message(("high", d, m), d, 1) for d in (0, 1) for m in others(d)}
    low_y, high_y = message(("low", 2), 2, -1), message(("high", 2), 2, 1)
    corners = {key: message(key, kind, sign) for key, (kind, sign) in CORNERS.items()}

    def matrix(m, h):
        return [[[load(m, part, i, j, h) for j in range(3)] for i in range(3)] for part in range(2)]

    def save(ref, index, value):
        for part in range(2):
            for i in range(len(value[part])):
                for j in range(3):
                    ref[index, part, i, j] = value[part][i][j]

    def saved(ref, index, rows=3):
        return [[[ref[index, part, i, j] for j in range(3)] for i in range(rows)] for part in range(2)]

    def rolled(m, d, h, part, i, j):
        v = load(m, part, i, j, h)
        if d == 3:
            return jnp.where(g.xcol == NX - 1, g.lanes(v, NX - 1), g.lanes(v, -1))
        if d == 2:
            return g.lanes(v, -NX)
        if d == 1:
            return g.rows(v, -1)
        if h + 1 < halves:
            beyond = g.rows(load(m, part, i, j, h + 1), -depth)
            return jnp.where(g.row >= SUB - depth, beyond, g.rows(v, -depth))
        return g.rows(v, -depth)

    def complete(d, h):
        return d == 3 or (d == 0 and h + 1 < halves)

    def far_edge(d):
        return (g.row >= SUB - depth, g.zrow == depth - 1, g.lane >= LANES - NX)[d]

    ahead_slot = {}

    def prepare(m, d, h, rows):
        value = [
            [[rolled(m, d, h, part, i, j) for j in range(3)] for i in range(3 if rows == 3 or complete(d, h) else 2)]
            for part in range(2)
        ]
        ahead_slot[m, d, h] = len(ahead_slot)
        keep = 3 if complete(d, h) else 2
        save(ahead_s, ahead_slot[m, d, h], [part[:keep] for part in value])
        return value

    def transported(b, m, d, h, b_h):
        moved = prepare(m, d, h, 3)
        value = [
            [[entry(b, moved, i, j, part, b_h, False) for j in range(3)] for i in range(2)]
            for part in range(2)
        ]
        if not complete(d, h):
            edge = far_edge(d)
            for part in range(2):
                for i in range(2):
                    for j in range(3):
                        own = b[part][j][i] if b_h else b[part][i][j]
                        own = -own if b_h and part else own
                        value[part][i][j] = jnp.where(edge, own, value[part][i][j])
        return flat(value)

    local = {}

    def local_product(mu, nu, h):
        b = product(matrix(mu, h), matrix(nu, h), left_h=True)
        save(local_s, PLANES.index((mu, nu)) * halves + h, b)
        return b

    acc[...] = jnp.zeros_like(acc)
    upper_rows.wait()
    pack_corner(0, 1)
    pack_corner(0, 2)
    last_rows.wait()
    for m in (3, 1, 2):
        b = local_product(0, m, last)
        pack_vt(m, transported(b, 0, m, last, False))
    above_t, below_t = [high[0, m] for m in (3, 1, 2)], [low[0, m] for m in (3, 1, 2)]
    below_z = [low[1, m] for m in (3, 0, 2)]
    for d in (1, 2):
        early(*CORNERS[0, d], [corners[0, d]])
    early(0, 1, above_t)
    for m in (3, 1, 2):
        pack_t(m)
    early(0, -1, below_t)
    for m in (3, 0, 2):
        pack_z(m)
    early(1, -1, below_z)
    pack_y()
    early(2, -1, [low_y])
    for key in ((1, 0), (2, 0), (1, 2), (2, 1)):
        pack_corner(*key)
    for key in ((1, 0), (2, 0), (1, 2), (2, 1)):
        early(*CORNERS[key], [corners[key]])
    answers(0)
    late(2, -1, [low_y])
    late(1, -1, below_z)
    for key in ((1, 2), (2, 1), (0, 1), (0, 2)):
        middle(*CORNERS[key], [corners[key]])
    late(0, 1, above_t)
    for key in ((1, 0), (2, 0)):
        between = jnp.logical_and(me[0] > 0, jnp.logical_not(highest(*CORNERS[key])))
        pl.when(between)(corners[key].start)

    lifted = {}

    def lift(mu, nu):
        for h in range(halves):
            if mu == 0 and h == last:
                b = saved(local_s, PLANES.index((mu, nu)) * halves + h)
            else:
                b = local_product(mu, nu, h)
            if mu:
                lifted[mu, nu, h] = transported(b, mu, nu, h, False)
            elif h != last:
                prepare(mu, nu, h, 2)
            if nu != 3:
                lifted[nu, mu, h] = transported(b, nu, mu, h, True)
            else:
                prepare(nu, mu, h, 2)
        for d, m in ((mu, nu), (nu, mu)):
            if d == 1:
                for h in range(halves):
                    pack_vz(m, h, lifted[d, m, h])
            elif d == 2:
                pack_vy(m, [x for h in range(halves) for x in lifted[d, m, h]])

    lift(1, 3)
    high[1, 3].start()
    lift(0, 1)
    high[1, 0].start()
    lift(1, 2)
    high[1, 2].start()
    lift(2, 3)
    lift(0, 2)
    high_y.start()
    lift(0, 3)
    answers(1)
    for key in ((0, 1), (0, 2), (1, 2), (2, 1)):
        late(*CORNERS[key], [corners[key]])

    def ahead(m, d, h):
        if complete(d, h):
            return saved(ahead_s, ahead_slot[m, d, h])
        index = {c: n for n, c in enumerate(all_comps(d))}

        def get(part, i, j):
            v = ahead_s[ahead_slot[m, d, h], part, i, j]
            c = index[(m, part, i, j)]
            k = c % 12
            if d == 0:
                edge = g.rows(got(("low", 0, m), k // g.per * SUB), SUB - depth - depth * (k % g.per))
            elif d == 1:
                edge = g.rows(got(("low", 1, m), (k // depth * halves + h) * SUB), depth - 1 - k % depth)
            else:
                edge = g.lanes(
                    got(("low", 2), (c // g.ygroups * halves + h) * SUB), LANES - NX - NX * (c % g.ygroups)
                )
            return jnp.where(far_edge(d), edge, v)

        return complete_rows(get)

    def complete_rows(get):
        real = [[get(0, i, j) for j in range(3)] for i in range(2)]
        imag = [[get(1, i, j) for j in range(3)] for i in range(2)]
        third_r, third_i = third_row(real, imag)
        return [real + [third_r], imag + [third_i]]

    def add(m, c, h, value):
        r = ((m * 8 + c) * halves + h) * SUB
        acc[r : r + SUB, :] += value

    def shifted(q, d):
        if d == 3:
            return jnp.where(g.xcol == 0, g.lanes(q, 1 - NX), g.lanes(q, 1))
        if d == 2:
            return jnp.where(g.lane >= NX, g.lanes(q, NX), 0.0)
        if d == 1:
            return jnp.where(g.zrow > 0, g.rows(q, 1), 0.0)
        return jnp.where(g.row >= depth, g.rows(q, depth), 0.0)

    def plane(mu, nu, h):
        a = product(ahead(nu, mu, h), ahead(mu, nu, h), right_h=True)
        b = saved(local_s, PLANES.index((mu, nu)) * halves + h)
        e = product(matrix(mu, h), a)
        upper = projected(e, matrix(nu, h), right_h=True)
        q = projected(a, b, left_h=True)
        for c in range(8):
            add(mu, c, h, shifted(q[c], nu) + upper[c])
        q = projected(a, b, right_h=True)
        for c in range(8):
            add(nu, c, h, shifted(q[c], mu) - upper[c])
            if mu == 0 and h + 1 < halves:
                add(nu, c, h + 1, jnp.where(g.row < depth, g.rows(q[c], depth), 0.0))

    fixed_slot = {}

    def fix(d, m, h):
        beyond = complete_rows(lambda part, i, j: corner(d, m, h, part * 6 + i * 3 + j))
        own = matrix(m, h)
        moved = product(own, beyond, right_h=True)
        edge = far_edge(m)
        fixed_slot[d, m, h] = len(fixed_slot)
        save(
            fixed_s, fixed_slot[d, m, h],
            [[[jnp.where(edge, moved[p][i][j], own[p][i][j]) for j in range(3)] for i in range(3)] for p in range(2)],
        )

    def lower(d, m, h):
        def get(part, i, j):
            c = part * 6 + i * 3 + j
            if d == 0:
                return g.rows(got(("high", 0, m), c // g.per * SUB), -depth * (c % g.per))
            if d == 1:
                return g.rows(got(("high", 1, m), (c // depth * halves + h) * SUB), -(c % depth))
            n, k = places["high", 2][1] // 3, h * 12 + c
            r = others(2).index(m) * n + k // g.ygroups * SUB
            return g.lanes(got(("high", 2), r), -NX * (k % g.ygroups))

        if (d, m, h) in fixed_slot:
            left = saved(fixed_s, fixed_slot[d, m, h])
        else:
            left = matrix(m, h)
        q = projected(left, complete_rows(get), right_h=True)
        near = (g.row < depth, g.zrow == 0, g.lane < NX)[d]
        for c in range(8):
            add(m, c, h, jnp.where(near, q[c], 0.0))

    def y_part():
        arrived(("low", 2))
        for h in range(halves):
            plane(2, 3, h)
        for h in range(last):
            plane(0, 2, h)

    def z_part():
        arrived(("low", 1, 3))
        for h in range(halves):
            plane(1, 3, h)
        arrived(("low", 1, 0))
        for h in range(last):
            plane(0, 1, h)

    def around_part():
        answers(2)
        late(0, -1, below_t)

    for h in range(last):
        plane(0, 3, h)
    even = lax.rem(me[2], 2) == 0

    @pl.when(even)
    def _():
        y_part()
        around_part()
        z_part()

    @pl.when(jnp.logical_not(even))
    def _():
        around_part()
        z_part()
        y_part()

    answers(3)
    for key in ((1, 0), (2, 0)):
        first = jnp.logical_and(me[0] == 0, jnp.logical_not(highest(*CORNERS[key])))
        pl.when(first)(corners[key].start)

    arrived(("low", 1, 2))
    for h in range(halves):
        plane(1, 2, h)
    arrived(("high", 2))
    for h in range(halves):
        fix(2, 1, h)
    for m in (3, 1, 0):
        for h in range(halves if m else last):
            lower(2, m, h)
    arrived(("low", 0, 3))
    plane(0, 3, last)
    arrived(("low", 0, 1))
    plane(0, 1, last)
    plane(0, 2, last)
    arrived(("high", 1, 3))
    for m in (3, 0):
        for h in range(halves if m else last):
            lower(1, m, h)
    arrived(("high", 1, 2))
    for h in range(halves):
        fix(1, 2, h)
        lower(1, 2, h)
    arrived((1, 0))
    for d in (1, 2):
        fix(d, 0, last)
        lower(d, 0, last)
    arrived(("high", 0, 3))
    for m in (1, 2):
        fix(0, m, 0)
    lower(0, 3, 0)
    arrived(("high", 0, 1))
    lower(0, 1, 0)
    arrived(("high", 0, 2))
    lower(0, 2, 0)
    remote(0, spans[-1][1], 0, 0, 1).wait_send()


def expand(halves, acc, hbm, out, sems):
    copies = []
    for m in range(4):
        for h in range(halves):
            rows = [((m * 8 + c) * halves + h) * SUB for c in range(8)]
            f = [acc[r : r + SUB, :] * (COEFF * 0.5 if c < 6 else COEFF) for c, r in enumerate(rows)]

            def put(part, i, j, value):
                out[m, part, i, j, h * SUB : (h + 1) * SUB, :] = value

            for n, (i, j) in enumerate(((0, 1), (0, 2), (1, 2))):
                put(0, i, j, f[n])
                put(0, j, i, -f[n])
                put(1, i, j, f[3 + n])
                put(1, j, i, f[3 + n])
            for i in range(3):
                put(0, i, i, jnp.zeros((SUB, LANES), jnp.float32))
            put(1, 0, 0, f[6])
            put(1, 1, 1, f[7])
            put(1, 2, 2, -(f[6] + f[7]))
        copies.append(pltpu.make_async_copy(out.at[m], hbm.at[m], sems.at[m]))
        copies[-1].start()
    for copy in copies:
        copy.wait()


def per_device(counts, links):
    time_len, depth, flat = links.shape[4:]
    sites = time_len * depth
    assert flat == LANES and SUB % depth == 0 and sites % SUB == 0 and 2 <= depth <= SUB // 2
    halves = sites // SUB
    spans = mail(depth, halves)[1]
    vmem = lambda *s: pltpu.VMEM(s + (LANES,), jnp.float32)
    shape = links.shape[:4] + (sites, flat)
    terms = pl.pallas_call(
        functools.partial(force_terms, counts, depth, halves),
        out_shape=pltpu.VMEM((32 * sites, flat), jnp.float32),
        in_specs=[pl.BlockSpec(memory_space=pl.ANY)],
        out_specs=pl.BlockSpec(memory_space=pltpu.VMEM),
        scratch_shapes=[
            vmem(*shape[:-1]),
            vmem(12 * halves, 2, 3, 3, SUB),
            vmem(6 * halves, 2, 3, 3, SUB),
            vmem(4 + 2 * halves, 2, 3, 3, SUB),
            vmem(spans[-1][1]),
            vmem(spans[-1][1]),
            pltpu.SemaphoreType.DMA((2,)),
            pltpu.SemaphoreType.DMA((1,)),
            pltpu.SemaphoreType.DMA((len(spans),)),
            pltpu.SemaphoreType.REGULAR((4,)),
        ],
        compiler_params=pltpu.CompilerParams(collective_id=0, has_side_effects=True),
        name="force_terms",
    )(links.reshape(shape))
    out = pl.pallas_call(
        functools.partial(expand, halves),
        out_shape=jax.ShapeDtypeStruct(shape, jnp.float32),
        in_specs=[pl.BlockSpec(memory_space=pltpu.VMEM)],
        out_specs=pl.BlockSpec(memory_space=pl.ANY),
        scratch_shapes=[vmem(*shape[:-1]), pltpu.SemaphoreType.DMA((4,))],
        name="expand",
    )(pltpu.with_memory_space_constraint(terms, pltpu.VMEM))
    return out.reshape(links.shape)


def solution(mesh):
    assert mesh.axis_names == ("gx", "gz", "ta")
    counts = tuple(mesh.shape[a] for a in AXES)
    spec = P(None, None, None, None, "ta", "gz", "gx")
    return jax.shard_map(
        functools.partial(per_device, counts),
        mesh=mesh,
        in_specs=(spec,),
        out_specs=spec,
        check_vma=False,
    )
```

```python
import functools

import jax
import jax.numpy as jnp
from jax import lax
from jax.experimental import pallas as pl
from jax.experimental.pallas import tpu as pltpu
from jax.sharding import PartitionSpec as P

NX = 16
COEFF = -1.9
AXES = ("ta", "gz", "gx")
SUB, LANES = 8, 128


def others(d):
    return [m for m in range(4) if m != d]


class Lattice:
    def __init__(self, depth):
        self.depth = depth
        self.per = SUB // depth
        self.ygroups = LANES // NX
        self.row = lax.broadcasted_iota(jnp.int32, (SUB, LANES), 0)
        self.lane = lax.broadcasted_iota(jnp.int32, (SUB, LANES), 1)
        self.zrow = self.row % depth
        self.xcol = self.lane % NX

    def rows(self, value, shift):
        shift %= SUB
        return pltpu.roll(value, shift, 0) if shift else value

    def lanes(self, value, shift):
        shift %= LANES
        return pltpu.roll(value, shift, 1) if shift else value


def entry(left, right, i, j, part, left_h, right_h):
    total = None
    for k in range(3):
        li = (k, i) if left_h else (i, k)
        ri = (j, k) if right_h else (k, j)
        lr, lm = left[0][li[0]][li[1]], left[1][li[0]][li[1]]
        rr, rm = right[0][ri[0]][ri[1]], right[1][ri[0]][ri[1]]
        if part == 0:
            first, second = lr * rr, lm * rm
            minus = left_h == right_h
        elif left_h:
            first, second = lr * rm, lm * rr
            minus = True
        else:
            first, second = lm * rr, lr * rm
            minus = right_h
        value = first - second if minus else first + second
        total = value if total is None else total + value
    return total


def product(left, right, left_h=False, right_h=False):
    return [
        [[entry(left, right, i, j, part, left_h, right_h) for j in range(3)] for i in range(3)]
        for part in range(2)
    ]


def projected(left, right, left_h=False, right_h=False):
    get = lambda i, j, part: entry(left, right, i, j, part, left_h, right_h)
    pairs = ((0, 1), (0, 2), (1, 2))
    real = [get(i, j, 0) - get(j, i, 0) for i, j in pairs]
    imag = [get(i, j, 1) + get(j, i, 1) for i, j in pairs]
    diag = [get(i, i, 1) for i in range(3)]
    third = (diag[0] + diag[1] + diag[2]) * (1.0 / 3.0)
    return real + imag + [diag[0] - third, diag[1] - third]


def third_row(real, imag):
    rows_r, rows_i = [], []
    for column in range(3):
        n, l = (column + 1) % 3, (column + 2) % 3
        rows_r.append(
            real[0][n] * real[1][l]
            - imag[0][n] * imag[1][l]
            - real[0][l] * real[1][n]
            + imag[0][l] * imag[1][n]
        )
        rows_i.append(
            real[0][l] * imag[1][n]
            + imag[0][l] * real[1][n]
            - real[0][n] * imag[1][l]
            - imag[0][n] * real[1][l]
        )
    return rows_r, rows_i


PLANES = ((2, 3), (1, 3), (1, 2), (0, 1), (0, 2), (0, 3))
KINDS = ({0: 1}, {1: 1}, {2: 1}, {0: 1, 1: -1}, {0: 1, 2: -1}, {1: 1, 2: -1})
CORNERS = {(0, 1): (3, 1), (1, 0): (3, -1), (0, 2): (4, 1), (2, 0): (4, -1), (1, 2): (5, 1), (2, 1): (5, -1)}
FIXED = [(0, 1, 0), (0, 2, 0), (1, 0, -1), (1, 2, None), (2, 0, -1), (2, 1, None)]


def by_largest(real, imag):
    size = [jnp.maximum(jnp.abs(r), jnp.abs(i)) for r, i in zip(real, imag)]
    first = jnp.logical_and(size[0] >= size[1], size[0] >= size[2])
    second = size[1] >= size[2]
    return lambda a, b, c: jnp.where(first, a, jnp.where(second, b, c))


def shortened(v):
    pick = by_largest(v[0:3], v[6:9])
    keep = v[0:3] + v[6:9]
    for turn in (1, 2):
        for row in (v[3:6], v[9:12]):
            keep.append(pick(*(row[(k + turn) % 3] for k in range(3))))
    return keep


def restored(v):
    real, imag = v[0:3], v[3:6]
    pick = by_largest(real, imag)
    (xr, xi), (yr, yi), (zr, zi) = (
        [pick(*(part[(k + turn) % 3] for k in range(3))) for part in (real, imag)] for turn in range(3)
    )
    pr, pi, qr, qi = v[6:10]
    sr = pr * yr + pi * yi + qr * zr + qi * zi
    si = pi * yr - pr * yi + qi * zr - qr * zi
    scale = -1.0 / (xr * xr + xi * xi)
    br, bi = (sr * xr - si * xi) * scale, (sr * xi + si * xr) * scale
    second_r = [pick(br, qr, pr), pick(pr, br, qr), pick(qr, pr, br)]
    second_i = [pick(bi, qi, pi), pick(pi, bi, qi), pick(qi, pi, bi)]
    third_r, third_i = third_row([real, second_r], [imag, second_i])
    return [[real, second_r, third_r], [imag, second_i, third_i]]


def mail(depth, halves):
    up = lambda a, b: -(-a // b) * SUB
    per, yg = SUB // depth, LANES // NX
    t, z, y = up(12, per), up(12, depth) * halves, up(36, yg) * halves
    short = up(10, per)
    groups = (
        ((("low", 2), y),),
        ((("low", 1, 3), z),),
        ((("low", 1, 0), z),),
        ((("low", 1, 2), z),),
        ((("high", 2), 3 * up(12 * halves, yg)),),
        ((("high", 1, 3), z), (("high", 1, 0), z), (("high", 1, 2), z)),
        ((("low", 0, 3), t),),
        ((("low", 0, 1), t), (("low", 0, 2), t)),
        (((2, 1), SUB * halves), ((1, 2), SUB * halves)),
        (((1, 0), 2 * SUB), ((2, 0), SUB)),
        ((("high", 0, 3), short), (("high", 0, 2), short)),
        (((0, 1), 2 * SUB), ((0, 2), SUB)),
        ((("high", 0, 1), short),),
    )
    places, spans, row = {}, [], 0
    for group in groups:
        first = row
        for name, rows in group:
            places[name] = (row, rows, len(spans))
            row += rows
        spans.append((first, row))
    return places, spans


def force_terms(
    counts, depth, halves, hbm, acc,
    u, ahead_s, local_s, fixed_s, outbox, inbox, load_sem, send, recv, ready,
):
    g = Lattice(depth)
    last = halves - 1
    me = [lax.axis_index(a) for a in AXES]
    places, spans = mail(depth, halves)

    cut = last * SUB
    load_last = pltpu.make_async_copy(
        hbm.at[:, :, :, :, cut:], u.at[:, :, :, :, cut:], load_sem.at[0]
    )
    load_rest = pltpu.make_async_copy(
        hbm.at[:, :, :, :, :cut], u.at[:, :, :, :, :cut], load_sem.at[1]
    )
    load_last.start()
    load_rest.start()

    def peer(kind, sign):
        where = list(me)
        for i, step in KINDS[kind].items():
            where[i] = lax.rem(me[i] + counts[i] + sign * step, counts[i])
        by = dict(zip(AXES, where))
        return (by["gx"], by["gz"], by["ta"])

    def above(axis, sign):
        return me[axis] < counts[axis] - 1 if sign > 0 else me[axis] == 0

    def lowest(kind, sign):
        tests = [above(i, sign * step) for i, step in KINDS[kind].items()]
        return functools.reduce(jnp.logical_and, tests)

    def highest(kind, sign):
        tests = [above(i, sign * step) for i, step in KINDS[kind].items()]
        return jnp.logical_not(functools.reduce(jnp.logical_or, tests))

    barrier = pltpu.get_barrier_semaphore()
    pairs = [(kind, sign) for kind in range(6) for sign in (1, -1)]
    expected = 0
    for kind, sign in pairs:
        expected = expected + jnp.where(highest(kind, sign), 1, 0)

        @pl.when(lowest(kind, sign))
        def _():
            pl.semaphore_signal(
                barrier, inc=1, device_id=peer(kind, sign), device_id_type=pl.DeviceIdType.MESH
            )

    @pl.when(expected > 0)
    def _():
        pl.semaphore_wait(barrier, expected)

    def answer_group(kind, sign):
        if kind < 3:
            return 2 if (kind, sign) == (0, -1) else 0
        return 3 if kind < 5 and sign < 0 else 1

    for kind, sign in pairs:

        @pl.when(highest(kind, sign))
        def _():
            pl.semaphore_signal(
                ready.at[answer_group(kind, -sign)], inc=1,
                device_id=peer(kind, sign), device_id_type=pl.DeviceIdType.MESH,
            )

    def answers(group):
        count = 0
        for kind, sign in pairs:
            if answer_group(kind, sign) == group:
                count = count + jnp.where(lowest(kind, sign), 1, 0)

        @pl.when(count > 0)
        def _():
            pl.semaphore_wait(ready.at[group], count)

    def start(copies):
        for copy in copies:
            copy.start()

    def early(kind, sign, copies):
        pl.when(highest(kind, sign))(lambda: start(copies))

    def late(kind, sign, copies):
        pl.when(lowest(kind, sign))(lambda: start(copies))

    def middle(kind, sign, copies):
        between = jnp.logical_not(jnp.logical_or(lowest(kind, sign), highest(kind, sign)))
        pl.when(between)(lambda: start(copies))

    def put(name, r, value):
        row = places[name][0] + r
        outbox[row : row + SUB, :] = value

    def got(name, r):
        row = places[name][0] + r
        return inbox[row : row + SUB, :]

    def load(m, part, i, j, h):
        return u[m, part, i, j, h * SUB : (h + 1) * SUB, :]

    COMPS = [(part, i, j) for part in range(2) for i in range(2) for j in range(3)]

    def comps(m):
        return [(m,) + c for c in COMPS]

    def all_comps(d):
        return [c for m in others(d) for c in comps(m)]

    def flat(value):
        return [value[part][i][j] for part, i, j in COMPS]

    def merge(values, index, step):
        total = None
        for k, x in enumerate(values):
            total = x if total is None else jnp.where(index >= step * k, x, total)
        return total

    def pack_t(m):
        cs = comps(m)
        for c0 in range(0, 12, g.per):
            put(
                ("low", 0, m), c0 // g.per * SUB,
                merge([g.rows(load(*cs[c0 + k], 0), depth * k) for k in range(g.per)], g.row, depth),
            )

    def pack_z(m):
        cs = comps(m)
        for c0 in range(0, 12, depth):
            for h in range(halves):
                put(
                    ("low", 1, m), (c0 // depth * halves + h) * SUB,
                    merge([g.rows(load(*cs[c0 + k], h), k) for k in range(depth)], g.zrow, 1),
                )

    def pack_y():
        cs = all_comps(2)
        for c0 in range(0, len(cs), g.ygroups):
            for h in range(halves):
                ks = range(min(g.ygroups, len(cs) - c0))
                put(
                    ("low", 2), (c0 // g.ygroups * halves + h) * SUB,
                    merge([g.lanes(load(*cs[c0 + k], h), NX * k) for k in ks], g.lane, NX),
                )

    def pack_vt(m, v):
        v = shortened(v)
        for c0 in range(0, 10, g.per):
            ks = range(min(g.per, 10 - c0))
            put(
                ("high", 0, m), c0 // g.per * SUB,
                merge([g.rows(v[c0 + k], depth * (k + 1)) for k in ks], g.row, depth),
            )

    def pack_vz(m, h, v):
        for c0 in range(0, 12, depth):
            put(
                ("high", 1, m), (c0 // depth * halves + h) * SUB,
                merge([g.rows(v[c0 + k], k + 1 - depth) for k in range(depth)], g.zrow, 1),
            )

    def pack_vy(m, v):
        n = places["high", 2][1] // 3
        for c0 in range(0, 12 * halves, g.ygroups):
            ks = range(min(g.ygroups, 12 * halves - c0))
            put(
                ("high", 2), others(2).index(m) * n + c0 // g.ygroups * SUB,
                merge([g.lanes(v[c0 + k], NX * (k + 1)) for k in ks], g.lane, NX),
            )

    def by_groups(d, h, up, shift, index, step):
        cs = comps(d)
        return merge(
            [
                merge(
                    [
                        g.lanes(g.rows(load(*cs[c], h), shift(c // g.ygroups)), NX * (c % g.ygroups + up))
                        for c in range(c0, min(12, c0 + g.ygroups))
                    ],
                    g.lane, NX,
                )
                for c0 in range(0, 12, g.ygroups)
            ],
            index, step,
        )

    def pack_corner(d, m):
        cs = comps(d)
        if (d, m) in ((0, 1), (1, 0)):
            source = SUB - depth if d == 0 else depth - 1
            for c0 in range(0, 12, SUB):
                ks = range(min(SUB, 12 - c0))
                values = [g.rows(load(*cs[c0 + k], last if d == 0 else 0), k - source) for k in ks]
                put((d, m), c0, merge(values, g.row, 1))
        elif (d, m) == (0, 2):
            put((d, m), 0, by_groups(0, last, 0, lambda k: depth * (k + 1), g.row, depth))
        elif (d, m) == (2, 0):
            put((d, m), 0, by_groups(2, 0, 1, lambda k: depth * k, g.row, depth))
        else:
            for h in range(halves):
                up, source = (0, depth - 1) if d == 1 else (1, 0)
                put((d, m), h * SUB, by_groups(d, h, up, lambda k: k - source, g.zrow, 1))

    def corner(d, m, h, c):
        k, group = c // g.ygroups, NX * (c % g.ygroups)
        if (d, m) in ((0, 1), (1, 0)):
            target = depth - 1 if d == 0 else SUB - depth
            return g.rows(got((d, m), c // SUB * SUB), target - c % SUB)
        if (d, m) == (0, 2):
            return g.lanes(g.rows(got((d, m), 0), -depth * k), LANES - NX - group)
        if (d, m) == (2, 0):
            return g.lanes(g.rows(got((d, m), 0), SUB - depth - depth * k), -group)
        if d == 1:
            return g.lanes(g.rows(got((d, m), h * SUB), -k), LANES - NX - group)
        return g.lanes(g.rows(got((d, m), h * SUB), depth - 1 - k), -group)

    def remote(first, end, group, kind, sign):
        return pltpu.make_async_remote_copy(
            src_ref=outbox.at[first:end], dst_ref=inbox.at[first:end],
            send_sem=send.at[0], recv_sem=recv.at[group],
            device_id=peer(kind, sign), device_id_type=pl.DeviceIdType.MESH,
        )

    def message(name, kind, sign):
        first, rows, group = places[name]
        return remote(first, first + rows, group, kind, sign)

    def arrived(name):
        group = places[name][2]
        remote(*spans[group], group, 0, 1).wait_recv()

    low = {(d, m): message(("low", d, m), d, -1) for d in (0, 1) for m in others(d)}
    high = {(d, m): message(("high", d, m), d, 1) for d in (0, 1) for m in others(d)}
    low_y, high_y = message(("low", 2), 2, -1), message(("high", 2), 2, 1)
    corners = {key: message(key, kind, sign) for key, (kind, sign) in CORNERS.items()}

    def matrix(m, h):
        return [[[load(m, part, i, j, h) for j in range(3)] for i in range(3)] for part in range(2)]

    def save(ref, index, value):
        for part in range(2):
            for i in range(len(value[part])):
                for j in range(3):
                    ref[index, part, i, j] = value[part][i][j]

    def saved(ref, index, rows=3):
        return [[[ref[index, part, i, j] for j in range(3)] for i in range(rows)] for part in range(2)]

    def rolled(m, d, h, part, i, j):
        v = load(m, part, i, j, h)
        if d == 3:
            return jnp.where(g.xcol == NX - 1, g.lanes(v, NX - 1), g.lanes(v, -1))
        if d == 2:
            return g.lanes(v, -NX)
        if d == 1:
            return g.rows(v, -1)
        if h + 1 < halves:
            beyond = g.rows(load(m, part, i, j, h + 1), -depth)
            return jnp.where(g.row >= SUB - depth, beyond, g.rows(v, -depth))
        return g.rows(v, -depth)

    def complete(d, h):
        return d == 3 or (d == 0 and h + 1 < halves)

    def far_edge(d):
        return (g.row >= SUB - depth, g.zrow == depth - 1, g.lane >= LANES - NX)[d]

    ahead_slot = {}

    def prepare(m, d, h, rows):
        value = [
            [[rolled(m, d, h, part, i, j) for j in range(3)] for i in range(3 if rows == 3 or complete(d, h) else 2)]
            for part in range(2)
        ]
        ahead_slot[m, d, h] = len(ahead_slot)
        keep = 3 if complete(d, h) else 2
        save(ahead_s, ahead_slot[m, d, h], [part[:keep] for part in value])
        return value

    def transported(b, m, d, h, b_h):
        moved = prepare(m, d, h, 3)
        value = [
            [[entry(b, moved, i, j, part, b_h, False) for j in range(3)] for i in range(2)]
            for part in range(2)
        ]
        if not complete(d, h):
            edge = far_edge(d)
            for part in range(2):
                for i in range(2):
                    for j in range(3):
                        own = b[part][j][i] if b_h else b[part][i][j]
                        own = -own if b_h and part else own
                        value[part][i][j] = jnp.where(edge, own, value[part][i][j])
        return flat(value)

    local = {}

    def local_product(mu, nu, h):
        b = product(matrix(mu, h), matrix(nu, h), left_h=True)
        save(local_s, PLANES.index((mu, nu)) * halves + h, b)
        return b

    below_t, below_z = [low[0, m] for m in (3, 1, 2)], [low[1, m] for m in (3, 0, 2)]
    above_t = [high[0, m] for m in (3, 2, 1)]
    at_end = me[0] == counts[0] - 1

    def faces():
        load_rest.wait()
        for m in (3, 1, 2):
            pack_t(m)
        early(0, -1, below_t)
        for m in (3, 0, 2):
            pack_z(m)
        early(1, -1, below_z)

    acc[...] = jnp.zeros_like(acc)
    load_last.wait()
    for d in (1, 2):
        pack_corner(0, d)
        early(*CORNERS[0, d], [corners[0, d]])
    pl.when(jnp.logical_not(at_end))(faces)
    for m in (3, 2, 1):
        b = local_product(0, m, last)
        pack_vt(m, transported(b, 0, m, last, False))
        early(0, 1, [high[0, m]])
    pl.when(at_end)(faces)
    pack_y()
    early(2, -1, [low_y])
    for key in ((1, 0), (2, 0), (1, 2), (2, 1)):
        pack_corner(*key)
    for key in ((1, 0), (2, 0), (1, 2), (2, 1)):
        early(*CORNERS[key], [corners[key]])

    lifted = {}

    def lift(mu, nu):
        for h in range(halves):
            if mu == 0 and h == last:
                b = saved(local_s, PLANES.index((mu, nu)) * halves + h)
            else:
                b = local_product(mu, nu, h)
            if mu:
                lifted[mu, nu, h] = transported(b, mu, nu, h, False)
            elif h != last:
                prepare(mu, nu, h, 2)
            if nu != 3:
                lifted[nu, mu, h] = transported(b, nu, mu, h, True)
            else:
                prepare(nu, mu, h, 2)
        for d, m in ((mu, nu), (nu, mu)):
            if d == 1:
                for h in range(halves):
                    pack_vz(m, h, lifted[d, m, h])
            elif d == 2:
                pack_vy(m, [x for h in range(halves) for x in lifted[d, m, h]])

    def greeted():
        answers(0)
        late(2, -1, [low_y])
        for key in ((0, 1), (0, 2), (1, 2), (2, 1)):
            middle(*CORNERS[key], [corners[key]])
        late(1, -1, below_z)
        late(0, 1, above_t)
        for key in ((1, 0), (2, 0)):
            between = jnp.logical_and(me[0] > 0, jnp.logical_not(highest(*CORNERS[key])))
            pl.when(between)(corners[key].start)

    pl.when(at_end)(greeted)
    lift(1, 3)
    lift(0, 1)
    lift(1, 2)
    pl.when(jnp.logical_not(at_end))(greeted)
    for m in (3, 0, 2):
        high[1, m].start()
    lift(2, 3)
    lift(0, 2)
    high_y.start()
    lift(0, 3)
    answers(1)
    for key in ((0, 1), (0, 2), (1, 2), (2, 1)):
        late(*CORNERS[key], [corners[key]])

    def ahead(m, d, h):
        if complete(d, h):
            return saved(ahead_s, ahead_slot[m, d, h])
        index = {c: n for n, c in enumerate(all_comps(d))}

        def get(part, i, j):
            v = ahead_s[ahead_slot[m, d, h], part, i, j]
            c = index[(m, part, i, j)]
            k = c % 12
            if d == 0:
                edge = g.rows(got(("low", 0, m), k // g.per * SUB), SUB - depth - depth * (k % g.per))
            elif d == 1:
                edge = g.rows(got(("low", 1, m), (k // depth * halves + h) * SUB), depth - 1 - k % depth)
            else:
                edge = g.lanes(
                    got(("low", 2), (c // g.ygroups * halves + h) * SUB), LANES - NX - NX * (c % g.ygroups)
                )
            return jnp.where(far_edge(d), edge, v)

        return complete_rows(get)

    def complete_rows(get):
        real = [[get(0, i, j) for j in range(3)] for i in range(2)]
        imag = [[get(1, i, j) for j in range(3)] for i in range(2)]
        third_r, third_i = third_row(real, imag)
        return [real + [third_r], imag + [third_i]]

    def add(m, c, h, value):
        r = ((m * 8 + c) * halves + h) * SUB
        acc[r : r + SUB, :] += value

    def shifted(q, d):
        if d == 3:
            return jnp.where(g.xcol == 0, g.lanes(q, 1 - NX), g.lanes(q, 1))
        if d == 2:
            return jnp.where(g.lane >= NX, g.lanes(q, NX), 0.0)
        if d == 1:
            return jnp.where(g.zrow > 0, g.rows(q, 1), 0.0)
        return jnp.where(g.row >= depth, g.rows(q, depth), 0.0)

    def plane(mu, nu, h):
        a = product(ahead(nu, mu, h), ahead(mu, nu, h), right_h=True)
        b = saved(local_s, PLANES.index((mu, nu)) * halves + h)
        e = product(matrix(mu, h), a)
        upper = projected(e, matrix(nu, h), right_h=True)
        q = projected(a, b, left_h=True)
        for c in range(8):
            add(mu, c, h, shifted(q[c], nu) + upper[c])
        q = projected(a, b, right_h=True)
        for c in range(8):
            add(nu, c, h, shifted(q[c], mu) - upper[c])
            if mu == 0 and h + 1 < halves:
                add(nu, c, h + 1, jnp.where(g.row < depth, g.rows(q[c], depth), 0.0))

    fixed_slot = {}

    def fix(d, m, h):
        beyond = complete_rows(lambda part, i, j: corner(d, m, h, part * 6 + i * 3 + j))
        own = matrix(m, h)
        moved = product(own, beyond, right_h=True)
        edge = far_edge(m)
        fixed_slot[d, m, h] = len(fixed_slot)
        save(
            fixed_s, fixed_slot[d, m, h],
            [[[jnp.where(edge, moved[p][i][j], own[p][i][j]) for j in range(3)] for i in range(3)] for p in range(2)],
        )

    def lower(d, m, h):
        def get(part, i, j):
            c = part * 6 + i * 3 + j
            if d == 1:
                return g.rows(got(("high", 1, m), (c // depth * halves + h) * SUB), -(c % depth))
            n, k = places["high", 2][1] // 3, h * 12 + c
            r = others(2).index(m) * n + k // g.ygroups * SUB
            return g.lanes(got(("high", 2), r), -NX * (k % g.ygroups))

        if (d, m, h) in fixed_slot:
            left = saved(fixed_s, fixed_slot[d, m, h])
        else:
            left = matrix(m, h)
        if d == 0:
            lifts = restored(
                [g.rows(got(("high", 0, m), c // g.per * SUB), -depth * (c % g.per)) for c in range(10)]
            )
        else:
            lifts = complete_rows(get)
        q = projected(left, lifts, right_h=True)
        near = (g.row < depth, g.zrow == 0, g.lane < NX)[d]
        for c in range(8):
            add(m, c, h, jnp.where(near, q[c], 0.0))

    def y_part():
        arrived(("low", 2))
        for h in range(halves):
            plane(2, 3, h)
        for h in range(last):
            plane(0, 2, h)

    def z_part():
        arrived(("low", 1, 3))
        for h in range(halves):
            plane(1, 3, h)

    def around_part():
        answers(2)
        late(0, -1, below_t)

    def rest_part():
        arrived(("low", 1, 0))
        for h in range(last):
            plane(0, 1, h)

    for h in range(last):
        plane(0, 3, h)
    even = lax.rem(me[2], 2) == 0

    @pl.when(even)
    def _():
        y_part()
        around_part()
        z_part()
        rest_part()

    @pl.when(jnp.logical_not(even))
    def _():
        z_part()
        around_part()
        rest_part()
        y_part()

    answers(3)
    for key in ((1, 0), (2, 0)):
        first = jnp.logical_and(me[0] == 0, jnp.logical_not(highest(*CORNERS[key])))
        pl.when(first)(corners[key].start)

    arrived(("low", 1, 2))
    for h in range(halves):
        plane(1, 2, h)
    arrived(("high", 2))
    for m in (3, 0):
        for h in range(halves if m else last):
            lower(2, m, h)
    arrived(("low", 0, 3))
    plane(0, 3, last)
    arrived(("low", 0, 1))
    plane(0, 1, last)
    plane(0, 2, last)
    arrived((2, 1))
    for h in range(halves):
        fix(2, 1, h)
        lower(2, 1, h)
        fix(1, 2, h)
    arrived((1, 0))
    fix(2, 0, last)
    lower(2, 0, last)
    fix(1, 0, last)
    arrived(("high", 1, 3))
    for m in (3, 0, 2):
        for h in range(halves):
            lower(1, m, h)
    arrived(("high", 0, 3))
    lower(0, 3, 0)
    arrived((0, 1))
    fix(0, 2, 0)
    fix(0, 1, 0)
    lower(0, 2, 0)
    arrived(("high", 0, 1))
    lower(0, 1, 0)
    remote(0, spans[-1][1], 0, 0, 1).wait_send()


def expand(halves, acc, hbm, out, sems):
    copies = []
    for m in range(4):
        for h in range(halves):
            rows = [((m * 8 + c) * halves + h) * SUB for c in range(8)]
            f = [acc[r : r + SUB, :] * (COEFF * 0.5 if c < 6 else COEFF) for c, r in enumerate(rows)]

            def put(part, i, j, value):
                out[m, part, i, j, h * SUB : (h + 1) * SUB, :] = value

            for n, (i, j) in enumerate(((0, 1), (0, 2), (1, 2))):
                put(0, i, j, f[n])
                put(0, j, i, -f[n])
                put(1, i, j, f[3 + n])
                put(1, j, i, f[3 + n])
            for i in range(3):
                put(0, i, i, jnp.zeros((SUB, LANES), jnp.float32))
            put(1, 0, 0, f[6])
            put(1, 1, 1, f[7])
            put(1, 2, 2, -(f[6] + f[7]))
        copies.append(pltpu.make_async_copy(out.at[m], hbm.at[m], sems.at[m]))
        copies[-1].start()
    for copy in copies:
        copy.wait()


def per_device(counts, links):
    time_len, depth, flat = links.shape[4:]
    sites = time_len * depth
    assert flat == LANES and SUB % depth == 0 and sites % SUB == 0 and 2 <= depth <= SUB // 2
    halves = sites // SUB
    spans = mail(depth, halves)[1]
    vmem = lambda *s: pltpu.VMEM(s + (LANES,), jnp.float32)
    shape = links.shape[:4] + (sites, flat)
    terms = pl.pallas_call(
        functools.partial(force_terms, counts, depth, halves),
        out_shape=pltpu.VMEM((32 * sites, flat), jnp.float32),
        in_specs=[pl.BlockSpec(memory_space=pl.ANY)],
        out_specs=pl.BlockSpec(memory_space=pltpu.VMEM),
        scratch_shapes=[
            vmem(*shape[:-1]),
            vmem(12 * halves, 2, 3, 3, SUB),
            vmem(6 * halves, 2, 3, 3, SUB),
            vmem(4 + 2 * halves, 2, 3, 3, SUB),
            vmem(spans[-1][1]),
            vmem(spans[-1][1]),
            pltpu.SemaphoreType.DMA((2,)),
            pltpu.SemaphoreType.DMA((1,)),
            pltpu.SemaphoreType.DMA((len(spans),)),
            pltpu.SemaphoreType.REGULAR((4,)),
        ],
        compiler_params=pltpu.CompilerParams(collective_id=0, has_side_effects=True),
        name="force_terms",
    )(links.reshape(shape))
    out = pl.pallas_call(
        functools.partial(expand, halves),
        out_shape=jax.ShapeDtypeStruct(shape, jnp.float32),
        in_specs=[pl.BlockSpec(memory_space=pltpu.VMEM)],
        out_specs=pl.BlockSpec(memory_space=pl.ANY),
        scratch_shapes=[vmem(*shape[:-1]), pltpu.SemaphoreType.DMA((4,))],
        name="expand",
    )(pltpu.with_memory_space_constraint(terms, pltpu.VMEM))
    return out.reshape(links.shape)


def solution(mesh):
    assert mesh.axis_names == ("gx", "gz", "ta")
    counts = tuple(mesh.shape[a] for a in AXES)
    spec = P(None, None, None, None, "ta", "gz", "gx")
    return jax.shard_map(
        functools.partial(per_device, counts),
        mesh=mesh,
        in_specs=(spec,),
        out_specs=spec,
        check_vma=False,
    )
```

```python
import functools

import jax
import jax.numpy as jnp
from jax import lax
from jax.experimental import pallas as pl
from jax.experimental.pallas import tpu as pltpu
from jax.sharding import PartitionSpec as P

NX = 16
COEFF = -1.9
AXES = ("ta", "gz", "gx")
SUB, LANES = 8, 128


def others(d):
    return [m for m in range(4) if m != d]


class Lattice:
    def __init__(self, depth):
        self.depth = depth
        self.per = SUB // depth
        self.ygroups = LANES // NX
        self.row = lax.broadcasted_iota(jnp.int32, (SUB, LANES), 0)
        self.lane = lax.broadcasted_iota(jnp.int32, (SUB, LANES), 1)
        self.zrow = self.row % depth
        self.xcol = self.lane % NX

    def rows(self, value, shift):
        shift %= SUB
        return pltpu.roll(value, shift, 0) if shift else value

    def lanes(self, value, shift):
        shift %= LANES
        return pltpu.roll(value, shift, 1) if shift else value


def entry(left, right, i, j, part, left_h, right_h):
    total = None
    for k in range(3):
        li = (k, i) if left_h else (i, k)
        ri = (j, k) if right_h else (k, j)
        lr, lm = left[0][li[0]][li[1]], left[1][li[0]][li[1]]
        rr, rm = right[0][ri[0]][ri[1]], right[1][ri[0]][ri[1]]
        if part == 0:
            first, second = lr * rr, lm * rm
            minus = left_h == right_h
        elif left_h:
            first, second = lr * rm, lm * rr
            minus = True
        else:
            first, second = lm * rr, lr * rm
            minus = right_h
        value = first - second if minus else first + second
        total = value if total is None else total + value
    return total


def product(left, right, left_h=False, right_h=False):
    return [
        [[entry(left, right, i, j, part, left_h, right_h) for j in range(3)] for i in range(3)]
        for part in range(2)
    ]


def projected(left, right, left_h=False, right_h=False):
    get = lambda i, j, part: entry(left, right, i, j, part, left_h, right_h)
    pairs = ((0, 1), (0, 2), (1, 2))
    real = [get(i, j, 0) - get(j, i, 0) for i, j in pairs]
    imag = [get(i, j, 1) + get(j, i, 1) for i, j in pairs]
    diag = [get(i, i, 1) for i in range(3)]
    third = (diag[0] + diag[1] + diag[2]) * (1.0 / 3.0)
    return real + imag + [diag[0] - third, diag[1] - third]


def third_row(real, imag):
    rows_r, rows_i = [], []
    for column in range(3):
        n, l = (column + 1) % 3, (column + 2) % 3
        rows_r.append(
            real[0][n] * real[1][l]
            - imag[0][n] * imag[1][l]
            - real[0][l] * real[1][n]
            + imag[0][l] * imag[1][n]
        )
        rows_i.append(
            real[0][l] * imag[1][n]
            + imag[0][l] * real[1][n]
            - real[0][n] * imag[1][l]
            - imag[0][n] * real[1][l]
        )
    return rows_r, rows_i


PLANES = ((2, 3), (1, 3), (1, 2), (0, 1), (0, 2), (0, 3))
KINDS = ({0: 1}, {1: 1}, {2: 1}, {0: 1, 1: -1}, {0: 1, 2: -1}, {1: 1, 2: -1})
CORNERS = {(0, 1): (3, 1), (1, 0): (3, -1), (0, 2): (4, 1), (2, 0): (4, -1), (1, 2): (5, 1), (2, 1): (5, -1)}
FIXED = [(0, 1, 0), (0, 2, 0), (1, 0, -1), (1, 2, None), (2, 0, -1), (2, 1, None)]


def by_largest(real, imag):
    size = [jnp.maximum(jnp.abs(r), jnp.abs(i)) for r, i in zip(real, imag)]
    first = jnp.logical_and(size[0] >= size[1], size[0] >= size[2])
    second = size[1] >= size[2]
    return lambda a, b, c: jnp.where(first, a, jnp.where(second, b, c))


def shortened(v):
    pick = by_largest(v[0:3], v[6:9])
    keep = v[0:3] + v[6:9]
    for turn in (1, 2):
        for row in (v[3:6], v[9:12]):
            keep.append(pick(*(row[(k + turn) % 3] for k in range(3))))
    return keep


def restored(v):
    real, imag = v[0:3], v[3:6]
    pick = by_largest(real, imag)
    (xr, xi), (yr, yi), (zr, zi) = (
        [pick(*(part[(k + turn) % 3] for k in range(3))) for part in (real, imag)] for turn in range(3)
    )
    pr, pi, qr, qi = v[6:10]
    sr = pr * yr + pi * yi + qr * zr + qi * zi
    si = pi * yr - pr * yi + qi * zr - qr * zi
    scale = -1.0 / (xr * xr + xi * xi)
    br, bi = (sr * xr - si * xi) * scale, (sr * xi + si * xr) * scale
    second_r = [pick(br, qr, pr), pick(pr, br, qr), pick(qr, pr, br)]
    second_i = [pick(bi, qi, pi), pick(pi, bi, qi), pick(qi, pi, bi)]
    third_r, third_i = third_row([real, second_r], [imag, second_i])
    return [[real, second_r, third_r], [imag, second_i, third_i]]


def mail(depth, halves):
    up = lambda a, b: -(-a // b) * SUB
    per, yg = SUB // depth, LANES // NX
    t, z, y = up(12, per), up(12, depth) * halves, up(36, yg) * halves
    short = up(10, per)
    groups = (
        ((("low", 2), y),),
        ((("low", 1, 3), z),),
        ((("low", 1, 0), z),),
        ((("low", 1, 2), z),),
        ((("high", 2), 3 * up(12 * halves, yg)),),
        ((("high", 1, 3), z), (("high", 1, 0), z), (("high", 1, 2), z)),
        ((("low", 0, 3), t),),
        ((("low", 0, 1), t), (("low", 0, 2), t)),
        (((2, 1), SUB * halves), ((1, 2), SUB * halves), ((1, 0), 2 * SUB), ((2, 0), SUB)),
        ((("high", 0, 3), short),),
        (((0, 1), 2 * SUB), ((0, 2), SUB)),
        ((("high", 0, "pair"), 10 * SUB),),
    )
    places, spans, row = {}, [], 0
    for group in groups:
        first = row
        for name, rows in group:
            places[name] = (row, rows, len(spans))
            row += rows
        spans.append((first, row))
    return places, spans


def force_terms(
    counts, depth, halves, hbm, acc,
    u, ahead_s, local_s, fixed_s, outbox, inbox, load_sem, send, recv, ready,
):
    g = Lattice(depth)
    last = halves - 1
    me = [lax.axis_index(a) for a in AXES]
    places, spans = mail(depth, halves)

    cut = last * SUB
    cut = last * SUB

    def loads(m, p, from_last):
        rows = slice(cut, None) if from_last else slice(0, cut)
        return pltpu.make_async_copy(
            hbm.at[m, p, :, :, rows], u.at[m, p, :, :, rows], load_sem.at[1 - from_last]
        )

    for from_last in (1, 0):
        for m in (0, 3, 2, 1):
            for p in range(2):
                loads(m, p, from_last).start()
    load_last, load_rest = loads(slice(None), slice(None), 1), loads(slice(None), slice(None), 0)

    def peer(kind, sign):
        where = list(me)
        for i, step in KINDS[kind].items():
            where[i] = lax.rem(me[i] + counts[i] + sign * step, counts[i])
        by = dict(zip(AXES, where))
        return (by["gx"], by["gz"], by["ta"])

    def above(axis, sign):
        rank = lambda i: i + 1 - 2 * lax.rem(i, 2) if False else i
        return rank(lax.rem(me[axis] + counts[axis] + sign, counts[axis])) > rank(me[axis])

    def lowest(kind, sign):
        tests = [above(i, sign * step) for i, step in KINDS[kind].items()]
        return functools.reduce(jnp.logical_and, tests)

    def highest(kind, sign):
        tests = [above(i, sign * step) for i, step in KINDS[kind].items()]
        return jnp.logical_not(functools.reduce(jnp.logical_or, tests))

    barrier = pltpu.get_barrier_semaphore()
    pairs = [(kind, sign) for kind in range(6) for sign in (1, -1)]
    expected = 0
    for kind, sign in pairs:
        expected = expected + jnp.where(highest(kind, sign), 1, 0)

        @pl.when(lowest(kind, sign))
        def _():
            pl.semaphore_signal(
                barrier, inc=1, device_id=peer(kind, sign), device_id_type=pl.DeviceIdType.MESH
            )

    @pl.when(expected > 0)
    def _():
        pl.semaphore_wait(barrier, expected)

    def answer_group(kind, sign):
        if kind < 3:
            return 2 if (kind, sign) == (0, -1) else 0
        return 3 if kind < 5 and sign < 0 else 1

    for kind, sign in pairs:

        @pl.when(highest(kind, sign))
        def _():
            pl.semaphore_signal(
                ready.at[answer_group(kind, -sign)], inc=1,
                device_id=peer(kind, sign), device_id_type=pl.DeviceIdType.MESH,
            )

    def answers(group):
        count = 0
        for kind, sign in pairs:
            if answer_group(kind, sign) == group:
                count = count + jnp.where(lowest(kind, sign), 1, 0)

        @pl.when(count > 0)
        def _():
            pl.semaphore_wait(ready.at[group], count)

    def start(copies):
        for copy in copies:
            copy.start()

    def early(kind, sign, copies):
        pl.when(highest(kind, sign))(lambda: start(copies))

    def late(kind, sign, copies):
        pl.when(lowest(kind, sign))(lambda: start(copies))

    def middle(kind, sign, copies):
        between = jnp.logical_not(jnp.logical_or(lowest(kind, sign), highest(kind, sign)))
        pl.when(between)(lambda: start(copies))

    def put(name, r, value):
        row = places[name][0] + r
        outbox[row : row + SUB, :] = value

    def got(name, r):
        row = places[name][0] + r
        return inbox[row : row + SUB, :]

    def load(m, part, i, j, h):
        return u[m, part, i, j, h * SUB : (h + 1) * SUB, :]

    COMPS = [(part, i, j) for part in range(2) for i in range(2) for j in range(3)]

    def comps(m):
        return [(m,) + c for c in COMPS]

    def all_comps(d):
        return [c for m in others(d) for c in comps(m)]

    def flat(value):
        return [value[part][i][j] for part, i, j in COMPS]

    def merge(values, index, step):
        total = None
        for k, x in enumerate(values):
            total = x if total is None else jnp.where(index >= step * k, x, total)
        return total

    def pack_t(m):
        cs = comps(m)
        for c0 in range(0, 12, g.per):
            put(
                ("low", 0, m), c0 // g.per * SUB,
                merge([g.rows(load(*cs[c0 + k], 0), depth * k) for k in range(g.per)], g.row, depth),
            )

    def pack_z(m):
        cs = comps(m)
        for c0 in range(0, 12, depth):
            for h in range(halves):
                put(
                    ("low", 1, m), (c0 // depth * halves + h) * SUB,
                    merge([g.rows(load(*cs[c0 + k], h), k) for k in range(depth)], g.zrow, 1),
                )

    def pack_y():
        cs = all_comps(2)
        for c0 in range(0, len(cs), g.ygroups):
            for h in range(halves):
                ks = range(min(g.ygroups, len(cs) - c0))
                put(
                    ("low", 2), (c0 // g.ygroups * halves + h) * SUB,
                    merge([g.lanes(load(*cs[c0 + k], h), NX * k) for k in ks], g.lane, NX),
                )

    def pack_vt(v):
        v = shortened(v)
        for c0 in range(0, 10, g.per):
            ks = range(min(g.per, 10 - c0))
            put(
                ("high", 0, 3), c0 // g.per * SUB,
                merge([g.rows(v[c0 + k], depth * (k + 1)) for k in ks], g.row, depth),
            )

    def pack_pair(one, two):
        for c, (v, w) in enumerate(zip(shortened(one), shortened(two))):
            put(("high", 0, "pair"), c * SUB, jnp.where(g.row >= depth, g.rows(w, 2 * depth), g.rows(v, depth)))

    def pack_vz(m, h, v):
        for c0 in range(0, 12, depth):
            put(
                ("high", 1, m), (c0 // depth * halves + h) * SUB,
                merge([g.rows(v[c0 + k], k + 1 - depth) for k in range(depth)], g.zrow, 1),
            )

    def pack_vy(m, v):
        n = places["high", 2][1] // 3
        for c0 in range(0, 12 * halves, g.ygroups):
            ks = range(min(g.ygroups, 12 * halves - c0))
            put(
                ("high", 2), others(2).index(m) * n + c0 // g.ygroups * SUB,
                merge([g.lanes(v[c0 + k], NX * (k + 1)) for k in ks], g.lane, NX),
            )

    def by_groups(d, h, up, shift, index, step):
        cs = comps(d)
        return merge(
            [
                merge(
                    [
                        g.lanes(g.rows(load(*cs[c], h), shift(c // g.ygroups)), NX * (c % g.ygroups + up))
                        for c in range(c0, min(12, c0 + g.ygroups))
                    ],
                    g.lane, NX,
                )
                for c0 in range(0, 12, g.ygroups)
            ],
            index, step,
        )

    def pack_corner(d, m):
        cs = comps(d)
        if (d, m) in ((0, 1), (1, 0)):
            source = SUB - depth if d == 0 else depth - 1
            for c0 in range(0, 12, SUB):
                ks = range(min(SUB, 12 - c0))
                values = [g.rows(load(*cs[c0 + k], last if d == 0 else 0), k - source) for k in ks]
                put((d, m), c0, merge(values, g.row, 1))
        elif (d, m) == (0, 2):
            put((d, m), 0, by_groups(0, last, 0, lambda k: depth * (k + 1), g.row, depth))
        elif (d, m) == (2, 0):
            put((d, m), 0, by_groups(2, 0, 1, lambda k: depth * k, g.row, depth))
        else:
            for h in range(halves):
                up, source = (0, depth - 1) if d == 1 else (1, 0)
                put((d, m), h * SUB, by_groups(d, h, up, lambda k: k - source, g.zrow, 1))

    def corner(d, m, h, c):
        k, group = c // g.ygroups, NX * (c % g.ygroups)
        if (d, m) in ((0, 1), (1, 0)):
            target = depth - 1 if d == 0 else SUB - depth
            return g.rows(got((d, m), c // SUB * SUB), target - c % SUB)
        if (d, m) == (0, 2):
            return g.lanes(g.rows(got((d, m), 0), -depth * k), LANES - NX - group)
        if (d, m) == (2, 0):
            return g.lanes(g.rows(got((d, m), 0), SUB - depth - depth * k), -group)
        if d == 1:
            return g.lanes(g.rows(got((d, m), h * SUB), -k), LANES - NX - group)
        return g.lanes(g.rows(got((d, m), h * SUB), depth - 1 - k), -group)

    def remote(first, end, group, kind, sign):
        return pltpu.make_async_remote_copy(
            src_ref=outbox.at[first:end], dst_ref=inbox.at[first:end],
            send_sem=send.at[0], recv_sem=recv.at[group],
            device_id=peer(kind, sign), device_id_type=pl.DeviceIdType.MESH,
        )

    def message(name, kind, sign):
        first, rows, group = places[name]
        return remote(first, first + rows, group, kind, sign)

    def arrived(name):
        group = places[name][2]
        remote(*spans[group], group, 0, 1).wait_recv()

    low = {(d, m): message(("low", d, m), d, -1) for d in (0, 1) for m in others(d)}
    high = {(d, m): message(("high", d, m), d, 1) for d, m in ((0, 3), (0, "pair"), (1, 0), (1, 2), (1, 3))}
    low_y, high_y = message(("low", 2), 2, -1), message(("high", 2), 2, 1)
    corners = {key: message(key, kind, sign) for key, (kind, sign) in CORNERS.items()}

    def matrix(m, h):
        return [[[load(m, part, i, j, h) for j in range(3)] for i in range(3)] for part in range(2)]

    def save(ref, index, value):
        for part in range(2):
            for i in range(len(value[part])):
                for j in range(3):
                    ref[index, part, i, j] = value[part][i][j]

    def saved(ref, index, rows=3):
        return [[[ref[index, part, i, j] for j in range(3)] for i in range(rows)] for part in range(2)]

    def rolled(m, d, h, part, i, j):
        v = load(m, part, i, j, h)
        if d == 3:
            return jnp.where(g.xcol == NX - 1, g.lanes(v, NX - 1), g.lanes(v, -1))
        if d == 2:
            return g.lanes(v, -NX)
        if d == 1:
            return g.rows(v, -1)
        if h + 1 < halves:
            beyond = g.rows(load(m, part, i, j, h + 1), -depth)
            return jnp.where(g.row >= SUB - depth, beyond, g.rows(v, -depth))
        return g.rows(v, -depth)

    def complete(d, h):
        return d == 3 or (d == 0 and h + 1 < halves)

    def far_edge(d):
        return (g.row >= SUB - depth, g.zrow == depth - 1, g.lane >= LANES - NX)[d]

    ahead_slot = {}

    def prepare(m, d, h, rows):
        value = [
            [[rolled(m, d, h, part, i, j) for j in range(3)] for i in range(3 if rows == 3 or complete(d, h) else 2)]
            for part in range(2)
        ]
        ahead_slot[m, d, h] = len(ahead_slot)
        keep = 3 if complete(d, h) else 2
        save(ahead_s, ahead_slot[m, d, h], [part[:keep] for part in value])
        return value

    def transported(b, m, d, h, b_h):
        moved = prepare(m, d, h, 3)
        value = [
            [[entry(b, moved, i, j, part, b_h, False) for j in range(3)] for i in range(2)]
            for part in range(2)
        ]
        if not complete(d, h):
            edge = far_edge(d)
            for part in range(2):
                for i in range(2):
                    for j in range(3):
                        own = b[part][j][i] if b_h else b[part][i][j]
                        own = -own if b_h and part else own
                        value[part][i][j] = jnp.where(edge, own, value[part][i][j])
        return flat(value)

    local = {}

    def local_product(mu, nu, h):
        b = product(matrix(mu, h), matrix(nu, h), left_h=True)
        save(local_s, PLANES.index((mu, nu)) * halves + h, b)
        return b

    below_t, below_z = [low[0, m] for m in (3, 1, 2)], [low[1, m] for m in (3, 0, 2)]
    above_t = [high[0, 3], high[0, "pair"]]
    even = lax.rem(me[2], 2) == 0
    at_end = me[0] == counts[0] - 1

    def faces():
        load_rest.wait()
        for m in (3, 1, 2):
            pack_t(m)
        pl.when(jnp.logical_not(at_end))(lambda: early(0, -1, below_t))
        for m in (3, 0, 2):
            pack_z(m)
        early(1, -1, below_z)
        pack_y()
        early(2, -1, [low_y])

    acc[...] = jnp.zeros_like(acc)
    load_last.wait()
    for d in (1, 2):
        pack_corner(0, d)
        early(*CORNERS[0, d], [corners[0, d]])
    pl.when(jnp.logical_not(at_end))(faces)
    pack_vt(transported(local_product(0, 3, last), 0, 3, last, False))
    early(0, 1, [high[0, 3]])
    pack_pair(*(transported(local_product(0, m, last), 0, m, last, False) for m in (1, 2)))
    early(0, 1, [high[0, "pair"]])
    pl.when(at_end)(faces)
    for key in ((1, 0), (2, 0), (1, 2), (2, 1)):
        pack_corner(*key)
    for key in ((1, 0), (2, 0), (1, 2), (2, 1)):
        early(*CORNERS[key], [corners[key]])

    lifted = {}

    def lift(mu, nu):
        for h in range(halves):
            if mu == 0 and h == last:
                b = saved(local_s, PLANES.index((mu, nu)) * halves + h)
            else:
                b = local_product(mu, nu, h)
            if mu:
                lifted[mu, nu, h] = transported(b, mu, nu, h, False)
            elif h != last:
                prepare(mu, nu, h, 2)
            if nu != 3:
                lifted[nu, mu, h] = transported(b, nu, mu, h, True)
            else:
                prepare(nu, mu, h, 2)
        for d, m in ((mu, nu), (nu, mu)):
            if d == 1:
                for h in range(halves):
                    pack_vz(m, h, lifted[d, m, h])
            elif d == 2:
                pack_vy(m, [x for h in range(halves) for x in lifted[d, m, h]])

    def greeted():
        answers(0)
        late(2, -1, [low_y])
        for key in ((0, 1), (0, 2), (1, 2), (2, 1)):
            middle(*CORNERS[key], [corners[key]])
        pl.when(at_end)(lambda: start(below_t))
        late(1, -1, below_z)
        late(0, 1, above_t)
        for key in ((1, 0), (2, 0)):
            between = jnp.logical_and(me[0] > 0, jnp.logical_not(highest(*CORNERS[key])))
            pl.when(between)(corners[key].start)

    pl.when(at_end)(greeted)
    lift(1, 3)
    lift(0, 1)
    lift(1, 2)
    pl.when(jnp.logical_not(at_end))(greeted)
    for m in (3, 0, 2):
        high[1, m].start()
    lift(2, 3)
    lift(0, 2)
    high_y.start()
    lift(0, 3)
    answers(1)
    for key in ((0, 1), (0, 2), (1, 2), (2, 1)):
        late(*CORNERS[key], [corners[key]])

    def ahead(m, d, h):
        if complete(d, h):
            return saved(ahead_s, ahead_slot[m, d, h])
        index = {c: n for n, c in enumerate(all_comps(d))}

        def get(part, i, j):
            v = ahead_s[ahead_slot[m, d, h], part, i, j]
            c = index[(m, part, i, j)]
            k = c % 12
            if d == 0:
                edge = g.rows(got(("low", 0, m), k // g.per * SUB), SUB - depth - depth * (k % g.per))
            elif d == 1:
                edge = g.rows(got(("low", 1, m), (k // depth * halves + h) * SUB), depth - 1 - k % depth)
            else:
                edge = g.lanes(
                    got(("low", 2), (c // g.ygroups * halves + h) * SUB), LANES - NX - NX * (c % g.ygroups)
                )
            return jnp.where(far_edge(d), edge, v)

        return complete_rows(get)

    def complete_rows(get):
        real = [[get(0, i, j) for j in range(3)] for i in range(2)]
        imag = [[get(1, i, j) for j in range(3)] for i in range(2)]
        third_r, third_i = third_row(real, imag)
        return [real + [third_r], imag + [third_i]]

    def add(m, c, h, value):
        r = ((m * 8 + c) * halves + h) * SUB
        acc[r : r + SUB, :] += value

    def shifted(q, d):
        if d == 3:
            return jnp.where(g.xcol == 0, g.lanes(q, 1 - NX), g.lanes(q, 1))
        if d == 2:
            return jnp.where(g.lane >= NX, g.lanes(q, NX), 0.0)
        if d == 1:
            return jnp.where(g.zrow > 0, g.rows(q, 1), 0.0)
        return jnp.where(g.row >= depth, g.rows(q, depth), 0.0)

    def plane(mu, nu, h):
        a = product(ahead(nu, mu, h), ahead(mu, nu, h), right_h=True)
        b = saved(local_s, PLANES.index((mu, nu)) * halves + h)
        e = product(matrix(mu, h), a)
        upper = projected(e, matrix(nu, h), right_h=True)
        q = projected(a, b, left_h=True)
        for c in range(8):
            add(mu, c, h, shifted(q[c], nu) + upper[c])
        q = projected(a, b, right_h=True)
        for c in range(8):
            add(nu, c, h, shifted(q[c], mu) - upper[c])
            if mu == 0 and h + 1 < halves:
                add(nu, c, h + 1, jnp.where(g.row < depth, g.rows(q[c], depth), 0.0))

    fixed_slot = {}

    def fix(d, m, h):
        beyond = complete_rows(lambda part, i, j: corner(d, m, h, part * 6 + i * 3 + j))
        own = matrix(m, h)
        moved = product(own, beyond, right_h=True)
        edge = far_edge(m)
        fixed_slot[d, m, h] = len(fixed_slot)
        save(
            fixed_s, fixed_slot[d, m, h],
            [[[jnp.where(edge, moved[p][i][j], own[p][i][j]) for j in range(3)] for i in range(3)] for p in range(2)],
        )

    def lower(d, m, h):
        def get(part, i, j):
            c = part * 6 + i * 3 + j
            if d == 1:
                return g.rows(got(("high", 1, m), (c // depth * halves + h) * SUB), -(c % depth))
            n, k = places["high", 2][1] // 3, h * 12 + c
            r = others(2).index(m) * n + k // g.ygroups * SUB
            return g.lanes(got(("high", 2), r), -NX * (k % g.ygroups))

        if (d, m, h) in fixed_slot:
            left = saved(fixed_s, fixed_slot[d, m, h])
        else:
            left = matrix(m, h)
        if d == 0:
            values = [got(("high", 0, 3), c // g.per * SUB) for c in range(10)]
            lifts = restored([g.rows(v, -depth * (c % g.per)) for c, v in enumerate(values)])
        else:
            lifts = complete_rows(get)
        q = projected(left, lifts, right_h=True)
        near = (g.row < depth, g.zrow == 0, g.lane < NX)[d]
        for c in range(8):
            add(m, c, h, jnp.where(near, q[c], 0.0))

    pair_slot = 2 + 2 * halves

    def pair_left():
        one, two = matrix(1, 0), matrix(2, 0)
        both = lambda p, i, j: jnp.where(g.row >= depth, g.rows(two[p][i][j], depth), one[p][i][j])
        save(fixed_s, pair_slot, [[[both(p, i, j) for j in range(3)] for i in range(3)] for p in range(2)])

    def pair_fix():
        def beyond(part, i, j):
            c = part * 6 + i * 3 + j
            k = c // g.ygroups
            value = g.lanes(
                g.rows(got((0, 2), 0), depth - depth * k), LANES - NX - NX * (c % g.ygroups)
            )
            return jnp.where(g.row >= depth, value, corner(0, 1, 0, c))

        own = saved(fixed_s, pair_slot)
        moved = product(own, complete_rows(beyond), right_h=True)
        edge = jnp.where(g.row >= depth, g.lane - (LANES - NX - 1), g.row - (depth - 2)) > 0
        save(
            fixed_s, pair_slot,
            [[[jnp.where(edge, moved[p][i][j], own[p][i][j]) for j in range(3)] for i in range(3)] for p in range(2)],
        )

    def pair_lower():
        lifts = restored([got(("high", 0, "pair"), c * SUB) for c in range(10)])
        q = projected(saved(fixed_s, pair_slot), lifts, right_h=True)
        for c in range(8):
            add(1, c, 0, jnp.where(g.row < depth, q[c], 0.0))
            add(2, c, 0, jnp.where(g.row < depth, g.rows(q[c], -depth), 0.0))

    def y_part():
        arrived(("low", 2))
        for h in range(halves):
            plane(2, 3, h)
        for h in range(last):
            plane(0, 2, h)

    def z_part():
        arrived(("low", 1, 3))
        for h in range(halves):
            plane(1, 3, h)

    def around_part():
        answers(2)
        for key in ((1, 0), (2, 0)):
            between = jnp.logical_not(jnp.logical_or(lowest(*CORNERS[key]), highest(*CORNERS[key])))
            pl.when(jnp.logical_and(me[0] == 0, between))(corners[key].start)
        late(0, -1, below_t)

    def rest_part():
        arrived(("low", 1, 0))
        for h in range(last):
            plane(0, 1, h)

    def high_y_part():
        arrived(("high", 2))
        for m in (3, 0):
            for h in range(halves if m else last):
                lower(2, m, h)

    def t_part():
        arrived(("low", 0, 3))
        plane(0, 3, last)

    def corner_part():
        answers(3)
        for key in ((1, 0), (2, 0)):
            pl.when(me[0] == 0)(functools.partial(late, *CORNERS[key], [corners[key]]))

    for h in range(last):
        plane(0, 3, h)
    @pl.when(even)
    def _():
        y_part()
        around_part()
        z_part()
        rest_part()
        corner_part()
        t_part()
        arrived(("low", 1, 2))
        for h in range(halves):
            plane(1, 2, h)
        high_y_part()

    @pl.when(jnp.logical_not(even))
    def _():
        z_part()
        around_part()
        rest_part()
        high_y_part()
        corner_part()
        t_part()
        y_part()
        arrived(("low", 1, 2))
        for h in range(halves):
            plane(1, 2, h)

    arrived(("low", 0, 1))
    plane(0, 1, last)
    plane(0, 2, last)
    arrived((2, 1))
    for h in range(halves):
        fix(2, 1, h)
        lower(2, 1, h)
        fix(1, 2, h)
    fix(2, 0, last)
    lower(2, 0, last)
    fix(1, 0, last)
    pair_left()
    arrived(("high", 1, 3))
    for m in (3, 0, 2):
        for h in range(halves):
            lower(1, m, h)
    arrived(("high", 0, 3))
    lower(0, 3, 0)
    arrived((0, 1))
    pair_fix()
    arrived(("high", 0, "pair"))
    pair_lower()
    remote(0, spans[-1][1], 0, 0, 1).wait_send()


def expand(halves, acc, hbm, out, sems):
    copies = []
    for m in range(4):
        for h in range(halves):
            rows = [((m * 8 + c) * halves + h) * SUB for c in range(8)]
            f = [acc[r : r + SUB, :] * (COEFF * 0.5 if c < 6 else COEFF) for c, r in enumerate(rows)]

            def put(part, i, j, value):
                out[m, part, i, j, h * SUB : (h + 1) * SUB, :] = value

            for n, (i, j) in enumerate(((0, 1), (0, 2), (1, 2))):
                put(0, i, j, f[n])
                put(0, j, i, -f[n])
                put(1, i, j, f[3 + n])
                put(1, j, i, f[3 + n])
            for i in range(3):
                put(0, i, i, jnp.zeros((SUB, LANES), jnp.float32))
            put(1, 0, 0, f[6])
            put(1, 1, 1, f[7])
            put(1, 2, 2, -(f[6] + f[7]))
        copies.append(pltpu.make_async_copy(out.at[m], hbm.at[m], sems.at[m]))
        copies[-1].start()
    for copy in copies:
        copy.wait()


def per_device(counts, links):
    time_len, depth, flat = links.shape[4:]
    sites = time_len * depth
    assert flat == LANES and SUB % depth == 0 and sites % SUB == 0 and 2 <= depth <= SUB // 2
    halves = sites // SUB
    spans = mail(depth, halves)[1]
    vmem = lambda *s: pltpu.VMEM(s + (LANES,), jnp.float32)
    shape = links.shape[:4] + (sites, flat)
    terms = pl.pallas_call(
        functools.partial(force_terms, counts, depth, halves),
        out_shape=pltpu.VMEM((32 * sites, flat), jnp.float32),
        in_specs=[pl.BlockSpec(memory_space=pl.ANY)],
        out_specs=pl.BlockSpec(memory_space=pltpu.VMEM),
        scratch_shapes=[
            vmem(*shape[:-1]),
            vmem(12 * halves, 2, 3, 3, SUB),
            vmem(6 * halves, 2, 3, 3, SUB),
            vmem(3 + 2 * halves, 2, 3, 3, SUB),
            vmem(spans[-1][1]),
            vmem(spans[-1][1]),
            pltpu.SemaphoreType.DMA((2,)),
            pltpu.SemaphoreType.DMA((1,)),
            pltpu.SemaphoreType.DMA((len(spans),)),
            pltpu.SemaphoreType.REGULAR((4,)),
        ],
        compiler_params=pltpu.CompilerParams(collective_id=0, has_side_effects=True),
        name="force_terms",
    )(links.reshape(shape))
    out = pl.pallas_call(
        functools.partial(expand, halves),
        out_shape=jax.ShapeDtypeStruct(shape, jnp.float32),
        in_specs=[pl.BlockSpec(memory_space=pltpu.VMEM)],
        out_specs=pl.BlockSpec(memory_space=pl.ANY),
        scratch_shapes=[vmem(*shape[:-1]), pltpu.SemaphoreType.DMA((4,))],
        name="expand",
    )(pltpu.with_memory_space_constraint(terms, pltpu.VMEM))
    return out.reshape(links.shape)


def solution(mesh):
    assert mesh.axis_names == ("gx", "gz", "ta")
    counts = tuple(mesh.shape[a] for a in AXES)
    spec = P(None, None, None, None, "ta", "gz", "gx")
    return jax.shard_map(
        functools.partial(per_device, counts),
        mesh=mesh,
        in_specs=(spec,),
        out_specs=spec,
        check_vma=False,
    )
```

```python
import functools

import jax
import jax.numpy as jnp
from jax import lax
from jax.experimental import pallas as pl
from jax.experimental.pallas import tpu as pltpu
from jax.sharding import PartitionSpec as P

NX = 16
COEFF = -1.9
AXES = ("ta", "gz", "gx")
SUB, LANES = 8, 128


def others(d):
    return [m for m in range(4) if m != d]


class Lattice:
    def __init__(self, depth):
        self.depth = depth
        self.per = SUB // depth
        self.ygroups = LANES // NX
        self.row = lax.broadcasted_iota(jnp.int32, (SUB, LANES), 0)
        self.lane = lax.broadcasted_iota(jnp.int32, (SUB, LANES), 1)
        self.zrow = self.row % depth
        self.xcol = self.lane % NX

    def rows(self, value, shift):
        shift %= SUB
        return pltpu.roll(value, shift, 0) if shift else value

    def lanes(self, value, shift):
        shift %= LANES
        return pltpu.roll(value, shift, 1) if shift else value


def entry(left, right, i, j, part, left_h, right_h):
    total = None
    for k in range(3):
        li = (k, i) if left_h else (i, k)
        ri = (j, k) if right_h else (k, j)
        lr, lm = left[0][li[0]][li[1]], left[1][li[0]][li[1]]
        rr, rm = right[0][ri[0]][ri[1]], right[1][ri[0]][ri[1]]
        if part == 0:
            first, second = lr * rr, lm * rm
            minus = left_h == right_h
        elif left_h:
            first, second = lr * rm, lm * rr
            minus = True
        else:
            first, second = lm * rr, lr * rm
            minus = right_h
        value = first - second if minus else first + second
        total = value if total is None else total + value
    return total


def product(left, right, left_h=False, right_h=False):
    return [
        [[entry(left, right, i, j, part, left_h, right_h) for j in range(3)] for i in range(3)]
        for part in range(2)
    ]


def projected(left, right, left_h=False, right_h=False):
    get = lambda i, j, part: entry(left, right, i, j, part, left_h, right_h)
    pairs = ((0, 1), (0, 2), (1, 2))
    real = [get(i, j, 0) - get(j, i, 0) for i, j in pairs]
    imag = [get(i, j, 1) + get(j, i, 1) for i, j in pairs]
    diag = [get(i, i, 1) for i in range(3)]
    third = (diag[0] + diag[1] + diag[2]) * (1.0 / 3.0)
    return real + imag + [diag[0] - third, diag[1] - third]


def third_row(real, imag):
    rows_r, rows_i = [], []
    for column in range(3):
        n, l = (column + 1) % 3, (column + 2) % 3
        rows_r.append(
            real[0][n] * real[1][l]
            - imag[0][n] * imag[1][l]
            - real[0][l] * real[1][n]
            + imag[0][l] * imag[1][n]
        )
        rows_i.append(
            real[0][l] * imag[1][n]
            + imag[0][l] * real[1][n]
            - real[0][n] * imag[1][l]
            - imag[0][n] * real[1][l]
        )
    return rows_r, rows_i


PLANES = ((2, 3), (1, 3), (1, 2), (0, 1), (0, 2), (0, 3))
KINDS = ({0: 1}, {1: 1}, {2: 1}, {0: 1, 1: -1}, {0: 1, 2: -1}, {1: 1, 2: -1})
CORNERS = {(0, 1): (3, 1), (1, 0): (3, -1), (0, 2): (4, 1), (2, 0): (4, -1), (1, 2): (5, 1), (2, 1): (5, -1)}
FIXED = [(0, 1, 0), (0, 2, 0), (1, 0, -1), (1, 2, None), (2, 0, -1), (2, 1, None)]


def by_largest(real, imag):
    size = [jnp.maximum(jnp.abs(r), jnp.abs(i)) for r, i in zip(real, imag)]
    first = jnp.logical_and(size[0] >= size[1], size[0] >= size[2])
    second = size[1] >= size[2]
    return lambda a, b, c: jnp.where(first, a, jnp.where(second, b, c))


def shortened(v):
    pick = by_largest(v[0:3], v[6:9])
    keep = v[0:3] + v[6:9]
    for turn in (1, 2):
        for row in (v[3:6], v[9:12]):
            keep.append(pick(*(row[(k + turn) % 3] for k in range(3))))
    return keep


def restored(v):
    real, imag = v[0:3], v[3:6]
    pick = by_largest(real, imag)
    (xr, xi), (yr, yi), (zr, zi) = (
        [pick(*(part[(k + turn) % 3] for k in range(3))) for part in (real, imag)] for turn in range(3)
    )
    pr, pi, qr, qi = v[6:10]
    sr = pr * yr + pi * yi + qr * zr + qi * zi
    si = pi * yr - pr * yi + qi * zr - qr * zi
    scale = -1.0 / (xr * xr + xi * xi)
    br, bi = (sr * xr - si * xi) * scale, (sr * xi + si * xr) * scale
    second_r = [pick(br, qr, pr), pick(pr, br, qr), pick(qr, pr, br)]
    second_i = [pick(bi, qi, pi), pick(pi, bi, qi), pick(qi, pi, bi)]
    return [[real, second_r], [imag, second_i]]


def with_third(rows):
    third_r, third_i = third_row(*rows)
    return [rows[0] + [third_r], rows[1] + [third_i]]


def mail(depth, halves):
    up = lambda a, b: -(-a // b) * SUB
    per, yg = SUB // depth, LANES // NX
    z, y = up(10 * halves, depth), up(36, yg) * halves
    short = up(10, per)
    groups = (
        ((("low", 2), y),),
        ((("low", 1, 3), z),),
        ((("low", 1, 0), z),),
        ((("low", 1, 2), z),),
        ((("high", 2), 3 * up(12 * halves, yg)),),
        ((("high", 1, 3), z), (("high", 1, 0), z), (("high", 1, 2), z), (("high", 0, 3), short)),
        ((("low", 0, 3), short), (("low", 0, 1), short), (("low", 0, 2), short)),
        (((2, 1), SUB * halves), ((1, 2), SUB * halves), ((1, 0), 2 * SUB), ((2, 0), SUB)),
        (((0, 1), 2 * SUB), ((0, 2), SUB)),
        ((("high", 0, "pair"), 10 * SUB),),
    )
    places, spans, row = {}, [], 0
    for group in groups:
        first = row
        for name, rows in group:
            places[name] = (row, rows, len(spans))
            row += rows
        spans.append((first, row))
    return places, spans


def force_terms(
    counts, depth, halves, hbm, acc,
    u, ahead_s, local_s, fixed_s, outbox, inbox, load_sem, send, recv, ready,
):
    g = Lattice(depth)
    last = halves - 1
    me = [lax.axis_index(a) for a in AXES]
    places, spans = mail(depth, halves)

    cut = last * SUB
    cut = last * SUB

    def loads(m, p, from_last):
        rows = slice(cut, None) if from_last else slice(0, cut)
        return pltpu.make_async_copy(
            hbm.at[m, p, :, :, rows], u.at[m, p, :, :, rows], load_sem.at[1 - from_last]
        )

    for from_last in (1, 0):
        for m in (0, 3, 2, 1):
            for p in range(2):
                loads(m, p, from_last).start()
    load_last, load_rest = loads(slice(None), slice(None), 1), loads(slice(None), slice(None), 0)

    def peer(kind, sign):
        where = list(me)
        for i, step in KINDS[kind].items():
            where[i] = lax.rem(me[i] + counts[i] + sign * step, counts[i])
        by = dict(zip(AXES, where))
        return (by["gx"], by["gz"], by["ta"])

    def above(axis, sign):
        rank = lambda i: i + 1 - 2 * lax.rem(i, 2) if False else i
        return rank(lax.rem(me[axis] + counts[axis] + sign, counts[axis])) > rank(me[axis])

    def lowest(kind, sign):
        tests = [above(i, sign * step) for i, step in KINDS[kind].items()]
        return functools.reduce(jnp.logical_and, tests)

    def highest(kind, sign):
        tests = [above(i, sign * step) for i, step in KINDS[kind].items()]
        return jnp.logical_not(functools.reduce(jnp.logical_or, tests))

    barrier = pltpu.get_barrier_semaphore()
    pairs = [(kind, sign) for kind in range(6) for sign in (1, -1)]
    expected = 0
    for kind, sign in pairs:
        expected = expected + jnp.where(highest(kind, sign), 1, 0)

        @pl.when(lowest(kind, sign))
        def _():
            pl.semaphore_signal(
                barrier, inc=1, device_id=peer(kind, sign), device_id_type=pl.DeviceIdType.MESH
            )

    @pl.when(expected > 0)
    def _():
        pl.semaphore_wait(barrier, expected)

    def answer_group(kind, sign):
        if kind < 3:
            return 2 if (kind, sign) == (0, -1) else 0
        return 3 if kind < 5 and sign < 0 else 1

    for kind, sign in pairs:

        @pl.when(highest(kind, sign))
        def _():
            pl.semaphore_signal(
                ready.at[answer_group(kind, -sign)], inc=1,
                device_id=peer(kind, sign), device_id_type=pl.DeviceIdType.MESH,
            )

    def answers(group):
        count = 0
        for kind, sign in pairs:
            if answer_group(kind, sign) == group:
                count = count + jnp.where(lowest(kind, sign), 1, 0)

        @pl.when(count > 0)
        def _():
            pl.semaphore_wait(ready.at[group], count)

    def start(copies):
        for copy in copies:
            copy.start()

    def early(kind, sign, copies):
        pl.when(highest(kind, sign))(lambda: start(copies))

    def late(kind, sign, copies):
        pl.when(lowest(kind, sign))(lambda: start(copies))

    def middle(kind, sign, copies):
        between = jnp.logical_not(jnp.logical_or(lowest(kind, sign), highest(kind, sign)))
        pl.when(between)(lambda: start(copies))

    def put(name, r, value):
        row = places[name][0] + r
        outbox[row : row + SUB, :] = value

    def got(name, r):
        row = places[name][0] + r
        return inbox[row : row + SUB, :]

    def load(m, part, i, j, h):
        return u[m, part, i, j, h * SUB : (h + 1) * SUB, :]

    COMPS = [(part, i, j) for part in range(2) for i in range(2) for j in range(3)]

    def comps(m):
        return [(m,) + c for c in COMPS]

    def all_comps(d):
        return [c for m in others(d) for c in comps(m)]

    def flat(value):
        return [value[part][i][j] for part, i, j in COMPS]

    def merge(values, index, step):
        total = None
        for k, x in enumerate(values):
            total = x if total is None else jnp.where(index >= step * k, x, total)
        return total

    def pack_t(m):
        v = shortened([load(*c, 0) for c in comps(m)])
        for c0 in range(0, 10, g.per):
            ks = range(min(g.per, 10 - c0))
            put(("low", 0, m), c0 // g.per * SUB, merge([g.rows(v[c0 + k], depth * k) for k in ks], g.row, depth))

    def pack_z(m):
        v = [x for h in range(halves) for x in shortened([load(*c, h) for c in comps(m)])]
        for c0 in range(0, len(v), depth):
            ks = range(min(depth, len(v) - c0))
            put(("low", 1, m), c0 // depth * SUB, merge([g.rows(v[c0 + k], k) for k in ks], g.zrow, 1))

    def pack_y():
        cs = all_comps(2)
        for c0 in range(0, len(cs), g.ygroups):
            for h in range(halves):
                ks = range(min(g.ygroups, len(cs) - c0))
                put(
                    ("low", 2), (c0 // g.ygroups * halves + h) * SUB,
                    merge([g.lanes(load(*cs[c0 + k], h), NX * k) for k in ks], g.lane, NX),
                )

    def pack_vt(v):
        v = shortened(v)
        for c0 in range(0, 10, g.per):
            ks = range(min(g.per, 10 - c0))
            put(
                ("high", 0, 3), c0 // g.per * SUB,
                merge([g.rows(v[c0 + k], depth * (k + 1)) for k in ks], g.row, depth),
            )

    def pack_pair(one, two):
        for c, (v, w) in enumerate(zip(shortened(one), shortened(two))):
            put(("high", 0, "pair"), c * SUB, jnp.where(g.row >= depth, g.rows(w, 2 * depth), g.rows(v, depth)))

    def pack_vz(m, v):
        for c0 in range(0, len(v), depth):
            ks = range(min(depth, len(v) - c0))
            put(
                ("high", 1, m), c0 // depth * SUB,
                merge([g.rows(v[c0 + k], k + 1 - depth) for k in ks], g.zrow, 1),
            )

    def got_z(side, m, h, c, row):
        n = 10 * h + c
        return g.rows(got((side, 1, m), n // depth * SUB), row - n % depth)

    def pack_vy(m, v):
        n = places["high", 2][1] // 3
        for c0 in range(0, 12 * halves, g.ygroups):
            ks = range(min(g.ygroups, 12 * halves - c0))
            put(
                ("high", 2), others(2).index(m) * n + c0 // g.ygroups * SUB,
                merge([g.lanes(v[c0 + k], NX * (k + 1)) for k in ks], g.lane, NX),
            )

    def by_groups(d, h, up, shift, index, step):
        cs = comps(d)
        return merge(
            [
                merge(
                    [
                        g.lanes(g.rows(load(*cs[c], h), shift(c // g.ygroups)), NX * (c % g.ygroups + up))
                        for c in range(c0, min(12, c0 + g.ygroups))
                    ],
                    g.lane, NX,
                )
                for c0 in range(0, 12, g.ygroups)
            ],
            index, step,
        )

    def pack_corner(d, m):
        cs = comps(d)
        if (d, m) in ((0, 1), (1, 0)):
            source = SUB - depth if d == 0 else depth - 1
            for c0 in range(0, 12, SUB):
                ks = range(min(SUB, 12 - c0))
                values = [g.rows(load(*cs[c0 + k], last if d == 0 else 0), k - source) for k in ks]
                put((d, m), c0, merge(values, g.row, 1))
        elif (d, m) == (0, 2):
            put((d, m), 0, by_groups(0, last, 0, lambda k: depth * (k + 1), g.row, depth))
        elif (d, m) == (2, 0):
            put((d, m), 0, by_groups(2, 0, 1, lambda k: depth * k, g.row, depth))
        else:
            for h in range(halves):
                up, source = (0, depth - 1) if d == 1 else (1, 0)
                put((d, m), h * SUB, by_groups(d, h, up, lambda k: k - source, g.zrow, 1))

    def corner(d, m, h, c):
        k, group = c // g.ygroups, NX * (c % g.ygroups)
        if (d, m) in ((0, 1), (1, 0)):
            target = depth - 1 if d == 0 else SUB - depth
            return g.rows(got((d, m), c // SUB * SUB), target - c % SUB)
        if (d, m) == (0, 2):
            return g.lanes(g.rows(got((d, m), 0), -depth * k), LANES - NX - group)
        if (d, m) == (2, 0):
            return g.lanes(g.rows(got((d, m), 0), SUB - depth - depth * k), -group)
        if d == 1:
            return g.lanes(g.rows(got((d, m), h * SUB), -k), LANES - NX - group)
        return g.lanes(g.rows(got((d, m), h * SUB), depth - 1 - k), -group)

    def remote(first, end, group, kind, sign):
        return pltpu.make_async_remote_copy(
            src_ref=outbox.at[first:end], dst_ref=inbox.at[first:end],
            send_sem=send.at[0], recv_sem=recv.at[group],
            device_id=peer(kind, sign), device_id_type=pl.DeviceIdType.MESH,
        )

    def message(name, kind, sign):
        first, rows, group = places[name]
        return remote(first, first + rows, group, kind, sign)

    def arrived(name):
        group = places[name][2]
        remote(*spans[group], group, 0, 1).wait_recv()

    low = {(d, m): message(("low", d, m), d, -1) for d in (0, 1) for m in others(d)}
    high = {(d, m): message(("high", d, m), d, 1) for d, m in ((0, 3), (0, "pair"), (1, 0), (1, 2), (1, 3))}
    low_y, high_y = message(("low", 2), 2, -1), message(("high", 2), 2, 1)
    corners = {key: message(key, kind, sign) for key, (kind, sign) in CORNERS.items()}

    def matrix(m, h):
        return [[[load(m, part, i, j, h) for j in range(3)] for i in range(3)] for part in range(2)]

    def save(ref, index, value):
        for part in range(2):
            for i in range(len(value[part])):
                for j in range(3):
                    ref[index, part, i, j] = value[part][i][j]

    def saved(ref, index, rows=3):
        return [[[ref[index, part, i, j] for j in range(3)] for i in range(rows)] for part in range(2)]

    def rolled(m, d, h, part, i, j):
        v = load(m, part, i, j, h)
        if d == 3:
            return jnp.where(g.xcol == NX - 1, g.lanes(v, NX - 1), g.lanes(v, -1))
        if d == 2:
            return g.lanes(v, -NX)
        if d == 1:
            return g.rows(v, -1)
        if h + 1 < halves:
            beyond = g.rows(load(m, part, i, j, h + 1), -depth)
            return jnp.where(g.row >= SUB - depth, beyond, g.rows(v, -depth))
        return g.rows(v, -depth)

    def complete(d, h):
        return d == 3 or (d == 0 and h + 1 < halves)

    def far_edge(d):
        return (g.row >= SUB - depth, g.zrow == depth - 1, g.lane >= LANES - NX)[d]

    ahead_slot = {}

    def prepare(m, d, h, rows):
        value = [
            [[rolled(m, d, h, part, i, j) for j in range(3)] for i in range(3 if rows == 3 or complete(d, h) else 2)]
            for part in range(2)
        ]
        ahead_slot[m, d, h] = len(ahead_slot)
        keep = 3 if complete(d, h) else 2
        save(ahead_s, ahead_slot[m, d, h], [part[:keep] for part in value])
        return value

    def transported(b, m, d, h, b_h):
        moved = prepare(m, d, h, 3)
        value = [
            [[entry(b, moved, i, j, part, b_h, False) for j in range(3)] for i in range(2)]
            for part in range(2)
        ]
        if not complete(d, h):
            edge = far_edge(d)
            for part in range(2):
                for i in range(2):
                    for j in range(3):
                        own = b[part][j][i] if b_h else b[part][i][j]
                        own = -own if b_h and part else own
                        value[part][i][j] = jnp.where(edge, own, value[part][i][j])
        return flat(value)

    local = {}

    def local_product(mu, nu, h):
        b = product(matrix(mu, h), matrix(nu, h), left_h=True)
        save(local_s, PLANES.index((mu, nu)) * halves + h, b)
        return b

    below_t, below_z = [low[0, m] for m in (3, 1, 2)], [low[1, m] for m in (3, 0, 2)]
    above_t = [high[0, 3], high[0, "pair"]]
    even = lax.rem(me[2], 2) == 0
    at_end = me[0] == counts[0] - 1

    def faces():
        load_rest.wait()
        for m in (3, 1, 2):
            pack_t(m)
        pl.when(jnp.logical_not(at_end))(lambda: early(0, -1, below_t))
        for m in (3, 0, 2):
            pack_z(m)
        early(1, -1, below_z)
        pack_y()
        early(2, -1, [low_y])

    acc[...] = jnp.zeros_like(acc)
    load_last.wait()
    for d in (1, 2):
        pack_corner(0, d)
        early(*CORNERS[0, d], [corners[0, d]])
    pl.when(jnp.logical_not(at_end))(faces)
    pack_vt(transported(local_product(0, 3, last), 0, 3, last, False))
    early(0, 1, [high[0, 3]])
    pack_pair(*(transported(local_product(0, m, last), 0, m, last, False) for m in (1, 2)))
    early(0, 1, [high[0, "pair"]])
    pl.when(at_end)(faces)
    for key in ((1, 0), (2, 0), (1, 2), (2, 1)):
        pack_corner(*key)
    for key in ((1, 0), (2, 0), (1, 2), (2, 1)):
        early(*CORNERS[key], [corners[key]])

    lifted = {}

    def lift(mu, nu):
        for h in range(halves):
            if mu == 0 and h == last:
                b = saved(local_s, PLANES.index((mu, nu)) * halves + h)
            else:
                b = local_product(mu, nu, h)
            if mu:
                lifted[mu, nu, h] = transported(b, mu, nu, h, False)
            elif h != last:
                prepare(mu, nu, h, 2)
            if nu != 3:
                lifted[nu, mu, h] = transported(b, nu, mu, h, True)
            else:
                prepare(nu, mu, h, 2)
        for d, m in ((mu, nu), (nu, mu)):
            if d == 1:
                pack_vz(m, [x for h in range(halves) for x in shortened(lifted[d, m, h])])
            elif d == 2:
                pack_vy(m, [x for h in range(halves) for x in lifted[d, m, h]])

    def greeted():
        answers(0)
        late(2, -1, [low_y])
        for key in ((0, 1), (0, 2), (1, 2), (2, 1)):
            middle(*CORNERS[key], [corners[key]])
        pl.when(at_end)(lambda: start(below_t))
        late(1, -1, below_z)
        late(0, 1, above_t)
        for key in ((1, 0), (2, 0)):
            between = jnp.logical_and(me[0] > 0, jnp.logical_not(highest(*CORNERS[key])))
            pl.when(between)(corners[key].start)

    pl.when(at_end)(greeted)
    lift(1, 3)
    lift(0, 1)
    lift(1, 2)
    pl.when(jnp.logical_not(at_end))(greeted)
    above_z = [high[1, m] for m in (3, 0, 2)]
    start(above_z)
    lift(2, 3)
    lift(0, 2)
    high_y.start()
    lift(0, 3)
    answers(1)
    for key in ((0, 1), (0, 2), (1, 2), (2, 1)):
        late(*CORNERS[key], [corners[key]])

    def ahead(m, d, h):
        if complete(d, h):
            return saved(ahead_s, ahead_slot[m, d, h])
        index = {c: n for n, c in enumerate(all_comps(d))}
        if d == 1:
            edges = restored([got_z("low", m, h, c, depth - 1) for c in range(10)])
        elif d == 0:
            values = [got(("low", 0, m), c // g.per * SUB) for c in range(10)]
            edges = restored(
                [g.rows(v, SUB - depth - depth * (c % g.per)) for c, v in enumerate(values)]
            )

        def get(part, i, j):
            v = ahead_s[ahead_slot[m, d, h], part, i, j]
            c = index[(m, part, i, j)]
            if d < 2:
                edge = edges[part][i][j]
            else:
                edge = g.lanes(
                    got(("low", 2), (c // g.ygroups * halves + h) * SUB), LANES - NX - NX * (c % g.ygroups)
                )
            return jnp.where(far_edge(d), edge, v)

        return complete_rows(get)

    def complete_rows(get):
        real = [[get(0, i, j) for j in range(3)] for i in range(2)]
        imag = [[get(1, i, j) for j in range(3)] for i in range(2)]
        third_r, third_i = third_row(real, imag)
        return [real + [third_r], imag + [third_i]]

    def add(m, c, h, value):
        r = ((m * 8 + c) * halves + h) * SUB
        acc[r : r + SUB, :] += value

    def shifted(q, d):
        if d == 3:
            return jnp.where(g.xcol == 0, g.lanes(q, 1 - NX), g.lanes(q, 1))
        if d == 2:
            return jnp.where(g.lane >= NX, g.lanes(q, NX), 0.0)
        if d == 1:
            return jnp.where(g.zrow > 0, g.rows(q, 1), 0.0)
        return jnp.where(g.row >= depth, g.rows(q, depth), 0.0)

    def plane(mu, nu, h):
        a = product(ahead(nu, mu, h), ahead(mu, nu, h), right_h=True)
        b = saved(local_s, PLANES.index((mu, nu)) * halves + h)
        e = product(matrix(mu, h), a)
        upper = projected(e, matrix(nu, h), right_h=True)
        q = projected(a, b, left_h=True)
        for c in range(8):
            add(mu, c, h, shifted(q[c], nu) + upper[c])
        q = projected(a, b, right_h=True)
        for c in range(8):
            add(nu, c, h, shifted(q[c], mu) - upper[c])
            if mu == 0 and h + 1 < halves:
                add(nu, c, h + 1, jnp.where(g.row < depth, g.rows(q[c], depth), 0.0))

    fixed_slot = {}

    def fix(d, m, h):
        beyond = complete_rows(lambda part, i, j: corner(d, m, h, part * 6 + i * 3 + j))
        own = matrix(m, h)
        moved = product(own, beyond, right_h=True)
        edge = far_edge(m)
        fixed_slot[d, m, h] = len(fixed_slot)
        save(
            fixed_s, fixed_slot[d, m, h],
            [[[jnp.where(edge, moved[p][i][j], own[p][i][j]) for j in range(3)] for i in range(3)] for p in range(2)],
        )

    def lower(d, m, h):
        def get(part, i, j):
            c = part * 6 + i * 3 + j
            n, k = places["high", 2][1] // 3, h * 12 + c
            r = others(2).index(m) * n + k // g.ygroups * SUB
            return g.lanes(got(("high", 2), r), -NX * (k % g.ygroups))

        if (d, m, h) in fixed_slot:
            left = saved(fixed_s, fixed_slot[d, m, h])
        else:
            left = matrix(m, h)
        if d == 0:
            values = [got(("high", 0, 3), c // g.per * SUB) for c in range(10)]
            lifts = with_third(restored([g.rows(v, -depth * (c % g.per)) for c, v in enumerate(values)]))
        elif d == 1:
            lifts = with_third(restored([got_z("high", m, h, c, 0) for c in range(10)]))
        else:
            lifts = complete_rows(get)
        q = projected(left, lifts, right_h=True)
        near = (g.row < depth, g.zrow == 0, g.lane < NX)[d]
        for c in range(8):
            add(m, c, h, jnp.where(near, q[c], 0.0))

    pair_slot = 2 + 2 * halves

    def pair_left():
        one, two = matrix(1, 0), matrix(2, 0)
        both = lambda p, i, j: jnp.where(g.row >= depth, g.rows(two[p][i][j], depth), one[p][i][j])
        save(fixed_s, pair_slot, [[[both(p, i, j) for j in range(3)] for i in range(3)] for p in range(2)])

    def pair_fix():
        def beyond(part, i, j):
            c = part * 6 + i * 3 + j
            k = c // g.ygroups
            value = g.lanes(
                g.rows(got((0, 2), 0), depth - depth * k), LANES - NX - NX * (c % g.ygroups)
            )
            return jnp.where(g.row >= depth, value, corner(0, 1, 0, c))

        own = saved(fixed_s, pair_slot)
        moved = product(own, complete_rows(beyond), right_h=True)
        edge = jnp.where(g.row >= depth, g.lane - (LANES - NX - 1), g.row - (depth - 2)) > 0
        save(
            fixed_s, pair_slot,
            [[[jnp.where(edge, moved[p][i][j], own[p][i][j]) for j in range(3)] for i in range(3)] for p in range(2)],
        )

    def pair_lower():
        lifts = with_third(restored([got(("high", 0, "pair"), c * SUB) for c in range(10)]))
        q = projected(saved(fixed_s, pair_slot), lifts, right_h=True)
        for c in range(8):
            add(1, c, 0, jnp.where(g.row < depth, q[c], 0.0))
            add(2, c, 0, jnp.where(g.row < depth, g.rows(q[c], -depth), 0.0))

    def y_part():
        arrived(("low", 2))
        for h in range(halves):
            plane(2, 3, h)
        for h in range(last):
            plane(0, 2, h)

    def z_part():
        arrived(("low", 1, 3))
        for h in range(halves):
            plane(1, 3, h)

    def around_part():
        answers(2)
        for key in ((1, 0), (2, 0)):
            between = jnp.logical_not(jnp.logical_or(lowest(*CORNERS[key]), highest(*CORNERS[key])))
            pl.when(jnp.logical_and(me[0] == 0, between))(corners[key].start)
        late(0, -1, below_t)

    def rest_part():
        arrived(("low", 1, 0))
        for h in range(last):
            plane(0, 1, h)

    def high_y_part():
        arrived(("high", 2))
        for m in (3, 0):
            for h in range(halves if m else last):
                lower(2, m, h)

    def t_part():
        arrived(("low", 0, 3))
        plane(0, 3, last)
        plane(0, 1, last)

    def corner_part():
        answers(3)
        for key in ((1, 0), (2, 0)):
            pl.when(me[0] == 0)(functools.partial(late, *CORNERS[key], [corners[key]]))

    for h in range(last):
        plane(0, 3, h)
    def cross_part():
        arrived(("low", 1, 2))
        for h in range(halves):
            plane(1, 2, h)

    near = me[0] == 0

    @pl.when(even)
    def _():
        y_part()
        around_part()
        z_part()
        rest_part()
        pl.when(near)(t_part)
        corner_part()
        cross_part()
        high_y_part()
        pl.when(jnp.logical_not(near))(t_part)

    @pl.when(jnp.logical_not(even))
    def _():
        z_part()
        around_part()
        rest_part()
        high_y_part()
        pl.when(near)(t_part)
        corner_part()
        y_part()
        cross_part()
        pl.when(jnp.logical_not(near))(t_part)

    plane(0, 2, last)
    arrived((2, 1))
    for h in range(halves):
        fix(2, 1, h)
        lower(2, 1, h)
        fix(1, 2, h)
    fix(2, 0, last)
    lower(2, 0, last)
    fix(1, 0, last)
    pair_left()
    arrived(("high", 1, 3))
    for m in (3, 0, 2):
        for h in range(halves):
            lower(1, m, h)
    lower(0, 3, 0)
    arrived((0, 1))
    pair_fix()
    arrived(("high", 0, "pair"))
    pair_lower()
    remote(0, spans[-1][1], 0, 0, 1).wait_send()


def expand(halves, acc, hbm, out, sems):
    copies = []
    for m in range(4):
        for h in range(halves):
            rows = [((m * 8 + c) * halves + h) * SUB for c in range(8)]
            f = [acc[r : r + SUB, :] * (COEFF * 0.5 if c < 6 else COEFF) for c, r in enumerate(rows)]

            def put(part, i, j, value):
                out[m, part, i, j, h * SUB : (h + 1) * SUB, :] = value

            for n, (i, j) in enumerate(((0, 1), (0, 2), (1, 2))):
                put(0, i, j, f[n])
                put(0, j, i, -f[n])
                put(1, i, j, f[3 + n])
                put(1, j, i, f[3 + n])
            for i in range(3):
                put(0, i, i, jnp.zeros((SUB, LANES), jnp.float32))
            put(1, 0, 0, f[6])
            put(1, 1, 1, f[7])
            put(1, 2, 2, -(f[6] + f[7]))
        copies.append(pltpu.make_async_copy(out.at[m], hbm.at[m], sems.at[m]))
        copies[-1].start()
    for copy in copies:
        copy.wait()


def per_device(counts, links):
    time_len, depth, flat = links.shape[4:]
    sites = time_len * depth
    assert flat == LANES and SUB % depth == 0 and sites % SUB == 0 and 2 <= depth <= SUB // 2
    halves = sites // SUB
    spans = mail(depth, halves)[1]
    vmem = lambda *s: pltpu.VMEM(s + (LANES,), jnp.float32)
    shape = links.shape[:4] + (sites, flat)
    terms = pl.pallas_call(
        functools.partial(force_terms, counts, depth, halves),
        out_shape=pltpu.VMEM((32 * sites, flat), jnp.float32),
        in_specs=[pl.BlockSpec(memory_space=pl.ANY)],
        out_specs=pl.BlockSpec(memory_space=pltpu.VMEM),
        scratch_shapes=[
            vmem(*shape[:-1]),
            vmem(12 * halves, 2, 3, 3, SUB),
            vmem(6 * halves, 2, 3, 3, SUB),
            vmem(3 + 2 * halves, 2, 3, 3, SUB),
            vmem(spans[-1][1]),
            vmem(spans[-1][1]),
            pltpu.SemaphoreType.DMA((2,)),
            pltpu.SemaphoreType.DMA((1,)),
            pltpu.SemaphoreType.DMA((len(spans),)),
            pltpu.SemaphoreType.REGULAR((4,)),
        ],
        compiler_params=pltpu.CompilerParams(collective_id=0, has_side_effects=True),
        name="force_terms",
    )(links.reshape(shape))
    out = pl.pallas_call(
        functools.partial(expand, halves),
        out_shape=jax.ShapeDtypeStruct(shape, jnp.float32),
        in_specs=[pl.BlockSpec(memory_space=pltpu.VMEM)],
        out_specs=pl.BlockSpec(memory_space=pl.ANY),
        scratch_shapes=[vmem(*shape[:-1]), pltpu.SemaphoreType.DMA((4,))],
        name="expand",
    )(pltpu.with_memory_space_constraint(terms, pltpu.VMEM))
    return out.reshape(links.shape)


def solution(mesh):
    assert mesh.axis_names == ("gx", "gz", "ta")
    counts = tuple(mesh.shape[a] for a in AXES)
    spec = P(None, None, None, None, "ta", "gz", "gx")
    return jax.shard_map(
        functools.partial(per_device, counts),
        mesh=mesh,
        in_specs=(spec,),
        out_specs=spec,
        check_vma=False,
    )
```

```python
import functools

import jax
import jax.numpy as jnp
from jax import lax
from jax.experimental import pallas as pl
from jax.experimental.pallas import tpu as pltpu
from jax.sharding import PartitionSpec as P

NX = 16
COEFF = -1.9
AXES = ("ta", "gz", "gx")
SUB, LANES = 8, 128


def others(d):
    return [m for m in range(4) if m != d]


class Lattice:
    def __init__(self, depth):
        self.depth = depth
        self.per = SUB // depth
        self.ygroups = LANES // NX
        self.row = lax.broadcasted_iota(jnp.int32, (SUB, LANES), 0)
        self.lane = lax.broadcasted_iota(jnp.int32, (SUB, LANES), 1)
        self.zrow = self.row % depth
        self.xcol = self.lane % NX

    def rows(self, value, shift):
        shift %= SUB
        return pltpu.roll(value, shift, 0) if shift else value

    def lanes(self, value, shift):
        shift %= LANES
        return pltpu.roll(value, shift, 1) if shift else value


def entry(left, right, i, j, part, left_h, right_h):
    total = None
    for k in range(3):
        li = (k, i) if left_h else (i, k)
        ri = (j, k) if right_h else (k, j)
        lr, lm = left[0][li[0]][li[1]], left[1][li[0]][li[1]]
        rr, rm = right[0][ri[0]][ri[1]], right[1][ri[0]][ri[1]]
        if part == 0:
            first, second = lr * rr, lm * rm
            minus = left_h == right_h
        elif left_h:
            first, second = lr * rm, lm * rr
            minus = True
        else:
            first, second = lm * rr, lr * rm
            minus = right_h
        value = first - second if minus else first + second
        total = value if total is None else total + value
    return total


def product(left, right, left_h=False, right_h=False):
    return [
        [[entry(left, right, i, j, part, left_h, right_h) for j in range(3)] for i in range(3)]
        for part in range(2)
    ]


def projected(left, right, left_h=False, right_h=False):
    get = lambda i, j, part: entry(left, right, i, j, part, left_h, right_h)
    pairs = ((0, 1), (0, 2), (1, 2))
    real = [get(i, j, 0) - get(j, i, 0) for i, j in pairs]
    imag = [get(i, j, 1) + get(j, i, 1) for i, j in pairs]
    diag = [get(i, i, 1) for i in range(3)]
    third = (diag[0] + diag[1] + diag[2]) * (1.0 / 3.0)
    return real + imag + [diag[0] - third, diag[1] - third]


def third_row(real, imag):
    rows_r, rows_i = [], []
    for column in range(3):
        n, l = (column + 1) % 3, (column + 2) % 3
        rows_r.append(
            real[0][n] * real[1][l]
            - imag[0][n] * imag[1][l]
            - real[0][l] * real[1][n]
            + imag[0][l] * imag[1][n]
        )
        rows_i.append(
            real[0][l] * imag[1][n]
            + imag[0][l] * real[1][n]
            - real[0][n] * imag[1][l]
            - imag[0][n] * real[1][l]
        )
    return rows_r, rows_i


PLANES = ((2, 3), (1, 3), (1, 2), (0, 1), (0, 2), (0, 3))
KINDS = ({0: 1}, {1: 1}, {2: 1}, {0: 1, 1: -1}, {0: 1, 2: -1}, {1: 1, 2: -1})
CORNERS = {(0, 1): (3, 1), (1, 0): (3, -1), (0, 2): (4, 1), (2, 0): (4, -1), (1, 2): (5, 1), (2, 1): (5, -1)}
FIXED = [(0, 1, 0), (0, 2, 0), (1, 0, -1), (1, 2, None), (2, 0, -1), (2, 1, None)]


def by_largest(real, imag):
    size = [jnp.maximum(jnp.abs(r), jnp.abs(i)) for r, i in zip(real, imag)]
    first = jnp.logical_and(size[0] >= size[1], size[0] >= size[2])
    second = size[1] >= size[2]
    return lambda a, b, c: jnp.where(first, a, jnp.where(second, b, c))


def shortened(v):
    pick = by_largest(v[0:3], v[6:9])
    keep = v[0:3] + v[6:9]
    for turn in (1, 2):
        for row in (v[3:6], v[9:12]):
            keep.append(pick(*(row[(k + turn) % 3] for k in range(3))))
    return keep


def restored(v):
    real, imag = v[0:3], v[3:6]
    pick = by_largest(real, imag)
    (xr, xi), (yr, yi), (zr, zi) = (
        [pick(*(part[(k + turn) % 3] for k in range(3))) for part in (real, imag)] for turn in range(3)
    )
    pr, pi, qr, qi = v[6:10]
    sr = pr * yr + pi * yi + qr * zr + qi * zi
    si = pi * yr - pr * yi + qi * zr - qr * zi
    scale = -1.0 / (xr * xr + xi * xi)
    br, bi = (sr * xr - si * xi) * scale, (sr * xi + si * xr) * scale
    second_r = [pick(br, qr, pr), pick(pr, br, qr), pick(qr, pr, br)]
    second_i = [pick(bi, qi, pi), pick(pi, bi, qi), pick(qi, pi, bi)]
    return [[real, second_r], [imag, second_i]]


def with_third(rows):
    third_r, third_i = third_row(*rows)
    return [rows[0] + [third_r], rows[1] + [third_i]]


def mail(depth, halves):
    up = lambda a, b: -(-a // b) * SUB
    per, yg = SUB // depth, LANES // NX
    z, y = up(10 * halves, depth), up(36, yg) * halves
    short = up(10, per)
    groups = (
        ((("low", 2), y),),
        ((("low", 1, 3), z),),
        ((("low", 1, 0), z),),
        ((("low", 1, 2), z),),
        ((("high", 2), 3 * up(12 * halves, yg)),),
        ((("high", 1, 3), z), (("high", 1, 0), z), (("high", 1, 2), z), (("high", 0, 3), short)),
        ((("low", 0, 3), short), (("low", 0, 1), short), (("low", 0, 2), short)),
        (((2, 1), SUB * halves), ((1, 2), SUB * halves), ((1, 0), 2 * SUB), ((2, 0), SUB)),
        (((0, 1), 2 * SUB), ((0, 2), SUB)),
        ((("high", 0, "pair"), 10 * SUB),),
    )
    places, spans, row = {}, [], 0
    for group in groups:
        first = row
        for name, rows in group:
            places[name] = (row, rows, len(spans))
            row += rows
        spans.append((first, row))
    return places, spans


def force_terms(
    counts, depth, halves, hbm, acc,
    u, ahead_s, local_s, fixed_s, outbox, inbox, load_sem, send, recv, ready,
):
    g = Lattice(depth)
    last = halves - 1
    me = [lax.axis_index(a) for a in AXES]
    places, spans = mail(depth, halves)

    cut = last * SUB
    cut = last * SUB

    def loads(m, p, from_last, sem):
        rows = slice(cut, None) if from_last else slice(0, cut)
        return pltpu.make_async_copy(
            hbm.at[m, p, :, :, rows], u.at[m, p, :, :, rows], load_sem.at[sem]
        )

    for from_last in (True, False):
        for m in (0, 3, 2, 1):
            for p in range(2):
                loads(m, p, from_last, (1 if m else 0) if from_last else 2).start()
    load_time = loads(0, slice(None), True, 0)
    load_last = loads(slice(1, None), slice(None), True, 1)
    load_rest = loads(slice(None), slice(None), False, 2)

    def peer(kind, sign):
        where = list(me)
        for i, step in KINDS[kind].items():
            where[i] = lax.rem(me[i] + counts[i] + sign * step, counts[i])
        by = dict(zip(AXES, where))
        return (by["gx"], by["gz"], by["ta"])

    def above(axis, sign):
        rank = lambda i: i + 1 - 2 * lax.rem(i, 2) if False else i
        return rank(lax.rem(me[axis] + counts[axis] + sign, counts[axis])) > rank(me[axis])

    def lowest(kind, sign):
        tests = [above(i, sign * step) for i, step in KINDS[kind].items()]
        return functools.reduce(jnp.logical_and, tests)

    def highest(kind, sign):
        tests = [above(i, sign * step) for i, step in KINDS[kind].items()]
        return jnp.logical_not(functools.reduce(jnp.logical_or, tests))

    barrier = pltpu.get_barrier_semaphore()
    pairs = [(kind, sign) for kind in range(6) for sign in (1, -1)]
    expected = 0
    for kind, sign in pairs:
        expected = expected + jnp.where(highest(kind, sign), 1, 0)

        @pl.when(lowest(kind, sign))
        def _():
            pl.semaphore_signal(
                barrier, inc=1, device_id=peer(kind, sign), device_id_type=pl.DeviceIdType.MESH
            )

    @pl.when(expected > 0)
    def _():
        pl.semaphore_wait(barrier, expected)

    def answer_group(kind, sign):
        if kind < 3:
            return 2 if (kind, sign) == (0, -1) else 0
        return 3 if kind < 5 and sign < 0 else 1

    for kind, sign in pairs:

        @pl.when(highest(kind, sign))
        def _():
            pl.semaphore_signal(
                ready.at[answer_group(kind, -sign)], inc=1,
                device_id=peer(kind, sign), device_id_type=pl.DeviceIdType.MESH,
            )

    def answers(group):
        count = 0
        for kind, sign in pairs:
            if answer_group(kind, sign) == group:
                count = count + jnp.where(lowest(kind, sign), 1, 0)

        @pl.when(count > 0)
        def _():
            pl.semaphore_wait(ready.at[group], count)

    def start(copies):
        for copy in copies:
            copy.start()

    def early(kind, sign, copies):
        pl.when(highest(kind, sign))(lambda: start(copies))

    def late(kind, sign, copies):
        pl.when(lowest(kind, sign))(lambda: start(copies))

    def middle(kind, sign, copies):
        between = jnp.logical_not(jnp.logical_or(lowest(kind, sign), highest(kind, sign)))
        pl.when(between)(lambda: start(copies))

    def put(name, r, value):
        row = places[name][0] + r
        outbox[row : row + SUB, :] = value

    def got(name, r):
        row = places[name][0] + r
        return inbox[row : row + SUB, :]

    def load(m, part, i, j, h):
        return u[m, part, i, j, h * SUB : (h + 1) * SUB, :]

    COMPS = [(part, i, j) for part in range(2) for i in range(2) for j in range(3)]

    def comps(m):
        return [(m,) + c for c in COMPS]

    def all_comps(d):
        return [c for m in others(d) for c in comps(m)]

    def flat(value):
        return [value[part][i][j] for part, i, j in COMPS]

    def merge(values, index, step):
        total = None
        for k, x in enumerate(values):
            total = x if total is None else jnp.where(index >= step * k, x, total)
        return total

    def pack_t(m):
        v = shortened([load(*c, 0) for c in comps(m)])
        for c0 in range(0, 10, g.per):
            ks = range(min(g.per, 10 - c0))
            put(("low", 0, m), c0 // g.per * SUB, merge([g.rows(v[c0 + k], depth * k) for k in ks], g.row, depth))

    def pack_z(m):
        v = [x for h in range(halves) for x in shortened([load(*c, h) for c in comps(m)])]
        for c0 in range(0, len(v), depth):
            ks = range(min(depth, len(v) - c0))
            put(("low", 1, m), c0 // depth * SUB, merge([g.rows(v[c0 + k], k) for k in ks], g.zrow, 1))

    def pack_y():
        cs = all_comps(2)
        for c0 in range(0, len(cs), g.ygroups):
            for h in range(halves):
                ks = range(min(g.ygroups, len(cs) - c0))
                put(
                    ("low", 2), (c0 // g.ygroups * halves + h) * SUB,
                    merge([g.lanes(load(*cs[c0 + k], h), NX * k) for k in ks], g.lane, NX),
                )

    def pack_vt(v):
        v = shortened(v)
        for c0 in range(0, 10, g.per):
            ks = range(min(g.per, 10 - c0))
            put(
                ("high", 0, 3), c0 // g.per * SUB,
                merge([g.rows(v[c0 + k], depth * (k + 1)) for k in ks], g.row, depth),
            )

    def pack_pair(one, two):
        for c, (v, w) in enumerate(zip(shortened(one), shortened(two))):
            put(("high", 0, "pair"), c * SUB, jnp.where(g.row >= depth, g.rows(w, 2 * depth), g.rows(v, depth)))

    def pack_vz(m, v):
        for c0 in range(0, len(v), depth):
            ks = range(min(depth, len(v) - c0))
            put(
                ("high", 1, m), c0 // depth * SUB,
                merge([g.rows(v[c0 + k], k + 1 - depth) for k in ks], g.zrow, 1),
            )

    def got_z(side, m, h, c, row):
        n = 10 * h + c
        return g.rows(got((side, 1, m), n // depth * SUB), row - n % depth)

    def pack_vy(m, v):
        n = places["high", 2][1] // 3
        for c0 in range(0, 12 * halves, g.ygroups):
            ks = range(min(g.ygroups, 12 * halves - c0))
            put(
                ("high", 2), others(2).index(m) * n + c0 // g.ygroups * SUB,
                merge([g.lanes(v[c0 + k], NX * (k + 1)) for k in ks], g.lane, NX),
            )

    def by_groups(d, h, up, shift, index, step):
        cs = comps(d)
        return merge(
            [
                merge(
                    [
                        g.lanes(g.rows(load(*cs[c], h), shift(c // g.ygroups)), NX * (c % g.ygroups + up))
                        for c in range(c0, min(12, c0 + g.ygroups))
                    ],
                    g.lane, NX,
                )
                for c0 in range(0, 12, g.ygroups)
            ],
            index, step,
        )

    def pack_corner(d, m):
        cs = comps(d)
        if (d, m) in ((0, 1), (1, 0)):
            source = SUB - depth if d == 0 else depth - 1
            for c0 in range(0, 12, SUB):
                ks = range(min(SUB, 12 - c0))
                values = [g.rows(load(*cs[c0 + k], last if d == 0 else 0), k - source) for k in ks]
                put((d, m), c0, merge(values, g.row, 1))
        elif (d, m) == (0, 2):
            put((d, m), 0, by_groups(0, last, 0, lambda k: depth * (k + 1), g.row, depth))
        elif (d, m) == (2, 0):
            put((d, m), 0, by_groups(2, 0, 1, lambda k: depth * k, g.row, depth))
        else:
            for h in range(halves):
                up, source = (0, depth - 1) if d == 1 else (1, 0)
                put((d, m), h * SUB, by_groups(d, h, up, lambda k: k - source, g.zrow, 1))

    def corner(d, m, h, c):
        k, group = c // g.ygroups, NX * (c % g.ygroups)
        if (d, m) in ((0, 1), (1, 0)):
            target = depth - 1 if d == 0 else SUB - depth
            return g.rows(got((d, m), c // SUB * SUB), target - c % SUB)
        if (d, m) == (0, 2):
            return g.lanes(g.rows(got((d, m), 0), -depth * k), LANES - NX - group)
        if (d, m) == (2, 0):
            return g.lanes(g.rows(got((d, m), 0), SUB - depth - depth * k), -group)
        if d == 1:
            return g.lanes(g.rows(got((d, m), h * SUB), -k), LANES - NX - group)
        return g.lanes(g.rows(got((d, m), h * SUB), depth - 1 - k), -group)

    def remote(first, end, group, kind, sign):
        return pltpu.make_async_remote_copy(
            src_ref=outbox.at[first:end], dst_ref=inbox.at[first:end],
            send_sem=send.at[0], recv_sem=recv.at[group],
            device_id=peer(kind, sign), device_id_type=pl.DeviceIdType.MESH,
        )

    def message(name, kind, sign):
        first, rows, group = places[name]
        return remote(first, first + rows, group, kind, sign)

    def arrived(name):
        group = places[name][2]
        remote(*spans[group], group, 0, 1).wait_recv()

    low = {(d, m): message(("low", d, m), d, -1) for d in (0, 1) for m in others(d)}
    high = {(d, m): message(("high", d, m), d, 1) for d, m in ((0, 3), (0, "pair"), (1, 0), (1, 2), (1, 3))}
    low_y, high_y = message(("low", 2), 2, -1), message(("high", 2), 2, 1)
    corners = {key: message(key, kind, sign) for key, (kind, sign) in CORNERS.items()}

    def matrix(m, h):
        return [[[load(m, part, i, j, h) for j in range(3)] for i in range(3)] for part in range(2)]

    def save(ref, index, value):
        for part in range(2):
            for i in range(len(value[part])):
                for j in range(3):
                    ref[index, part, i, j] = value[part][i][j]

    def saved(ref, index, rows=3):
        return [[[ref[index, part, i, j] for j in range(3)] for i in range(rows)] for part in range(2)]

    def rolled(m, d, h, part, i, j):
        v = load(m, part, i, j, h)
        if d == 3:
            return jnp.where(g.xcol == NX - 1, g.lanes(v, NX - 1), g.lanes(v, -1))
        if d == 2:
            return g.lanes(v, -NX)
        if d == 1:
            return g.rows(v, -1)
        if h + 1 < halves:
            beyond = g.rows(load(m, part, i, j, h + 1), -depth)
            return jnp.where(g.row >= SUB - depth, beyond, g.rows(v, -depth))
        return g.rows(v, -depth)

    def complete(d, h):
        return d == 3 or (d == 0 and h + 1 < halves)

    def far_edge(d):
        return (g.row >= SUB - depth, g.zrow == depth - 1, g.lane >= LANES - NX)[d]

    ahead_slot = {}

    def prepare(m, d, h, rows):
        value = [
            [[rolled(m, d, h, part, i, j) for j in range(3)] for i in range(3 if rows == 3 or complete(d, h) else 2)]
            for part in range(2)
        ]
        ahead_slot[m, d, h] = len(ahead_slot)
        keep = 3 if complete(d, h) else 2
        save(ahead_s, ahead_slot[m, d, h], [part[:keep] for part in value])
        return value

    def transported(b, m, d, h, b_h):
        moved = prepare(m, d, h, 3)
        value = [
            [[entry(b, moved, i, j, part, b_h, False) for j in range(3)] for i in range(2)]
            for part in range(2)
        ]
        if not complete(d, h):
            edge = far_edge(d)
            for part in range(2):
                for i in range(2):
                    for j in range(3):
                        own = b[part][j][i] if b_h else b[part][i][j]
                        own = -own if b_h and part else own
                        value[part][i][j] = jnp.where(edge, own, value[part][i][j])
        return flat(value)

    local = {}

    def local_product(mu, nu, h):
        b = product(matrix(mu, h), matrix(nu, h), left_h=True)
        save(local_s, PLANES.index((mu, nu)) * halves + h, b)
        return b

    below_t, below_z = [low[0, m] for m in (3, 1, 2)], [low[1, m] for m in (3, 0, 2)]
    above_t = [high[0, 3], high[0, "pair"]]
    even = lax.rem(me[2], 2) == 0
    at_end = me[0] == counts[0] - 1

    def faces():
        load_rest.wait()
        for m in (3, 1, 2):
            pack_t(m)
        pl.when(jnp.logical_not(at_end))(lambda: early(0, -1, below_t))
        for m in (3, 0, 2):
            pack_z(m)
        early(1, -1, below_z)
        pack_y()
        early(2, -1, [low_y])

    acc[...] = jnp.zeros_like(acc)
    load_time.wait()
    for d in (1, 2):
        pack_corner(0, d)
        early(*CORNERS[0, d], [corners[0, d]])
    load_last.wait()
    pl.when(jnp.logical_not(at_end))(faces)
    pack_vt(transported(local_product(0, 3, last), 0, 3, last, False))
    early(0, 1, [high[0, 3]])
    pack_pair(*(transported(local_product(0, m, last), 0, m, last, False) for m in (1, 2)))
    early(0, 1, [high[0, "pair"]])
    pl.when(at_end)(faces)
    for key in ((1, 0), (2, 0), (1, 2), (2, 1)):
        pack_corner(*key)
    for key in ((1, 0), (2, 0), (1, 2), (2, 1)):
        early(*CORNERS[key], [corners[key]])

    lifted = {}

    def lift(mu, nu):
        for h in range(halves):
            if mu == 0 and h == last:
                b = saved(local_s, PLANES.index((mu, nu)) * halves + h)
            else:
                b = local_product(mu, nu, h)
            if mu:
                lifted[mu, nu, h] = transported(b, mu, nu, h, False)
            elif h != last:
                prepare(mu, nu, h, 2)
            if nu != 3:
                lifted[nu, mu, h] = transported(b, nu, mu, h, True)
            else:
                prepare(nu, mu, h, 2)
        for d, m in ((mu, nu), (nu, mu)):
            if d == 1:
                pack_vz(m, [x for h in range(halves) for x in shortened(lifted[d, m, h])])
            elif d == 2:
                pack_vy(m, [x for h in range(halves) for x in lifted[d, m, h]])

    def greeted():
        answers(0)
        late(2, -1, [low_y])
        for key in ((0, 1), (0, 2), (1, 2), (2, 1)):
            middle(*CORNERS[key], [corners[key]])
        pl.when(at_end)(lambda: start(below_t))
        late(1, -1, below_z)
        late(0, 1, above_t)
        for key in ((1, 0), (2, 0)):
            between = jnp.logical_and(me[0] > 0, jnp.logical_not(highest(*CORNERS[key])))
            pl.when(between)(corners[key].start)

    pl.when(at_end)(greeted)
    lift(1, 3)
    lift(0, 1)
    lift(1, 2)
    pl.when(jnp.logical_not(at_end))(greeted)
    above_z = [high[1, m] for m in (3, 0, 2)]
    start(above_z)
    lift(2, 3)
    lift(0, 2)
    high_y.start()
    lift(0, 3)
    answers(1)
    for key in ((0, 1), (0, 2), (1, 2), (2, 1)):
        late(*CORNERS[key], [corners[key]])

    def ahead(m, d, h):
        if complete(d, h):
            return saved(ahead_s, ahead_slot[m, d, h])
        index = {c: n for n, c in enumerate(all_comps(d))}
        if d == 1:
            edges = restored([got_z("low", m, h, c, depth - 1) for c in range(10)])
        elif d == 0:
            values = [got(("low", 0, m), c // g.per * SUB) for c in range(10)]
            edges = restored(
                [g.rows(v, SUB - depth - depth * (c % g.per)) for c, v in enumerate(values)]
            )

        def get(part, i, j):
            v = ahead_s[ahead_slot[m, d, h], part, i, j]
            c = index[(m, part, i, j)]
            if d < 2:
                edge = edges[part][i][j]
            else:
                edge = g.lanes(
                    got(("low", 2), (c // g.ygroups * halves + h) * SUB), LANES - NX - NX * (c % g.ygroups)
                )
            return jnp.where(far_edge(d), edge, v)

        return complete_rows(get)

    def complete_rows(get):
        real = [[get(0, i, j) for j in range(3)] for i in range(2)]
        imag = [[get(1, i, j) for j in range(3)] for i in range(2)]
        third_r, third_i = third_row(real, imag)
        return [real + [third_r], imag + [third_i]]

    def add(m, c, h, value):
        r = ((m * 8 + c) * halves + h) * SUB
        acc[r : r + SUB, :] += value

    def shifted(q, d):
        if d == 3:
            return jnp.where(g.xcol == 0, g.lanes(q, 1 - NX), g.lanes(q, 1))
        if d == 2:
            return jnp.where(g.lane >= NX, g.lanes(q, NX), 0.0)
        if d == 1:
            return jnp.where(g.zrow > 0, g.rows(q, 1), 0.0)
        return jnp.where(g.row >= depth, g.rows(q, depth), 0.0)

    def plane(mu, nu, h):
        a = product(ahead(nu, mu, h), ahead(mu, nu, h), right_h=True)
        b = saved(local_s, PLANES.index((mu, nu)) * halves + h)
        e = product(matrix(mu, h), a)
        upper = projected(e, matrix(nu, h), right_h=True)
        q = projected(a, b, left_h=True)
        for c in range(8):
            add(mu, c, h, shifted(q[c], nu) + upper[c])
        q = projected(a, b, right_h=True)
        for c in range(8):
            add(nu, c, h, shifted(q[c], mu) - upper[c])
            if mu == 0 and h + 1 < halves:
                add(nu, c, h + 1, jnp.where(g.row < depth, g.rows(q[c], depth), 0.0))

    fixed_slot = {}

    def fix(d, m, h):
        beyond = complete_rows(lambda part, i, j: corner(d, m, h, part * 6 + i * 3 + j))
        own = matrix(m, h)
        moved = product(own, beyond, right_h=True)
        edge = far_edge(m)
        fixed_slot[d, m, h] = len(fixed_slot)
        save(
            fixed_s, fixed_slot[d, m, h],
            [[[jnp.where(edge, moved[p][i][j], own[p][i][j]) for j in range(3)] for i in range(3)] for p in range(2)],
        )

    def lower(d, m, h):
        def get(part, i, j):
            c = part * 6 + i * 3 + j
            n, k = places["high", 2][1] // 3, h * 12 + c
            r = others(2).index(m) * n + k // g.ygroups * SUB
            return g.lanes(got(("high", 2), r), -NX * (k % g.ygroups))

        if (d, m, h) in fixed_slot:
            left = saved(fixed_s, fixed_slot[d, m, h])
        else:
            left = matrix(m, h)
        if d == 0:
            values = [got(("high", 0, 3), c // g.per * SUB) for c in range(10)]
            lifts = with_third(restored([g.rows(v, -depth * (c % g.per)) for c, v in enumerate(values)]))
        elif d == 1:
            lifts = with_third(restored([got_z("high", m, h, c, 0) for c in range(10)]))
        else:
            lifts = complete_rows(get)
        q = projected(left, lifts, right_h=True)
        near = (g.row < depth, g.zrow == 0, g.lane < NX)[d]
        for c in range(8):
            add(m, c, h, jnp.where(near, q[c], 0.0))

    pair_slot = 2 + 2 * halves

    def pair_left():
        one, two = matrix(1, 0), matrix(2, 0)
        both = lambda p, i, j: jnp.where(g.row >= depth, g.rows(two[p][i][j], depth), one[p][i][j])
        save(fixed_s, pair_slot, [[[both(p, i, j) for j in range(3)] for i in range(3)] for p in range(2)])

    def pair_fix():
        def beyond(part, i, j):
            c = part * 6 + i * 3 + j
            k = c // g.ygroups
            value = g.lanes(
                g.rows(got((0, 2), 0), depth - depth * k), LANES - NX - NX * (c % g.ygroups)
            )
            return jnp.where(g.row >= depth, value, corner(0, 1, 0, c))

        own = saved(fixed_s, pair_slot)
        moved = product(own, complete_rows(beyond), right_h=True)
        edge = jnp.where(g.row >= depth, g.lane - (LANES - NX - 1), g.row - (depth - 2)) > 0
        save(
            fixed_s, pair_slot,
            [[[jnp.where(edge, moved[p][i][j], own[p][i][j]) for j in range(3)] for i in range(3)] for p in range(2)],
        )

    def pair_lift():
        return with_third(restored([got(("high", 0, "pair"), c * SUB) for c in range(10)]))

    def pair_lower(lifts):
        q = projected(saved(fixed_s, pair_slot), lifts, right_h=True)
        for c in range(8):
            add(1, c, 0, jnp.where(g.row < depth, q[c], 0.0))
            add(2, c, 0, jnp.where(g.row < depth, g.rows(q[c], -depth), 0.0))

    def y_part():
        arrived(("low", 2))
        for h in range(halves):
            plane(2, 3, h)
        for h in range(last):
            plane(0, 2, h)

    def z_part():
        arrived(("low", 1, 3))
        for h in range(halves):
            plane(1, 3, h)

    def around_part():
        answers(2)
        for key in ((1, 0), (2, 0)):
            between = jnp.logical_not(jnp.logical_or(lowest(*CORNERS[key]), highest(*CORNERS[key])))
            pl.when(jnp.logical_and(me[0] == 0, between))(corners[key].start)
        late(0, -1, below_t)

    def rest_part():
        arrived(("low", 1, 0))
        for h in range(last):
            plane(0, 1, h)

    def high_y_part():
        arrived(("high", 2))
        for m in (3, 0):
            for h in range(halves if m else last):
                lower(2, m, h)

    def t_part():
        arrived(("low", 0, 3))
        plane(0, 3, last)
        plane(0, 1, last)

    def corner_part():
        answers(3)
        for key in ((1, 0), (2, 0)):
            pl.when(me[0] == 0)(functools.partial(late, *CORNERS[key], [corners[key]]))

    for h in range(last):
        plane(0, 3, h)
    def cross_part():
        arrived(("low", 1, 2))
        for h in range(halves):
            plane(1, 2, h)

    near = me[0] == 0

    @pl.when(even)
    def _():
        y_part()
        around_part()
        z_part()
        rest_part()
        pl.when(near)(t_part)
        corner_part()
        cross_part()
        high_y_part()
        pl.when(jnp.logical_not(near))(t_part)

    @pl.when(jnp.logical_not(even))
    def _():
        z_part()
        around_part()
        rest_part()
        high_y_part()
        pl.when(near)(t_part)
        corner_part()
        y_part()
        cross_part()
        pl.when(jnp.logical_not(near))(t_part)

    plane(0, 2, last)
    arrived((2, 1))
    for h in range(halves):
        fix(2, 1, h)
        lower(2, 1, h)
        fix(1, 2, h)
    fix(2, 0, last)
    lower(2, 0, last)
    fix(1, 0, last)
    pair_left()
    arrived(("high", 1, 3))
    for m in (3, 0, 2):
        for h in range(halves):
            lower(1, m, h)
    lower(0, 3, 0)
    arrived(("high", 0, "pair"))
    lifts = pair_lift()
    arrived((0, 1))
    pair_fix()
    pair_lower(lifts)
    remote(0, spans[-1][1], 0, 0, 1).wait_send()


def expand(halves, acc, hbm, out, sems):
    copies = []
    for m in range(4):
        for h in range(halves):
            rows = [((m * 8 + c) * halves + h) * SUB for c in range(8)]
            f = [acc[r : r + SUB, :] * (COEFF * 0.5 if c < 6 else COEFF) for c, r in enumerate(rows)]

            def put(part, i, j, value):
                out[m, part, i, j, h * SUB : (h + 1) * SUB, :] = value

            for n, (i, j) in enumerate(((0, 1), (0, 2), (1, 2))):
                put(0, i, j, f[n])
                put(0, j, i, -f[n])
                put(1, i, j, f[3 + n])
                put(1, j, i, f[3 + n])
            for i in range(3):
                put(0, i, i, jnp.zeros((SUB, LANES), jnp.float32))
            put(1, 0, 0, f[6])
            put(1, 1, 1, f[7])
            put(1, 2, 2, -(f[6] + f[7]))
        copies.append(pltpu.make_async_copy(out.at[m], hbm.at[m], sems.at[m]))
        copies[-1].start()
    for copy in copies:
        copy.wait()


def per_device(counts, links):
    time_len, depth, flat = links.shape[4:]
    sites = time_len * depth
    assert flat == LANES and SUB % depth == 0 and sites % SUB == 0 and 2 <= depth <= SUB // 2
    halves = sites // SUB
    spans = mail(depth, halves)[1]
    vmem = lambda *s: pltpu.VMEM(s + (LANES,), jnp.float32)
    shape = links.shape[:4] + (sites, flat)
    terms = pl.pallas_call(
        functools.partial(force_terms, counts, depth, halves),
        out_shape=pltpu.VMEM((32 * sites, flat), jnp.float32),
        in_specs=[pl.BlockSpec(memory_space=pl.ANY)],
        out_specs=pl.BlockSpec(memory_space=pltpu.VMEM),
        scratch_shapes=[
            vmem(*shape[:-1]),
            vmem(12 * halves, 2, 3, 3, SUB),
            vmem(6 * halves, 2, 3, 3, SUB),
            vmem(3 + 2 * halves, 2, 3, 3, SUB),
            vmem(spans[-1][1]),
            vmem(spans[-1][1]),
            pltpu.SemaphoreType.DMA((3,)),
            pltpu.SemaphoreType.DMA((1,)),
            pltpu.SemaphoreType.DMA((len(spans),)),
            pltpu.SemaphoreType.REGULAR((4,)),
        ],
        compiler_params=pltpu.CompilerParams(collective_id=0, has_side_effects=True),
        name="force_terms",
    )(links.reshape(shape))
    out = pl.pallas_call(
        functools.partial(expand, halves),
        out_shape=jax.ShapeDtypeStruct(shape, jnp.float32),
        in_specs=[pl.BlockSpec(memory_space=pltpu.VMEM)],
        out_specs=pl.BlockSpec(memory_space=pl.ANY),
        scratch_shapes=[vmem(*shape[:-1]), pltpu.SemaphoreType.DMA((4,))],
        name="expand",
    )(pltpu.with_memory_space_constraint(terms, pltpu.VMEM))
    return out.reshape(links.shape)


def solution(mesh):
    assert mesh.axis_names == ("gx", "gz", "ta")
    counts = tuple(mesh.shape[a] for a in AXES)
    spec = P(None, None, None, None, "ta", "gz", "gx")
    return jax.shard_map(
        functools.partial(per_device, counts),
        mesh=mesh,
        in_specs=(spec,),
        out_specs=spec,
        check_vma=False,
    )
```

```python
import functools

import jax
import jax.numpy as jnp
from jax import lax
from jax.experimental import pallas as pl
from jax.experimental.pallas import tpu as pltpu
from jax.sharding import PartitionSpec as P

NX = 16
COEFF = -1.9
AXES = ("ta", "gz", "gx")
SUB, LANES = 8, 128


def others(d):
    return [m for m in range(4) if m != d]


class Lattice:
    def __init__(self, depth):
        self.depth = depth
        self.per = SUB // depth
        self.ygroups = LANES // NX
        self.row = lax.broadcasted_iota(jnp.int32, (SUB, LANES), 0)
        self.lane = lax.broadcasted_iota(jnp.int32, (SUB, LANES), 1)
        self.zrow = self.row % depth
        self.xcol = self.lane % NX

    def rows(self, value, shift):
        shift %= SUB
        return pltpu.roll(value, shift, 0) if shift else value

    def lanes(self, value, shift):
        shift %= LANES
        return pltpu.roll(value, shift, 1) if shift else value


def entry(left, right, i, j, part, left_h, right_h):
    total = None
    for k in range(3):
        li = (k, i) if left_h else (i, k)
        ri = (j, k) if right_h else (k, j)
        lr, lm = left[0][li[0]][li[1]], left[1][li[0]][li[1]]
        rr, rm = right[0][ri[0]][ri[1]], right[1][ri[0]][ri[1]]
        if part == 0:
            first, second = lr * rr, lm * rm
            minus = left_h == right_h
        elif left_h:
            first, second = lr * rm, lm * rr
            minus = True
        else:
            first, second = lm * rr, lr * rm
            minus = right_h
        value = first - second if minus else first + second
        total = value if total is None else total + value
    return total


def product(left, right, left_h=False, right_h=False):
    return [
        [[entry(left, right, i, j, part, left_h, right_h) for j in range(3)] for i in range(3)]
        for part in range(2)
    ]


def projected(left, right, left_h=False, right_h=False):
    get = lambda i, j, part: entry(left, right, i, j, part, left_h, right_h)
    pairs = ((0, 1), (0, 2), (1, 2))
    real = [get(i, j, 0) - get(j, i, 0) for i, j in pairs]
    imag = [get(i, j, 1) + get(j, i, 1) for i, j in pairs]
    diag = [get(i, i, 1) for i in range(3)]
    third = (diag[0] + diag[1] + diag[2]) * (1.0 / 3.0)
    return real + imag + [diag[0] - third, diag[1] - third]


def third_row(real, imag):
    rows_r, rows_i = [], []
    for column in range(3):
        n, l = (column + 1) % 3, (column + 2) % 3
        rows_r.append(
            real[0][n] * real[1][l]
            - imag[0][n] * imag[1][l]
            - real[0][l] * real[1][n]
            + imag[0][l] * imag[1][n]
        )
        rows_i.append(
            real[0][l] * imag[1][n]
            + imag[0][l] * real[1][n]
            - real[0][n] * imag[1][l]
            - imag[0][n] * real[1][l]
        )
    return rows_r, rows_i


PLANES = ((2, 3), (1, 3), (1, 2), (0, 1), (0, 2), (0, 3))
KINDS = ({0: 1}, {1: 1}, {2: 1}, {0: 1, 1: -1}, {0: 1, 2: -1}, {1: 1, 2: -1})
CORNERS = {(0, 1): (3, 1), (1, 0): (3, -1), (0, 2): (4, 1), (2, 0): (4, -1), (1, 2): (5, 1), (2, 1): (5, -1)}
FIXED = [(0, 1, 0), (0, 2, 0), (1, 0, -1), (1, 2, None), (2, 0, -1), (2, 1, None)]


def by_largest(real, imag):
    size = [jnp.maximum(jnp.abs(r), jnp.abs(i)) for r, i in zip(real, imag)]
    first = jnp.logical_and(size[0] >= size[1], size[0] >= size[2])
    second = size[1] >= size[2]
    return lambda a, b, c: jnp.where(first, a, jnp.where(second, b, c))


def shortened(v):
    pick = by_largest(v[0:3], v[6:9])
    keep = v[0:3] + v[6:9]
    for turn in (1, 2):
        for row in (v[3:6], v[9:12]):
            keep.append(pick(*(row[(k + turn) % 3] for k in range(3))))
    return keep


def restored(v):
    real, imag = v[0:3], v[3:6]
    pick = by_largest(real, imag)
    (xr, xi), (yr, yi), (zr, zi) = (
        [pick(*(part[(k + turn) % 3] for k in range(3))) for part in (real, imag)] for turn in range(3)
    )
    pr, pi, qr, qi = v[6:10]
    sr = pr * yr + pi * yi + qr * zr + qi * zi
    si = pi * yr - pr * yi + qi * zr - qr * zi
    scale = -1.0 / (xr * xr + xi * xi)
    br, bi = (sr * xr - si * xi) * scale, (sr * xi + si * xr) * scale
    second_r = [pick(br, qr, pr), pick(pr, br, qr), pick(qr, pr, br)]
    second_i = [pick(bi, qi, pi), pick(pi, bi, qi), pick(qi, pi, bi)]
    return [[real, second_r], [imag, second_i]]


def with_third(rows):
    third_r, third_i = third_row(*rows)
    return [rows[0] + [third_r], rows[1] + [third_i]]


def mail(depth, halves):
    up = lambda a, b: -(-a // b) * SUB
    per, yg = SUB // depth, LANES // NX
    z, y = up(10 * halves, depth), up(36, yg) * halves
    short = up(10, per)
    groups = (
        ((("low", 2), y),),
        ((("low", 1, 3), z),),
        ((("low", 1, 0), z),),
        ((("low", 1, 2), z),),
        ((("high", 2), 3 * up(12 * halves, yg)),),
        ((("high", 1, 3), z), (("high", 1, 0), z), (("high", 1, 2), z), (("high", 0, 3), short)),
        ((("low", 0, 3), short), (("low", 0, 1), short), (("low", 0, 2), short)),
        (((2, 1), SUB * halves), ((1, 2), SUB * halves), ((1, 0), 2 * SUB), ((2, 0), SUB)),
        (((0, 1), 2 * SUB), ((0, 2), SUB)),
        ((("high", 0, "pair"), 10 * SUB),),
    )
    places, spans, row = {}, [], 0
    for group in groups:
        first = row
        for name, rows in group:
            places[name] = (row, rows, len(spans))
            row += rows
        spans.append((first, row))
    return places, spans


def force_terms(
    counts, depth, halves, hbm, acc,
    u, ahead_s, local_s, fixed_s, outbox, inbox, recv, ready, load_sem, send,
):
    g = Lattice(depth)
    last = halves - 1
    me = [lax.axis_index(a) for a in AXES]
    places, spans = mail(depth, halves)

    cut = last * SUB
    cut = last * SUB

    def loads(m, p, from_last, sem):
        rows = slice(cut, None) if from_last else slice(0, cut)
        return pltpu.make_async_copy(
            hbm.at[m, p, :, :, rows], u.at[m, p, :, :, rows], load_sem.at[sem]
        )

    for from_last in (True, False):
        for m in (0, 3, 2, 1):
            for p in range(2):
                loads(m, p, from_last, (1 if m else 0) if from_last else 2).start()
    load_time = loads(0, slice(None), True, 0)
    load_last = loads(slice(1, None), slice(None), True, 1)
    load_rest = loads(slice(None), slice(None), False, 2)

    def peer(kind, sign):
        where = list(me)
        for i, step in KINDS[kind].items():
            where[i] = lax.rem(me[i] + counts[i] + sign * step, counts[i])
        by = dict(zip(AXES, where))
        return (by["gx"], by["gz"], by["ta"])

    def above(axis, sign):
        rank = lambda i: i + 1 - 2 * lax.rem(i, 2) if False else i
        return rank(lax.rem(me[axis] + counts[axis] + sign, counts[axis])) > rank(me[axis])

    def lowest(kind, sign):
        tests = [above(i, sign * step) for i, step in KINDS[kind].items()]
        return functools.reduce(jnp.logical_and, tests)

    def highest(kind, sign):
        tests = [above(i, sign * step) for i, step in KINDS[kind].items()]
        return jnp.logical_not(functools.reduce(jnp.logical_or, tests))

    barrier = pltpu.get_barrier_semaphore()
    pairs = [(kind, sign) for kind in range(6) for sign in (1, -1)]
    expected = 0
    for kind, sign in pairs:
        expected = expected + jnp.where(highest(kind, sign), 1, 0)

        @pl.when(lowest(kind, sign))
        def _():
            pl.semaphore_signal(
                barrier, inc=1, device_id=peer(kind, sign), device_id_type=pl.DeviceIdType.MESH
            )

    @pl.when(expected > 0)
    def _():
        pl.semaphore_wait(barrier, expected)

    def answer_group(kind, sign):
        if kind < 3:
            return 2 if (kind, sign) == (0, -1) else 0
        return 3 if kind < 5 and sign < 0 else 1

    for kind, sign in pairs:

        @pl.when(highest(kind, sign))
        def _():
            pl.semaphore_signal(
                ready.at[answer_group(kind, -sign)], inc=1,
                device_id=peer(kind, sign), device_id_type=pl.DeviceIdType.MESH,
            )

    def answers(group):
        count = 0
        for kind, sign in pairs:
            if answer_group(kind, sign) == group:
                count = count + jnp.where(lowest(kind, sign), 1, 0)

        @pl.when(count > 0)
        def _():
            pl.semaphore_wait(ready.at[group], count)

    def start(copies):
        for copy in copies:
            copy.start()

    def early(kind, sign, copies):
        pl.when(highest(kind, sign))(lambda: start(copies))

    def late(kind, sign, copies):
        pl.when(lowest(kind, sign))(lambda: start(copies))

    def middle(kind, sign, copies):
        between = jnp.logical_not(jnp.logical_or(lowest(kind, sign), highest(kind, sign)))
        pl.when(between)(lambda: start(copies))

    def put(name, r, value):
        row = places[name][0] + r
        outbox[row : row + SUB, :] = value

    def got(name, r):
        row = places[name][0] + r
        return inbox[row : row + SUB, :]

    def load(m, part, i, j, h):
        return u[m, part, i, j, h * SUB : (h + 1) * SUB, :]

    COMPS = [(part, i, j) for part in range(2) for i in range(2) for j in range(3)]

    def comps(m):
        return [(m,) + c for c in COMPS]

    def all_comps(d):
        return [c for m in others(d) for c in comps(m)]

    def flat(value):
        return [value[part][i][j] for part, i, j in COMPS]

    def merge(values, index, step):
        total = None
        for k, x in enumerate(values):
            total = x if total is None else jnp.where(index >= step * k, x, total)
        return total

    def pack_t(m):
        v = shortened([load(*c, 0) for c in comps(m)])
        for c0 in range(0, 10, g.per):
            ks = range(min(g.per, 10 - c0))
            put(("low", 0, m), c0 // g.per * SUB, merge([g.rows(v[c0 + k], depth * k) for k in ks], g.row, depth))

    def pack_z(m):
        v = [x for h in range(halves) for x in shortened([load(*c, h) for c in comps(m)])]
        for c0 in range(0, len(v), depth):
            ks = range(min(depth, len(v) - c0))
            put(("low", 1, m), c0 // depth * SUB, merge([g.rows(v[c0 + k], k) for k in ks], g.zrow, 1))

    def pack_y():
        cs = all_comps(2)
        for c0 in range(0, len(cs), g.ygroups):
            for h in range(halves):
                ks = range(min(g.ygroups, len(cs) - c0))
                put(
                    ("low", 2), (c0 // g.ygroups * halves + h) * SUB,
                    merge([g.lanes(load(*cs[c0 + k], h), NX * k) for k in ks], g.lane, NX),
                )

    def pack_vt(v):
        v = shortened(v)
        for c0 in range(0, 10, g.per):
            ks = range(min(g.per, 10 - c0))
            put(
                ("high", 0, 3), c0 // g.per * SUB,
                merge([g.rows(v[c0 + k], depth * (k + 1)) for k in ks], g.row, depth),
            )

    def pack_pair(one, two):
        for c, (v, w) in enumerate(zip(shortened(one), shortened(two))):
            put(("high", 0, "pair"), c * SUB, jnp.where(g.row >= depth, g.rows(w, 2 * depth), g.rows(v, depth)))

    def pack_vz(m, v):
        for c0 in range(0, len(v), depth):
            ks = range(min(depth, len(v) - c0))
            put(
                ("high", 1, m), c0 // depth * SUB,
                merge([g.rows(v[c0 + k], k + 1 - depth) for k in ks], g.zrow, 1),
            )

    def got_z(side, m, h, c, row):
        n = 10 * h + c
        return g.rows(got((side, 1, m), n // depth * SUB), row - n % depth)

    def pack_vy(m, v):
        n = places["high", 2][1] // 3
        for c0 in range(0, 12 * halves, g.ygroups):
            ks = range(min(g.ygroups, 12 * halves - c0))
            put(
                ("high", 2), others(2).index(m) * n + c0 // g.ygroups * SUB,
                merge([g.lanes(v[c0 + k], NX * (k + 1)) for k in ks], g.lane, NX),
            )

    def by_groups(d, h, up, shift, index, step):
        cs = comps(d)
        return merge(
            [
                merge(
                    [
                        g.lanes(g.rows(load(*cs[c], h), shift(c // g.ygroups)), NX * (c % g.ygroups + up))
                        for c in range(c0, min(12, c0 + g.ygroups))
                    ],
                    g.lane, NX,
                )
                for c0 in range(0, 12, g.ygroups)
            ],
            index, step,
        )

    def pack_corner(d, m):
        cs = comps(d)
        if (d, m) in ((0, 1), (1, 0)):
            source = SUB - depth if d == 0 else depth - 1
            for c0 in range(0, 12, SUB):
                ks = range(min(SUB, 12 - c0))
                values = [g.rows(load(*cs[c0 + k], last if d == 0 else 0), k - source) for k in ks]
                put((d, m), c0, merge(values, g.row, 1))
        elif (d, m) == (0, 2):
            put((d, m), 0, by_groups(0, last, 0, lambda k: depth * (k + 1), g.row, depth))
        elif (d, m) == (2, 0):
            put((d, m), 0, by_groups(2, 0, 1, lambda k: depth * k, g.row, depth))
        else:
            for h in range(halves):
                up, source = (0, depth - 1) if d == 1 else (1, 0)
                put((d, m), h * SUB, by_groups(d, h, up, lambda k: k - source, g.zrow, 1))

    def corner(d, m, h, c):
        k, group = c // g.ygroups, NX * (c % g.ygroups)
        if (d, m) in ((0, 1), (1, 0)):
            target = depth - 1 if d == 0 else SUB - depth
            return g.rows(got((d, m), c // SUB * SUB), target - c % SUB)
        if (d, m) == (0, 2):
            return g.lanes(g.rows(got((d, m), 0), -depth * k), LANES - NX - group)
        if (d, m) == (2, 0):
            return g.lanes(g.rows(got((d, m), 0), SUB - depth - depth * k), -group)
        if d == 1:
            return g.lanes(g.rows(got((d, m), h * SUB), -k), LANES - NX - group)
        return g.lanes(g.rows(got((d, m), h * SUB), depth - 1 - k), -group)

    def remote(first, end, group, kind, sign):
        return pltpu.make_async_remote_copy(
            src_ref=outbox.at[first:end], dst_ref=inbox.at[first:end],
            send_sem=send.at[0], recv_sem=recv.at[group],
            device_id=peer(kind, sign), device_id_type=pl.DeviceIdType.MESH,
        )

    def message(name, kind, sign):
        first, rows, group = places[name]
        return remote(first, first + rows, group, kind, sign)

    def arrived(name):
        group = places[name][2]
        remote(*spans[group], group, 0, 1).wait_recv()

    low = {(d, m): message(("low", d, m), d, -1) for d in (0, 1) for m in others(d)}
    high = {(d, m): message(("high", d, m), d, 1) for d, m in ((0, 3), (0, "pair"), (1, 0), (1, 2), (1, 3))}
    low_y, high_y = message(("low", 2), 2, -1), message(("high", 2), 2, 1)
    corners = {key: message(key, kind, sign) for key, (kind, sign) in CORNERS.items()}

    def matrix(m, h):
        return [[[load(m, part, i, j, h) for j in range(3)] for i in range(3)] for part in range(2)]

    def save(ref, index, value):
        for part in range(2):
            for i in range(len(value[part])):
                for j in range(3):
                    ref[index, part, i, j] = value[part][i][j]

    def saved(ref, index, rows=3):
        return [[[ref[index, part, i, j] for j in range(3)] for i in range(rows)] for part in range(2)]

    def rolled(m, d, h, part, i, j):
        v = load(m, part, i, j, h)
        if d == 3:
            return jnp.where(g.xcol == NX - 1, g.lanes(v, NX - 1), g.lanes(v, -1))
        if d == 2:
            return g.lanes(v, -NX)
        if d == 1:
            return g.rows(v, -1)
        if h + 1 < halves:
            beyond = g.rows(load(m, part, i, j, h + 1), -depth)
            return jnp.where(g.row >= SUB - depth, beyond, g.rows(v, -depth))
        return g.rows(v, -depth)

    def complete(d, h):
        return d == 3 or (d == 0 and h + 1 < halves)

    def far_edge(d):
        return (g.row >= SUB - depth, g.zrow == depth - 1, g.lane >= LANES - NX)[d]

    ahead_slot = {}

    def prepare(m, d, h, rows):
        value = [
            [[rolled(m, d, h, part, i, j) for j in range(3)] for i in range(3 if rows == 3 or complete(d, h) else 2)]
            for part in range(2)
        ]
        ahead_slot[m, d, h] = len(ahead_slot)
        keep = 3 if complete(d, h) else 2
        save(ahead_s, ahead_slot[m, d, h], [part[:keep] for part in value])
        return value

    def transported(b, m, d, h, b_h):
        moved = prepare(m, d, h, 3)
        value = [
            [[entry(b, moved, i, j, part, b_h, False) for j in range(3)] for i in range(2)]
            for part in range(2)
        ]
        if not complete(d, h):
            edge = far_edge(d)
            for part in range(2):
                for i in range(2):
                    for j in range(3):
                        own = b[part][j][i] if b_h else b[part][i][j]
                        own = -own if b_h and part else own
                        value[part][i][j] = jnp.where(edge, own, value[part][i][j])
        return flat(value)

    local = {}

    def local_product(mu, nu, h):
        b = product(matrix(mu, h), matrix(nu, h), left_h=True)
        save(local_s, PLANES.index((mu, nu)) * halves + h, b)
        return b

    below_t, below_z = [low[0, m] for m in (3, 1, 2)], [low[1, m] for m in (3, 0, 2)]
    above_t = [high[0, 3], high[0, "pair"]]
    even = lax.rem(me[2], 2) == 0
    at_end = me[0] == counts[0] - 1

    def faces():
        load_rest.wait()
        for m in (3, 1, 2):
            pack_t(m)
        pl.when(jnp.logical_not(at_end))(lambda: early(0, -1, below_t))
        for m in (3, 0, 2):
            pack_z(m)
        early(1, -1, below_z)
        pack_y()
        early(2, -1, [low_y])

    acc[...] = jnp.zeros_like(acc)
    load_time.wait()
    for d in (1, 2):
        pack_corner(0, d)
        early(*CORNERS[0, d], [corners[0, d]])
    load_last.wait()
    pl.when(jnp.logical_not(at_end))(faces)
    pack_vt(transported(local_product(0, 3, last), 0, 3, last, False))
    early(0, 1, [high[0, 3]])
    pack_pair(*(transported(local_product(0, m, last), 0, m, last, False) for m in (1, 2)))
    early(0, 1, [high[0, "pair"]])
    pl.when(at_end)(faces)
    for key in ((1, 0), (2, 0), (1, 2), (2, 1)):
        pack_corner(*key)
    for key in ((1, 0), (2, 0), (1, 2), (2, 1)):
        early(*CORNERS[key], [corners[key]])

    lifted = {}

    def lift(mu, nu):
        for h in range(halves):
            if mu == 0 and h == last:
                b = saved(local_s, PLANES.index((mu, nu)) * halves + h)
            else:
                b = local_product(mu, nu, h)
            if mu:
                lifted[mu, nu, h] = transported(b, mu, nu, h, False)
            elif h != last:
                prepare(mu, nu, h, 2)
            if nu != 3:
                lifted[nu, mu, h] = transported(b, nu, mu, h, True)
            else:
                prepare(nu, mu, h, 2)
        for d, m in ((mu, nu), (nu, mu)):
            if d == 1:
                pack_vz(m, [x for h in range(halves) for x in shortened(lifted[d, m, h])])
            elif d == 2:
                pack_vy(m, [x for h in range(halves) for x in lifted[d, m, h]])

    def greeted():
        answers(0)
        late(2, -1, [low_y])
        for key in ((0, 1), (0, 2), (1, 2), (2, 1)):
            middle(*CORNERS[key], [corners[key]])
        pl.when(at_end)(lambda: start(below_t))
        late(1, -1, below_z)
        late(0, 1, above_t)
        for key in ((1, 0), (2, 0)):
            between = jnp.logical_and(me[0] > 0, jnp.logical_not(highest(*CORNERS[key])))
            pl.when(between)(corners[key].start)

    pl.when(at_end)(greeted)
    lift(1, 3)
    lift(0, 1)
    lift(1, 2)
    pl.when(jnp.logical_not(at_end))(greeted)
    above_z = [high[1, m] for m in (3, 0, 2)]
    start(above_z)
    lift(2, 3)
    lift(0, 2)
    high_y.start()
    lift(0, 3)
    answers(1)
    for key in ((0, 1), (0, 2), (1, 2), (2, 1)):
        late(*CORNERS[key], [corners[key]])

    def ahead(m, d, h):
        if complete(d, h):
            return saved(ahead_s, ahead_slot[m, d, h])
        index = {c: n for n, c in enumerate(all_comps(d))}
        if d == 1:
            edges = restored([got_z("low", m, h, c, depth - 1) for c in range(10)])
        elif d == 0:
            values = [got(("low", 0, m), c // g.per * SUB) for c in range(10)]
            edges = restored(
                [g.rows(v, SUB - depth - depth * (c % g.per)) for c, v in enumerate(values)]
            )

        def get(part, i, j):
            v = ahead_s[ahead_slot[m, d, h], part, i, j]
            c = index[(m, part, i, j)]
            if d < 2:
                edge = edges[part][i][j]
            else:
                edge = g.lanes(
                    got(("low", 2), (c // g.ygroups * halves + h) * SUB), LANES - NX - NX * (c % g.ygroups)
                )
            return jnp.where(far_edge(d), edge, v)

        return complete_rows(get)

    def complete_rows(get):
        real = [[get(0, i, j) for j in range(3)] for i in range(2)]
        imag = [[get(1, i, j) for j in range(3)] for i in range(2)]
        third_r, third_i = third_row(real, imag)
        return [real + [third_r], imag + [third_i]]

    def add(m, c, h, value):
        r = ((m * 8 + c) * halves + h) * SUB
        acc[r : r + SUB, :] += value

    def shifted(q, d):
        if d == 3:
            return jnp.where(g.xcol == 0, g.lanes(q, 1 - NX), g.lanes(q, 1))
        if d == 2:
            return jnp.where(g.lane >= NX, g.lanes(q, NX), 0.0)
        if d == 1:
            return jnp.where(g.zrow > 0, g.rows(q, 1), 0.0)
        return jnp.where(g.row >= depth, g.rows(q, depth), 0.0)

    def plane(mu, nu, h):
        a = product(ahead(nu, mu, h), ahead(mu, nu, h), right_h=True)
        b = saved(local_s, PLANES.index((mu, nu)) * halves + h)
        e = product(matrix(mu, h), a)
        upper = projected(e, matrix(nu, h), right_h=True)
        q = projected(a, b, left_h=True)
        for c in range(8):
            add(mu, c, h, shifted(q[c], nu) + upper[c])
        q = projected(a, b, right_h=True)
        for c in range(8):
            add(nu, c, h, shifted(q[c], mu) - upper[c])
            if mu == 0 and h + 1 < halves:
                add(nu, c, h + 1, jnp.where(g.row < depth, g.rows(q[c], depth), 0.0))

    fixed_slot = {}

    def fix(d, m, h):
        beyond = complete_rows(lambda part, i, j: corner(d, m, h, part * 6 + i * 3 + j))
        own = matrix(m, h)
        moved = product(own, beyond, right_h=True)
        edge = far_edge(m)
        fixed_slot[d, m, h] = len(fixed_slot)
        save(
            fixed_s, fixed_slot[d, m, h],
            [[[jnp.where(edge, moved[p][i][j], own[p][i][j]) for j in range(3)] for i in range(3)] for p in range(2)],
        )

    def lower(d, m, h):
        def get(part, i, j):
            c = part * 6 + i * 3 + j
            n, k = places["high", 2][1] // 3, h * 12 + c
            r = others(2).index(m) * n + k // g.ygroups * SUB
            return g.lanes(got(("high", 2), r), -NX * (k % g.ygroups))

        if (d, m, h) in fixed_slot:
            left = saved(fixed_s, fixed_slot[d, m, h])
        else:
            left = matrix(m, h)
        if d == 0:
            values = [got(("high", 0, 3), c // g.per * SUB) for c in range(10)]
            lifts = with_third(restored([g.rows(v, -depth * (c % g.per)) for c, v in enumerate(values)]))
        elif d == 1:
            lifts = with_third(restored([got_z("high", m, h, c, 0) for c in range(10)]))
        else:
            lifts = complete_rows(get)
        q = projected(left, lifts, right_h=True)
        near = (g.row < depth, g.zrow == 0, g.lane < NX)[d]
        for c in range(8):
            add(m, c, h, jnp.where(near, q[c], 0.0))

    pair_slot = 2 + 2 * halves

    def pair_left():
        one, two = matrix(1, 0), matrix(2, 0)
        both = lambda p, i, j: jnp.where(g.row >= depth, g.rows(two[p][i][j], depth), one[p][i][j])
        save(fixed_s, pair_slot, [[[both(p, i, j) for j in range(3)] for i in range(3)] for p in range(2)])

    def pair_fix():
        def beyond(part, i, j):
            c = part * 6 + i * 3 + j
            k = c // g.ygroups
            value = g.lanes(
                g.rows(got((0, 2), 0), depth - depth * k), LANES - NX - NX * (c % g.ygroups)
            )
            return jnp.where(g.row >= depth, value, corner(0, 1, 0, c))

        own = saved(fixed_s, pair_slot)
        moved = product(own, complete_rows(beyond), right_h=True)
        edge = jnp.where(g.row >= depth, g.lane - (LANES - NX - 1), g.row - (depth - 2)) > 0
        save(
            fixed_s, pair_slot,
            [[[jnp.where(edge, moved[p][i][j], own[p][i][j]) for j in range(3)] for i in range(3)] for p in range(2)],
        )

    def pair_lift():
        return with_third(restored([got(("high", 0, "pair"), c * SUB) for c in range(10)]))

    def pair_lower(lifts):
        q = projected(saved(fixed_s, pair_slot), lifts, right_h=True)
        for c in range(8):
            add(1, c, 0, jnp.where(g.row < depth, q[c], 0.0))
            add(2, c, 0, jnp.where(g.row < depth, g.rows(q[c], -depth), 0.0))

    def y_part():
        arrived(("low", 2))
        for h in range(halves):
            plane(2, 3, h)
        for h in range(last):
            plane(0, 2, h)

    def z_part():
        arrived(("low", 1, 3))
        for h in range(halves):
            plane(1, 3, h)

    def around_part():
        answers(2)
        for key in ((1, 0), (2, 0)):
            between = jnp.logical_not(jnp.logical_or(lowest(*CORNERS[key]), highest(*CORNERS[key])))
            pl.when(jnp.logical_and(me[0] == 0, between))(corners[key].start)
        late(0, -1, below_t)

    def rest_part():
        arrived(("low", 1, 0))
        for h in range(last):
            plane(0, 1, h)

    def high_y_part():
        arrived(("high", 2))
        for m in (3, 0):
            for h in range(halves if m else last):
                lower(2, m, h)

    def t_part():
        arrived(("low", 0, 3))
        plane(0, 3, last)
        plane(0, 1, last)

    def corner_part():
        answers(3)
        for key in ((1, 0), (2, 0)):
            pl.when(me[0] == 0)(functools.partial(late, *CORNERS[key], [corners[key]]))

    for h in range(last):
        plane(0, 3, h)
    def cross_part():
        arrived(("low", 1, 2))
        for h in range(halves):
            plane(1, 2, h)

    near = me[0] == 0

    @pl.when(even)
    def _():
        y_part()
        around_part()
        z_part()
        rest_part()
        pl.when(near)(t_part)
        corner_part()
        cross_part()
        high_y_part()
        pl.when(jnp.logical_not(near))(t_part)

    @pl.when(jnp.logical_not(even))
    def _():
        z_part()
        around_part()
        rest_part()
        high_y_part()
        pl.when(near)(t_part)
        corner_part()
        y_part()
        cross_part()
        pl.when(jnp.logical_not(near))(t_part)

    plane(0, 2, last)
    arrived((2, 1))
    for h in range(halves):
        fix(2, 1, h)
        lower(2, 1, h)
        fix(1, 2, h)
    fix(2, 0, last)
    lower(2, 0, last)
    fix(1, 0, last)
    pair_left()
    arrived(("high", 1, 3))
    for m in (3, 0, 2):
        for h in range(halves):
            lower(1, m, h)
    lower(0, 3, 0)
    arrived(("high", 0, "pair"))
    lifts = pair_lift()
    arrived((0, 1))
    pair_fix()
    pair_lower(lifts)
    remote(0, spans[-1][1], 0, 0, 1).wait_send()


def expand(halves, acc, hbm, out, sems):
    copies = []
    for m in range(4):
        for h in range(halves):
            rows = [((m * 8 + c) * halves + h) * SUB for c in range(8)]
            f = [acc[r : r + SUB, :] * (COEFF * 0.5 if c < 6 else COEFF) for c, r in enumerate(rows)]

            def put(part, i, j, value):
                out[m, part, i, j, h * SUB : (h + 1) * SUB, :] = value

            for n, (i, j) in enumerate(((0, 1), (0, 2), (1, 2))):
                put(0, i, j, f[n])
                put(0, j, i, -f[n])
                put(1, i, j, f[3 + n])
                put(1, j, i, f[3 + n])
            for i in range(3):
                put(0, i, i, jnp.zeros((SUB, LANES), jnp.float32))
            put(1, 0, 0, f[6])
            put(1, 1, 1, f[7])
            put(1, 2, 2, -(f[6] + f[7]))
        copies.append(pltpu.make_async_copy(out.at[m], hbm.at[m], sems.at[m]))
        copies[-1].start()
    for copy in copies:
        copy.wait()


def per_device(counts, links):
    time_len, depth, flat = links.shape[4:]
    sites = time_len * depth
    assert flat == LANES and SUB % depth == 0 and sites % SUB == 0 and 2 <= depth <= SUB // 2
    halves = sites // SUB
    spans = mail(depth, halves)[1]
    vmem = lambda *s: pltpu.VMEM(s + (LANES,), jnp.float32)
    shape = links.shape[:4] + (sites, flat)

    def kernel(*refs):
        pl.run_scoped(
            functools.partial(force_terms, counts, depth, halves, *refs),
            pltpu.SemaphoreType.DMA((3,)),
            pltpu.SemaphoreType.DMA((1,)),
        )

    terms = pl.pallas_call(
        kernel,
        out_shape=pltpu.VMEM((32 * sites, flat), jnp.float32),
        in_specs=[pl.BlockSpec(memory_space=pl.ANY)],
        out_specs=pl.BlockSpec(memory_space=pltpu.VMEM),
        scratch_shapes=[
            vmem(*shape[:-1]),
            vmem(12 * halves, 2, 3, 3, SUB),
            vmem(6 * halves, 2, 3, 3, SUB),
            vmem(3 + 2 * halves, 2, 3, 3, SUB),
            vmem(spans[-1][1]),
            vmem(spans[-1][1]),
            pltpu.SemaphoreType.DMA((len(spans),)),
            pltpu.SemaphoreType.REGULAR((4,)),
        ],
        compiler_params=pltpu.CompilerParams(collective_id=0, has_side_effects=True),
        name="force_terms",
    )(links.reshape(shape))
    out = pl.pallas_call(
        functools.partial(expand, halves),
        out_shape=jax.ShapeDtypeStruct(shape, jnp.float32),
        in_specs=[pl.BlockSpec(memory_space=pltpu.VMEM)],
        out_specs=pl.BlockSpec(memory_space=pl.ANY),
        scratch_shapes=[vmem(*shape[:-1]), pltpu.SemaphoreType.DMA((4,))],
        name="expand",
    )(pltpu.with_memory_space_constraint(terms, pltpu.VMEM))
    return out.reshape(links.shape)


def solution(mesh):
    assert mesh.axis_names == ("gx", "gz", "ta")
    counts = tuple(mesh.shape[a] for a in AXES)
    spec = P(None, None, None, None, "ta", "gz", "gx")
    return jax.shard_map(
        functools.partial(per_device, counts),
        mesh=mesh,
        in_specs=(spec,),
        out_specs=spec,
        check_vma=False,
    )
```
